32 devices in a mesh: seq: 16 (over z, y, x), head: 2 (over core).
Axes of the slice: x: 2, y: 2, z: 4, core: 2. Of those that a mesh axis runs over, the one named last changes fastest.
Arguments:
- queries: bfloat16 [2048, 2048], P('seq', 'head'), may hold values from -6 to 6
- key_vectors: bfloat16 [2, 2048, 2048], P(None, 'seq', 'head'), may hold values from -6 to 6
- values: bfloat16 [2, 2048, 2048], P(None, 'seq', 'head'), may hold values from -6 to 6
- strengths: float32 [2, 16, 2048], P(None, 'head', 'seq'), may hold values from 0.05 to 1.95
- out_weight: bfloat16 [2048, 4096], P('head', 'seq'), may hold values from -0.1875 to 0.1875
Outputs:
- mixed: bfloat16 [2048, 4096], P('seq', 'head')
The draws below stay inside these ranges and needn't reach their ends.
All inputs are finite; a program needn't handle non-finite values.
Results may differ from the reference program's by a relative error of at most 0.014.
Values may be sent and summed in bfloat16 or wider, within the bound.
No kernel may reach another device: no remote copies, remote signals or barrier semaphores. Data moves between devices by JAX's collectives and lax.ppermute only.
A program may use at most 64 MiB of HBM per device.

```python
import jax
import jax.numpy as jnp
from jax import lax

D = 4096
H = 16
DK = 128
BLOCK = 64
TOKENS = 2048
N_HEAD = 2


def draw_key_vectors(key, part):
    base_key, head_key, dim_key, scale_key = jax.random.split(jax.random.fold_in(key, 7), 4)
    base = jnp.clip(jax.random.normal(base_key, (2, TOKENS, H, DK), jnp.float32), -6.0, 6.0)
    slow_head = jax.random.randint(head_key, (H,), 0, 2) > 0
    weak_dim = jax.random.randint(dim_key, (H, DK), 0, 4) > 0
    block_scale = jnp.exp(jax.random.uniform(scale_key, (TOKENS // BLOCK, 1, H, 1), jnp.float32, jnp.log(0.01), jnp.log(0.04)))
    block_scale = jnp.repeat(block_scale, BLOCK, axis=0)[:, 0]
    factor = jnp.where((slow_head[:, None] & weak_dim)[None], block_scale, 1.0)
    return (base * factor[None]).reshape(2, TOKENS, H * DK).astype(jnp.bfloat16)


def raised(drawn, own_key, source, target, parts, factor):
    owner, partner = [(jnp.arange(drawn.shape[position]) // (drawn.shape[position] // parts)).reshape([-1 if axis == position else 1 for axis in range(drawn.ndim)]) for position in (source, target)]
    chosen = jax.random.permutation(own_key, parts)[partner]
    strong = (owner == chosen) | (owner == (partner + parts // 2) % parts)
    return jnp.where(strong, factor * drawn, drawn)


def level_of(stream_key, dims, pieces, low, high):
    gain = 1.0
    for position, shards_of in pieces:
        heights = jax.random.uniform(jax.random.fold_in(jax.random.fold_in(stream_key, 6), position), (shards_of,), jnp.float32, low / len(pieces), high / len(pieces))
        gain = gain * jnp.repeat(jnp.exp(heights), dims[position] // shards_of).reshape((-1,) + (1,) * (len(dims) - 1 - position))
    return gain


def gaussian(stream_key, extent, scale, bound, cuts=(), held_as=jnp.bfloat16):
    result = scale * jax.random.normal(stream_key, extent, jnp.float32)
    if cuts:
        result = result * level_of(stream_key, extent, cuts, -0.22, 0.18)
    return jnp.clip(result, -bound, bound).astype(held_as)


def heavy_noise(key, dims, width, reach, pieces, heavy, kind=jnp.bfloat16):
    drawn = width * jax.random.normal(key, dims, jnp.float32)
    if pieces:
        drawn = drawn * level_of(key, dims, pieces, -0.22, 0.18)
    return jnp.clip(raised(drawn, jax.random.fold_in(key, 3), *heavy), -reach, reach).astype(kind)


def setup_inputs(seed: int = 0) -> dict:
    key_of = jax.random.split(jax.random.key(seed), 6)
    queries = gaussian(key_of[0], (TOKENS, H * DK), 1.0, 6.0, ((0, 16), (1, 2)))
    key_vectors = draw_key_vectors(jax.random.fold_in(key_of[5], 71), 0)
    values = gaussian(key_of[2], (2, TOKENS, H * DK), 1.0, 6.0, ((1, 16), (2, 2)))
    strengths = jnp.clip(0.05 + 1.90000005 * jax.random.uniform(key_of[3], (2, H, TOKENS), jnp.float32) ** level_of(key_of[3], (2, H, TOKENS), ((1, 2), (2, 16)), -0.2, 0.2), 0.05, 1.95)
    out_weight = heavy_noise(key_of[4], (H * DK, D), (H * DK) ** -0.5, 0.1875, ((0, 2), (1, 16)), (0, 1, 16, 2.0))
    return dict(queries=queries, key_vectors=key_vectors, values=values, strengths=strengths, out_weight=out_weight)


HIGHEST_PRECISION = lax.Precision.HIGHEST

def unit_rows(matrix):
    return matrix * lax.rsqrt(lax.optimization_barrier(jnp.sum(matrix * matrix, axis=-1, keepdims=True)) + 1e-06)

def reflect_block(state, block):
    query_block, key_block, value_block, beta_block = block
    head_count = beta_block.shape[1]
    rows = query_block.shape[0]
    head_width = query_block.shape[1] // head_count
    query_heads = jnp.transpose(unit_rows(query_block.astype(jnp.float32).reshape(rows, head_count, head_width)), (1, 0, 2))
    key_heads = jnp.transpose(unit_rows(key_block.astype(jnp.float32).reshape(2, rows, head_count, head_width)), (2, 1, 0, 3)).reshape(head_count, 2 * rows, head_width)
    value_heads = jnp.transpose(value_block.astype(jnp.float32).reshape(2, rows, head_count, head_width), (2, 1, 0, 3)).reshape(head_count, 2 * rows, head_width)
    beta_heads = jnp.transpose(beta_block, (1, 2, 0)).reshape(head_count, 2 * rows)
    key_gram = jnp.einsum('hik,hjk->hij', key_heads, key_heads, precision=HIGHEST_PRECISION)
    system = jnp.tril(key_gram, -1) * beta_heads[:, :, None] + jnp.eye(2 * rows, dtype=jnp.float32)
    right_side = beta_heads[:, :, None] * (value_heads - jnp.einsum('hik,hvk->hiv', key_heads, state, precision=HIGHEST_PRECISION))
    updates = jax.scipy.linalg.solve_triangular(system, right_side, lower=True, unit_diagonal=True)
    row_ids = lax.broadcasted_iota(jnp.int32, (rows, 2 * rows), 0)
    col_ids = lax.broadcasted_iota(jnp.int32, (rows, 2 * rows), 1)
    reach_mask = (col_ids <= 2 * row_ids + 1).astype(jnp.float32)
    scores = jnp.einsum('htk,hik->hti', query_heads, key_heads, precision=HIGHEST_PRECISION) * reach_mask
    block_out = jnp.einsum('hvk,htk->htv', state, query_heads, precision=HIGHEST_PRECISION) + jnp.einsum('hti,hiv->htv', scores, updates, precision=HIGHEST_PRECISION)
    new_state = state + jnp.einsum('hiv,hik->hvk', updates, key_heads, precision=HIGHEST_PRECISION)
    return (new_state, block_out)

def reference(queries, key_vectors, values, strengths, out_weight):
    block_count = TOKENS // BLOCK
    query_blocks = queries.reshape(block_count, BLOCK, H * DK)
    key_blocks = jnp.moveaxis(key_vectors.reshape(2, block_count, BLOCK, H * DK), 1, 0)
    value_blocks = jnp.moveaxis(values.reshape(2, block_count, BLOCK, H * DK), 1, 0)
    beta_blocks = jnp.moveaxis(strengths.reshape(2, H, block_count, BLOCK), 2, 0)
    initial = jnp.zeros((H, DK, DK), jnp.float32)
    final_state, outputs = lax.scan(reflect_block, initial, (query_blocks, key_blocks, value_blocks, beta_blocks))
    heads_out = jnp.transpose(outputs, (0, 2, 1, 3)).reshape(TOKENS, H * DK).astype(jnp.bfloat16)
    group_rows = H * DK // N_HEAD
    total = jnp.zeros((TOKENS, D), jnp.float32)
    for group in range(N_HEAD):
        lower_row = group * group_rows
        upper_row = lower_row + group_rows
        group_sum = jnp.dot(heads_out[:, lower_row:upper_row].astype(jnp.float32), out_weight[lower_row:upper_row].astype(jnp.float32), preferred_element_type=jnp.float32)
        total = total + group_sum.astype(jnp.bfloat16).astype(jnp.float32)
    return total.astype(jnp.bfloat16)
```

```python
import functools

import jax
import jax.numpy as jnp
from jax import lax
from jax.experimental import pallas as pl
from jax.experimental.pallas import tpu as pltpu
from jax.sharding import PartitionSpec as P


CHUNK = 128
EPS = 1e-06
F32 = jnp.float32
BF16 = jnp.bfloat16


def dot(a, b):
    return jnp.dot(a, b, preferred_element_type=F32)


def dot_t(a, b):
    return lax.dot_general(a, b, (((1,), (1,)), ((), ())), preferred_element_type=F32)


def split(x):
    high = x.astype(BF16)
    return high, (x - high.astype(F32)).astype(BF16)


def product3(left, right):
    left_high, left_low = split(left)
    right_high, right_low = split(right)
    lhs = jnp.concatenate([left_high, left_low], axis=1)
    rhs = jnp.concatenate(
        [
            jnp.concatenate([right_high, right_low], axis=1),
            jnp.concatenate([right_high, jnp.zeros_like(right_low)], axis=1),
        ],
        axis=0,
    )
    wide = dot(lhs, rhs)
    width = right.shape[1]
    return wide[:, :width] + wide[:, width:]


def iota(shape, axis):
    return lax.broadcasted_iota(jnp.int32, shape, axis)


def weave(first, second):
    half = first.shape[0] // 2
    return jnp.concatenate([first[:half], second[:half], first[half:], second[half:]], axis=0)


def weave_lanes(first, second):
    half = first.shape[1] // 2
    return jnp.concatenate(
        [first[:, :half], second[:, :half], first[:, half:], second[:, half:]], axis=1
    )


def place(position, offset):
    return jnp.bitwise_xor(position, offset)


def gather_blocks(sources, target, sems, slots):
    copies = []
    for offset, (source, slot) in enumerate(zip(sources, slots)):
        copies.append(pltpu.make_async_copy(source, target.at[slot], sems.at[offset]))
    for copy in copies:
        copy.start()
    return copies


def recur_kernel(group, *refs):
    key_in, rest_in, beta_in = refs[:group], refs[group : 2 * group], refs[2 * group : 3 * group]
    out_ref, lift_ref, state_ref = refs[3 * group : 3 * group + 3]
    key_buf, rest_buf, beta_buf, a_buf, off_buf, t_buf, sems = refs[3 * group + 3 :]
    position = lax.rem(lax.axis_index("seq"), group)
    slots = [place(position, offset) for offset in range(group)]
    copies = gather_blocks(key_in, key_buf, sems.at[0], slots)
    copies += gather_blocks(beta_in, beta_buf, sems.at[1], slots)
    copies += gather_blocks(rest_in, rest_buf, sems.at[2], slots)
    for copy in copies:
        copy.wait()
    tokens = key_buf.shape[2]
    heads = beta_buf.shape[1]
    width = key_buf.shape[3] // heads
    chunk = min(CHUNK, tokens)
    half = chunk // 2
    per_source = tokens // chunk
    chunks = group * per_source

    row = iota((chunk, chunk), 0)
    col = iota((chunk, chunk), 1)
    row_time = 2 * lax.rem(row, half) + row // half
    col_time = 2 * lax.rem(col, half) + col // half
    levels = chunk.bit_length() - 1

    def joins(level):
        same = (row_time >> (level + 1)) == (col_time >> (level + 1))
        return same & (((row_time >> level) & 1) == 1) & (((col_time >> level) & 1) == 0)

    def one_head(head, carry):
        lanes = pl.ds(pl.multiple_of(head * width, width), width)
        keys, columns = [], []
        for index in range(chunks):
            source, first = index // per_source, (index % per_source) * chunk
            rows = pl.ds(first, chunk)
            key = weave(key_buf[source, 0, rows, lanes], key_buf[source, 1, rows, lanes])
            gram = dot_t(key, key)
            wide_row, wide_col = iota(gram.shape, 0), iota(gram.shape, 1)
            square = jnp.sum(jnp.where(wide_row == wide_col, gram, 0.0), axis=0, keepdims=True)
            scale_row = lax.rsqrt(square + EPS)
            beta_row = weave_lanes(
                beta_buf[source, head, 0:1, rows], beta_buf[source, head, 1:2, rows]
            )
            both_row = beta_row * scale_row
            table = jnp.concatenate(
                [scale_row, beta_row, both_row, jnp.zeros((5, 2 * chunk), F32)], axis=0
            ).T
            columns.append((scale_row, table))
            system = table[:, 2:3] * (gram * scale_row)
            for block in range(2):
                here = slice(block * chunk, (block + 1) * chunk)
                diagonal = system[here, here]
                a_buf[2 * index + block] = diagonal
                t_buf[2 * index + block] = jnp.where(row == col, 1.0, 0.0) - jnp.where(
                    joins(0), diagonal, 0.0
                )
            off_buf[index] = system[chunk:, :chunk]
            keys.append(key)
        for level in range(1, levels):
            mask = joins(level)
            inner = [
                product3(jnp.where(mask, a_buf[c], 0.0), t_buf[c]) for c in range(2 * chunks)
            ]
            for c in range(2 * chunks):
                t_buf[c] = t_buf[c] - product3(t_buf[c], inner[c])
        inner = [product3(off_buf[c], t_buf[2 * c]) for c in range(chunks)]
        for c in range(chunks):
            off_buf[c] = -product3(t_buf[2 * c + 1], inner[c])

        before = None
        for index in range(chunks):
            source, first = index // per_source, (index % per_source) * chunk
            rows = pl.ds(first, chunk)
            scale_row, table = columns[index]
            key = keys[index]
            value = weave(rest_buf[source, 0, rows, lanes], rest_buf[source, 1, rows, lanes])
            query = rest_buf[source, 2, rows, lanes]
            key_wide, query_wide = key.astype(F32), query.astype(F32)
            inverse = jnp.concatenate(
                [
                    jnp.concatenate([t_buf[2 * index], jnp.zeros((chunk, chunk), F32)], axis=1),
                    jnp.concatenate([off_buf[index], t_buf[2 * index + 1]], axis=1),
                ],
                axis=0,
            )
            right = jnp.concatenate(
                [table[:, 2:3] * key_wide, table[:, 1:2] * value.astype(F32)], axis=1
            )
            inverse_high, inverse_low = split(inverse)
            right_high, right_low = split(right)
            solved = (
                dot(inverse_high, right_high)
                + dot(inverse_low, right_high)
                + dot(inverse_high, right_low)
            )
            query_scale = lax.rsqrt(
                jnp.sum(query_wide * query_wide, axis=1, keepdims=True) + EPS
            )
            token_row = iota((chunk, 2 * chunk), 0)
            token_col = iota((chunk, 2 * chunk), 1)
            token_col = (token_col // chunk) * half + lax.rem(token_col, half)
            scores = jnp.where(
                token_col <= token_row, dot_t(query, key) * (query_scale * scale_row), 0.0
            )
            turned = (table[:, 0:1] * key_wide).T
            stack = jnp.concatenate([scores, turned], axis=0).astype(BF16)
            applied = dot(stack, solved.astype(BF16))
            lifted = query_scale * query_wide - applied[:chunk, :width]
            local = applied[:chunk, width:]
            step = applied[chunk:]
            place_rows = pl.ds(index * chunk, chunk)
            if before is None:
                before = step
            else:
                moved = dot(
                    jnp.concatenate([lifted, step[:, :width]], axis=0).astype(BF16),
                    before.astype(BF16),
                )
                local = local + moved[:chunk, width:]
                lifted = lifted - moved[:chunk, :width]
                before = before + step - moved[chunk:]
            out_ref[place_rows, lanes] = local
            lift_ref[place_rows, lanes] = lifted.astype(BF16)
        state_ref[head] = before.astype(BF16)
        return carry

    lax.fori_loop(0, heads, one_head, 0)


def recur(keys, rests, betas):
    group = len(keys)
    _, tokens, wide = keys[0].shape
    heads = betas[0].shape[0]
    width = wide // heads
    chunk = min(CHUNK, tokens)
    chunks = group * tokens // chunk
    anywhere = pl.BlockSpec(memory_space=pl.ANY)
    vmem = pl.BlockSpec(memory_space=pltpu.VMEM)
    return pl.pallas_call(
        functools.partial(recur_kernel, group),
        out_shape=(
            jax.ShapeDtypeStruct((group * tokens, wide), F32),
            jax.ShapeDtypeStruct((group * tokens, wide), BF16),
            jax.ShapeDtypeStruct((heads, width, 2 * width), BF16),
        ),
        in_specs=[anywhere] * (3 * group),
        out_specs=(vmem, vmem, vmem),
        scratch_shapes=[
            pltpu.VMEM((group, 2, tokens, wide), BF16),
            pltpu.VMEM((group, 3, tokens, wide), BF16),
            pltpu.VMEM((group,) + betas[0].shape, F32),
            pltpu.VMEM((2 * chunks, chunk, chunk), F32),
            pltpu.VMEM((chunks, chunk, chunk), F32),
            pltpu.VMEM((2 * chunks, chunk, chunk), F32),
            pltpu.SemaphoreType.DMA((3, group)),
        ],
        name="recur",
    )(*keys, *rests, *betas)


def join_kernel(count, *refs):
    states, (local_ref, lift_ref, out_ref) = refs[:count], refs[count:]
    heads, width, _ = states[0].shape
    for head in range(heads):
        lanes = slice(head * width, (head + 1) * width)
        total = None
        for state in reversed(states):
            step = state[head].astype(F32)
            if total is None:
                total = step[:, width:]
            else:
                total = (
                    total + step[:, width:] - dot(state[head, :, :width], total.astype(BF16))
                )
        out_ref[:, lanes] = (
            local_ref[:, lanes] + dot(lift_ref[:, lanes], total.astype(BF16))
        ).astype(BF16)


def join(states, local, lifted):
    return pl.pallas_call(
        functools.partial(join_kernel, len(states)),
        out_shape=jax.ShapeDtypeStruct(local.shape, BF16),
        name="join",
    )(*states, local, lifted)


def compose(earlier, later):
    width = earlier.shape[1]
    moved = jnp.einsum("hab,hbc->hac", later[:, :, :width], earlier, preferred_element_type=F32)
    return (earlier.astype(F32) + later.astype(F32) - moved).astype(BF16)


def project_kernel(group, planes, *refs):
    count = group + planes
    heads_in, weight_in = refs[:group], refs[group:count]
    send_ref, keep_ref = refs[count : count + 2]
    heads_buf, weight_buf, sems = refs[count + 2 :]
    device = lax.axis_index("seq")
    core = lax.axis_index("head")
    position, plane = lax.rem(device, group), device // group
    wide = heads_in[0].shape[1]
    copies = []
    for offset in range(planes):
        slot = lax.rem(plane + planes - offset, planes)
        copies.append(
            pltpu.make_async_copy(weight_in[offset], weight_buf.at[slot], sems.at[offset])
        )
    for offset in range(group):
        lanes = pl.ds(pl.multiple_of(place(position, offset) * wide, wide), wide)
        copies.append(
            pltpu.make_async_copy(
                heads_in[offset], heads_buf.at[:, lanes], sems.at[planes + offset]
            )
        )
    for copy in copies:
        copy.start()
    for copy in copies:
        copy.wait()
    columns = weight_buf.shape[2]
    side = planes // 2
    for target, owner in ((send_ref, 1 - core), (keep_ref, core)):
        for index in range(side):
            result = dot(heads_buf[...], weight_buf[owner * side + index])
            target[:, index * columns : (index + 1) * columns] = result.astype(BF16)


def project(heads, weights):
    group, planes = len(heads), len(weights)
    rows, wide = heads[0].shape
    depth, columns = weights[0].shape
    shape = jax.ShapeDtypeStruct((rows, columns * planes // 2), BF16)
    vmem = pl.BlockSpec(memory_space=pltpu.VMEM)
    return pl.pallas_call(
        functools.partial(project_kernel, group, planes),
        out_shape=(shape, shape),
        in_specs=[pl.BlockSpec(memory_space=pl.ANY)] * (group + planes),
        out_specs=(vmem, vmem),
        scratch_shapes=[
            pltpu.VMEM((rows, group * wide), BF16),
            pltpu.VMEM((planes, depth, columns), BF16),
            pltpu.SemaphoreType.DMA((planes + group,)),
        ],
        name="project",
    )(*heads, *weights)


def sum_kernel(group, keep_ref, other_ref, *outs):
    position = lax.rem(lax.axis_index("seq"), group)
    tokens = outs[0].shape[0]
    for offset in range(group):
        rows = pl.ds(pl.multiple_of(place(position, offset) * tokens, tokens), tokens)
        outs[offset][...] = (
            keep_ref[rows, :].astype(F32) + other_ref[rows, :].astype(F32)
        ).astype(BF16)


def sum_parts(keep, other, group):
    rows, columns = keep.shape
    return pl.pallas_call(
        functools.partial(sum_kernel, group),
        out_shape=[jax.ShapeDtypeStruct((rows // group, columns), BF16)] * group,
        name="sum_parts",
    )(keep, other)


def lay_kernel(group, columns, *refs):
    parts, out_ref = refs[:group], refs[group]
    position = lax.rem(lax.axis_index("seq"), group)
    for offset in range(group):
        for index in range(parts[0].shape[1] // columns):
            first = (index * group + place(position, offset)) * columns
            out_ref[:, pl.ds(pl.multiple_of(first, columns), columns)] = parts[offset][
                :, index * columns : (index + 1) * columns
            ]


def lay_out(parts, columns):
    group = len(parts)
    rows, wide = parts[0].shape
    return pl.pallas_call(
        functools.partial(lay_kernel, group, columns),
        out_shape=jax.ShapeDtypeStruct((rows, group * wide), BF16),
        name="lay_out",
    )(*parts)


def swap(value, group, offset, count):
    pairs = [(i, (i // group) * group + ((i % group) ^ offset)) for i in range(count)]
    return lax.ppermute(value, "seq", pairs)


def per_device(queries, key_vectors, values, strengths, out_weight):
    count = lax.axis_size("seq")
    sides = lax.axis_size("head")
    heads = strengths.shape[1]
    tokens = queries.shape[0]
    width = queries.shape[1] // heads
    group = 1
    while group < 4 and heads % (2 * group) == 0 and count % (2 * group) == 0:
        group *= 2
    planes = count // group
    position = lax.axis_index("seq") % group
    mine = heads // group
    beta = jnp.swapaxes(strengths, 0, 1)

    keys, rests, betas = [], [], []
    for offset in range(group):
        target = jnp.bitwise_xor(position, offset)
        lane = target * mine * width
        key = lax.dynamic_slice_in_dim(key_vectors, lane, mine * width, 2)
        rest = jnp.concatenate(
            [
                lax.dynamic_slice_in_dim(values, lane, mine * width, 2),
                lax.dynamic_slice_in_dim(queries, lane, mine * width, 1)[None],
            ],
            axis=0,
        )
        strength = lax.dynamic_slice_in_dim(beta, target * mine, mine, 0)
        if offset:
            strength = swap(strength, group, offset, count)
            key = swap(key, group, offset, count)
            rest = swap(rest, group, offset, count)
        keys.append(key)
        rests.append(rest)
        betas.append(strength)

    split_out = sides == 2 and planes % 2 == 0 and planes <= 4 and group > 1
    weights = [out_weight]
    if split_out:
        for offset in range(1, planes):
            pairs = [
                (i, ((i // group + offset) % planes) * group + i % group) for i in range(count)
            ]
            weights.append(lax.ppermute(out_weight, "seq", pairs))

    local, lifted, state = recur(keys, rests, betas)

    def from_earlier(value, distance):
        pairs = [(i, i + distance * group) for i in range(count - distance * group)]
        return lax.ppermute(value, "seq", pairs)

    if planes <= 4:
        states = [from_earlier(state, distance) for distance in range(1, planes)]
    else:
        total = from_earlier(state, 1)
        distance = 1
        while distance < planes - 1:
            total = compose(from_earlier(total, distance), total)
            distance *= 2
        states = [total]
    mixed_heads = join(states, local, lifted)

    if split_out:
        gathered = [mixed_heads] + [
            swap(mixed_heads, group, offset, count) for offset in range(1, group)
        ]
        send, keep = project(gathered, weights)
        other = lax.ppermute(send, "head", [(0, 1), (1, 0)])
        parts = sum_parts(keep, other, group)
        parts = [parts[0]] + [
            swap(parts[offset], group, offset, count) for offset in range(1, group)
        ]
        return lay_out(parts, out_weight.shape[1])

    if group > 1:
        position_rows = []
        for offset in range(group):
            first = jnp.bitwise_xor(position, offset) * tokens
            part = lax.dynamic_slice_in_dim(mixed_heads, first, tokens, 0)
            position_rows.append(swap(part, group, offset, count) if offset else part)
        stacked = jnp.stack(position_rows)
        order = jnp.bitwise_xor(position, jnp.arange(group))
        stacked = jnp.take(stacked, order, axis=0)
        mixed_heads = jnp.swapaxes(stacked, 0, 1).reshape(tokens, heads * width)
    partial_sums = jnp.dot(
        mixed_heads,
        lax.all_gather(out_weight, "seq", axis=1, tiled=True),
        preferred_element_type=F32,
    )
    return lax.psum_scatter(
        partial_sums.astype(BF16), "head", scatter_dimension=1, tiled=True
    )


def solution(mesh):
    return jax.shard_map(
        per_device,
        mesh=mesh,
        in_specs=(
            P("seq", "head"),
            P(None, "seq", "head"),
            P(None, "seq", "head"),
            P(None, "head", "seq"),
            P("head", "seq"),
        ),
        out_specs=P("seq", "head"),
        check_vma=False,
    )
```

```python
import functools

import jax
import jax.numpy as jnp
from jax import lax
from jax.experimental import pallas as pl
from jax.experimental.pallas import tpu as pltpu
from jax.sharding import PartitionSpec as P


CHUNK = 128
EPS = 1e-06
F32 = jnp.float32
BF16 = jnp.bfloat16


def dot(a, b):
    return jnp.dot(a, b, preferred_element_type=F32)


def dot_t(a, b):
    return lax.dot_general(a, b, (((1,), (1,)), ((), ())), preferred_element_type=F32)


def split(x):
    high = x.astype(BF16)
    return high, (x - high.astype(F32)).astype(BF16)


def product3(left, right):
    left_high, left_low = split(left)
    right_high, right_low = split(right)
    lhs = jnp.concatenate([left_high, left_low], axis=1)
    rhs = jnp.concatenate(
        [
            jnp.concatenate([right_high, right_low], axis=1),
            jnp.concatenate([right_high, jnp.zeros_like(right_low)], axis=1),
        ],
        axis=0,
    )
    wide = dot(lhs, rhs)
    width = right.shape[1]
    return wide[:, :width] + wide[:, width:]


def iota(shape, axis):
    return lax.broadcasted_iota(jnp.int32, shape, axis)


def weave(first, second):
    half = first.shape[0] // 2
    return jnp.concatenate([first[:half], second[:half], first[half:], second[half:]], axis=0)


def weave_lanes(first, second):
    half = first.shape[1] // 2
    return jnp.concatenate(
        [first[:, :half], second[:, :half], first[:, half:], second[:, half:]], axis=1
    )


def place(position, offset):
    return jnp.bitwise_xor(position, offset)


VMEM = pl.BlockSpec(memory_space=pltpu.VMEM)
PARAMS = pltpu.CompilerParams(vmem_limit_bytes=12 * 2**20)


def held(*arrays):
    return [pltpu.with_memory_space_constraint(array, pltpu.VMEM) for array in arrays]


def times(chunk):
    half = chunk // 2
    row, col = iota((chunk, chunk), 0), iota((chunk, chunk), 1)
    return 2 * lax.rem(row, half) + row // half, 2 * lax.rem(col, half) + col // half


def beta_rows(tokens, width):
    return -(-4 * max(tokens // width, 1) // 16) * 16


def invert_kernel(heads, tokens, *refs):
    key_in, (inverse_ref, table_ref, a_buf) = refs[:-3], refs[-3:]
    width = key_in[0].shape[1] // heads
    chunk = min(CHUNK, tokens)
    per_source = tokens // chunk
    chunks = len(key_in) * per_source
    pieces = max(tokens // width, 1)
    row_time, col_time = times(chunk)
    levels = chunk.bit_length() - 1

    def joins(level):
        same = (row_time >> (level + 1)) == (col_time >> (level + 1))
        return same & (((row_time >> level) & 1) == 1) & (((col_time >> level) & 1) == 0)

    def one_head(head, carry):
        lanes = pl.ds(pl.multiple_of(head * width, width), width)
        for index in range(chunks):
            key_ref, first = key_in[index // per_source], (index % per_source) * chunk
            key = weave(
                key_ref[first : first + chunk, lanes],
                key_ref[tokens + first : tokens + first + chunk, lanes],
            )
            gram = dot_t(key, key)
            wide_row, wide_col = iota(gram.shape, 0), iota(gram.shape, 1)
            square = jnp.sum(jnp.where(wide_row == wide_col, gram, 0.0), axis=0, keepdims=True)
            scale_row = lax.rsqrt(square + EPS)
            halves = key_ref[2 * tokens :, lanes].astype(F32)
            piece, inside = first // width, first % width

            def strength(reflection):
                high = reflection * pieces + piece
                low = (2 + reflection) * pieces + piece
                both = halves[high : high + 1] + halves[low : low + 1]
                return both[:, inside : inside + chunk]

            beta_row = weave_lanes(strength(0), strength(1))
            both_row = beta_row * scale_row
            table = jnp.concatenate(
                [scale_row, beta_row, both_row, jnp.zeros((5, 2 * chunk), F32)], axis=0
            )
            table_ref[head, index] = table
            system = table.T[:, 2:3] * (gram * scale_row)
            for block in range(2):
                here = slice(block * chunk, (block + 1) * chunk)
                diagonal = system[here, here]
                a_buf[2 * index + block] = diagonal
                inverse_ref[head, index, block] = jnp.where(
                    row_time == col_time, 1.0, 0.0
                ) - jnp.where(joins(0), diagonal, 0.0)
            inverse_ref[head, index, 2] = system[chunk:, :chunk]
        every = [(index, block) for index in range(chunks) for block in range(2)]
        for level in range(1, levels):
            mask = joins(level)
            inner = [
                product3(
                    jnp.where(mask, a_buf[2 * index + block], 0.0),
                    inverse_ref[head, index, block],
                )
                for index, block in every
            ]
            for (index, block), value in zip(every, inner):
                held = inverse_ref[head, index, block]
                inverse_ref[head, index, block] = held - product3(held, value)
        inner = [
            product3(inverse_ref[head, index, 2], inverse_ref[head, index, 0])
            for index in range(chunks)
        ]
        for index in range(chunks):
            inverse_ref[head, index, 2] = -product3(inverse_ref[head, index, 1], inner[index])
        return carry

    lax.fori_loop(0, heads, one_head, 0)


def invert(keys, heads, tokens):
    chunk = min(CHUNK, tokens)
    chunks = len(keys) * tokens // chunk
    return pl.pallas_call(
        functools.partial(invert_kernel, heads, tokens),
        out_shape=(
            pltpu.VMEM((heads, chunks, 3, chunk, chunk), F32),
            pltpu.VMEM((heads, chunks, 8, 2 * chunk), F32),
        ),
        in_specs=[VMEM] * len(keys),
        out_specs=(VMEM, VMEM),
        scratch_shapes=[pltpu.VMEM((2 * chunks, chunk, chunk), F32)],
        compiler_params=PARAMS,
        name="invert",
    )(*held(*keys))


def slot_of(group, index, per_source):
    position = lax.rem(lax.axis_index("seq"), group)
    return place(position, index // per_source) * per_source + index % per_source


def state_kernel(group, *refs):
    key_in, rest_in = refs[:group], refs[group : 2 * group]
    inverse_ref, table_ref = refs[2 * group : 2 * group + 2]
    high_ref, low_ref, before_ref, state_ref, step_buf = refs[2 * group + 2 :]
    heads, chunks, _, chunk, _ = inverse_ref.shape
    tokens = rest_in[0].shape[1]
    width = rest_in[0].shape[2] // heads
    per_source = tokens // chunk

    def one_head(head, carry):
        lanes = pl.ds(pl.multiple_of(head * width, width), width)
        for index in range(chunks):
            source, first = index // per_source, (index % per_source) * chunk
            key_ref, rest_ref = key_in[source], rest_in[source]
            key = weave(
                key_ref[first : first + chunk, lanes],
                key_ref[tokens + first : tokens + first + chunk, lanes],
            ).astype(F32)
            rows = slice(first, first + chunk)
            value = weave(rest_ref[0, rows, lanes], rest_ref[1, rows, lanes]).astype(F32)
            table = table_ref[head, index].T
            inverse = jnp.concatenate(
                [
                    jnp.concatenate(
                        [inverse_ref[head, index, 0], jnp.zeros((chunk, chunk), F32)], axis=1
                    ),
                    jnp.concatenate(
                        [inverse_ref[head, index, 2], inverse_ref[head, index, 1]], axis=1
                    ),
                ],
                axis=0,
            )
            right = jnp.concatenate([table[:, 2:3] * key, table[:, 1:2] * value], axis=1)
            high, low = split(dot3(inverse, *split(right)))
            high_ref[head, index] = high
            low_ref[head, index] = low
            step_buf[slot_of(group, index, per_source)] = dot3(
                (table[:, 0:1] * key).T, high, low
            )
        before = jnp.zeros((width, 2 * width), F32)
        for slot in range(chunks):
            narrow = before.astype(BF16)
            before_ref[head, slot] = narrow
            step = step_buf[slot]
            if slot:
                step = step - dot(step[:, :width].astype(BF16), narrow)
            before = before + step
        state_ref[head] = before.astype(BF16)
        return carry

    lax.fori_loop(0, heads, one_head, 0)


def dot3(left, high, low):
    left_high, left_low = split(left)
    return dot(left_high, high) + dot(left_low, high) + dot(left_high, low)


def carry_state(keys, rests, inverse, table):
    group = len(keys)
    heads, chunks, _, chunk, _ = inverse.shape
    width = rests[0].shape[2] // heads
    solved = pltpu.VMEM((heads, chunks, 2 * chunk, 2 * width), BF16)
    return pl.pallas_call(
        functools.partial(state_kernel, group),
        out_shape=(
            solved,
            solved,
            pltpu.VMEM((heads, chunks, width, 2 * width), BF16),
            pltpu.VMEM((heads, width, 2 * width), BF16),
        ),
        in_specs=[VMEM] * (2 * group + 2),
        out_specs=(VMEM,) * 4,
        scratch_shapes=[pltpu.VMEM((chunks, width, 2 * width), F32)],
        compiler_params=PARAMS,
        name="carry_state",
    )(*held(*keys, *rests, inverse, table))


def read_kernel(group, *refs):
    key_in, rest_in = refs[:group], refs[group : 2 * group]
    table_ref, high_ref, low_ref, before_ref, out_ref, lift_ref = refs[2 * group :]
    heads, chunks, _, wide = table_ref.shape
    chunk = wide // 2
    half = chunk // 2
    tokens = rest_in[0].shape[1]
    width = rest_in[0].shape[2] // heads
    per_source = tokens // chunk
    token_row = iota((chunk, 2 * chunk), 0)
    token_col = iota((chunk, 2 * chunk), 1)
    token_col = (token_col // chunk) * half + lax.rem(token_col, half)

    def one_head(head, carry):
        lanes = pl.ds(pl.multiple_of(head * width, width), width)
        for index in range(chunks):
            source, first = index // per_source, (index % per_source) * chunk
            key_ref, rest_ref = key_in[source], rest_in[source]
            key = weave(
                key_ref[first : first + chunk, lanes],
                key_ref[tokens + first : tokens + first + chunk, lanes],
            )
            query = rest_ref[2, first : first + chunk, lanes]
            wide_query = query.astype(F32)
            scale = lax.rsqrt(jnp.sum(wide_query * wide_query, axis=1, keepdims=True) + EPS)
            scores = jnp.where(
                token_col <= token_row,
                dot_t(query, key) * (scale * table_ref[head, index, 0:1, :]),
                0.0,
            )
            applied = dot3(scores, high_ref[head, index], low_ref[head, index])
            lifted = scale * wide_query - applied[:, :width]
            slot = slot_of(group, index, per_source)
            moved = dot(lifted.astype(BF16), before_ref[head, slot])
            rows = pl.ds(pl.multiple_of(slot * chunk, chunk), chunk)
            out_ref[rows, lanes] = applied[:, width:] + moved[:, width:]
            lift_ref[rows, lanes] = (lifted - moved[:, :width]).astype(BF16)
        return carry

    lax.fori_loop(0, heads, one_head, 0)


def read(keys, rests, table, high, low, before):
    group = len(keys)
    _, tokens, wide = rests[0].shape
    return pl.pallas_call(
        functools.partial(read_kernel, group),
        out_shape=(
            pltpu.VMEM((group * tokens, wide), F32),
            pltpu.VMEM((group * tokens, wide), BF16),
        ),
        in_specs=[VMEM] * (2 * group + 4),
        out_specs=(VMEM, VMEM),
        compiler_params=PARAMS,
        name="read",
    )(*held(*keys, *rests, table, high, low, before))


def join_kernel(count, *refs):
    states, (local_ref, lift_ref, out_ref) = refs[:count], refs[count:]
    heads, width, _ = states[0].shape
    for head in range(heads):
        lanes = slice(head * width, (head + 1) * width)
        total = None
        for state in reversed(states):
            step = state[head].astype(F32)
            if total is None:
                total = step[:, width:]
            else:
                total = (
                    total + step[:, width:] - dot(state[head, :, :width], total.astype(BF16))
                )
        out_ref[:, lanes] = (
            local_ref[:, lanes] + dot(lift_ref[:, lanes], total.astype(BF16))
        ).astype(BF16)


def join(states, local, lifted):
    return pl.pallas_call(
        functools.partial(join_kernel, len(states)),
        out_shape=pltpu.VMEM(local.shape, BF16),
        in_specs=[VMEM] * (len(states) + 2),
        out_specs=VMEM,
        compiler_params=PARAMS,
        name="join",
    )(*held(*states, local, lifted))


def compose(earlier, later):
    width = earlier.shape[1]
    moved = jnp.einsum("hab,hbc->hac", later[:, :, :width], earlier, preferred_element_type=F32)
    return (earlier.astype(F32) + later.astype(F32) - moved).astype(BF16)


def project_kernel(group, planes, *refs):
    count = group + planes
    heads_in, weight_in = refs[:group], refs[group:count]
    send_ref, keep_ref = refs[count:]
    device = lax.axis_index("seq")
    core = lax.axis_index("head")
    position, plane = lax.rem(device, group), device // group
    wide = heads_in[0].shape[1]
    side = planes // 2
    for offset in range(planes):
        columns = weight_in[offset].shape[1]
        owner = lax.rem(plane + planes - offset, planes)
        total = None
        for other in range(group):
            first = pl.multiple_of(place(position, other) * wide, wide)
            part = dot(heads_in[other][...], weight_in[offset][pl.ds(first, wide), :])
            total = part if total is None else total + part
        result = total.astype(BF16)
        lanes = pl.ds(pl.multiple_of(lax.rem(owner, side) * columns, columns), columns)

        @pl.when(owner // side == core)
        def _():
            keep_ref[:, lanes] = result

        @pl.when(owner // side != core)
        def _():
            send_ref[:, lanes] = result


def project(heads, weights):
    group, planes = len(heads), len(weights)
    rows = heads[0].shape[0]
    columns = weights[0].shape[1]
    shape = pltpu.VMEM((rows, columns * planes // 2), BF16)
    return pl.pallas_call(
        functools.partial(project_kernel, group, planes),
        out_shape=(shape, shape),
        in_specs=[VMEM] * (group + planes),
        out_specs=(VMEM, VMEM),
        compiler_params=PARAMS,
        name="project",
    )(*held(*heads, *weights))


def sum_kernel(group, keep_ref, other_ref, *outs):
    position = lax.rem(lax.axis_index("seq"), group)
    tokens = outs[0].shape[0]
    for offset in range(group):
        rows = pl.ds(pl.multiple_of(place(position, offset) * tokens, tokens), tokens)
        outs[offset][...] = (
            keep_ref[rows, :].astype(F32) + other_ref[rows, :].astype(F32)
        ).astype(BF16)


def sum_parts(keep, other, group):
    rows, columns = keep.shape
    return pl.pallas_call(
        functools.partial(sum_kernel, group),
        out_shape=[pltpu.VMEM((rows // group, columns), BF16)] * group,
        in_specs=[VMEM, VMEM],
        out_specs=[VMEM] * group,
        compiler_params=PARAMS,
        name="sum_parts",
    )(*held(keep, other))


def lay_kernel(group, columns, *refs):
    parts, out_ref, sems = refs[:group], refs[group], refs[group + 1]
    position = lax.rem(lax.axis_index("seq"), group)
    copies = []
    for offset in range(group):
        for index in range(parts[0].shape[1] // columns):
            first = (index * group + place(position, offset)) * columns
            copies.append(
                pltpu.make_async_copy(
                    parts[offset].at[:, index * columns : (index + 1) * columns],
                    out_ref.at[:, pl.ds(pl.multiple_of(first, columns), columns)],
                    sems.at[len(copies)],
                )
            )
    for copy in copies:
        copy.start()
    for copy in copies:
        copy.wait()


def lay_out(parts, columns):
    group = len(parts)
    rows, wide = parts[0].shape
    return pl.pallas_call(
        functools.partial(lay_kernel, group, columns),
        out_shape=jax.ShapeDtypeStruct((rows, group * wide), BF16),
        in_specs=[VMEM] * group,
        out_specs=pl.BlockSpec(memory_space=pl.ANY),
        scratch_shapes=[pltpu.SemaphoreType.DMA((group * wide // columns,))],
        compiler_params=PARAMS,
        name="lay_out",
    )(*held(*parts))


def swap(value, group, offset, count):
    pairs = [(i, (i // group) * group + ((i % group) ^ offset)) for i in range(count)]
    return lax.ppermute(value, "seq", pairs)


def per_device(queries, key_vectors, values, strengths, out_weight):
    count = lax.axis_size("seq")
    sides = lax.axis_size("head")
    heads = strengths.shape[1]
    tokens = queries.shape[0]
    width = queries.shape[1] // heads
    group = 1
    while group < 4 and heads % (2 * group) == 0 and count % (2 * group) == 0:
        group *= 2
    planes = count // group
    position = lax.axis_index("seq") % group
    mine = heads // group
    pieces = max(tokens // width, 1)
    high = lax.reduce_precision(strengths, 8, 7)
    beta = jnp.stack([high, strengths - high]).astype(BF16)
    beta = beta.reshape(4, heads, pieces, tokens // pieces)
    beta = jnp.pad(beta, ((0, 0), (0, 0), (0, 0), (0, width - tokens // pieces)))
    beta = jnp.swapaxes(beta, 1, 2).reshape(4 * pieces, heads * width)
    beta = jnp.pad(beta, ((0, beta_rows(tokens, width) - 4 * pieces), (0, 0)))
    packed = jnp.concatenate([key_vectors[0], key_vectors[1], beta], axis=0)

    keys, rests = [], []
    for offset in range(group):
        lane = jnp.bitwise_xor(position, offset) * mine * width
        key = lax.dynamic_slice_in_dim(packed, lane, mine * width, 1)
        rest = jnp.concatenate(
            [
                lax.dynamic_slice_in_dim(values, lane, mine * width, 2),
                lax.dynamic_slice_in_dim(queries, lane, mine * width, 1)[None],
            ],
            axis=0,
        )
        if offset:
            key = swap(key, group, offset, count)
            rest = swap(rest, group, offset, count)
        keys.append(key)
        rests.append(rest)

    split_out = sides == 2 and planes % 2 == 0 and planes <= 4 and group > 1
    weights = [out_weight]
    if split_out:
        for offset in range(1, planes):
            pairs = [
                (i, ((i // group + offset) % planes) * group + i % group)
                for i in range(count)
            ]
            weights.append(lax.ppermute(out_weight, "seq", pairs))

    inverse, table = invert(keys, mine, tokens)
    high, low, before, state = carry_state(keys, rests, inverse, table)
    local, lifted = read(keys, rests, table, high, low, before)

    def from_earlier(value, distance):
        pairs = [(i, i + distance * group) for i in range(count - distance * group)]
        return lax.ppermute(value, "seq", pairs)

    if planes <= 4:
        states = [from_earlier(state, distance) for distance in range(1, planes)]
    else:
        total = from_earlier(state, 1)
        distance = 1
        while distance < planes - 1:
            total = compose(from_earlier(total, distance), total)
            distance *= 2
        states = [total]
    mixed_heads = join(states, local, lifted)

    if split_out:
        gathered = [mixed_heads] + [
            swap(mixed_heads, group, offset, count) for offset in range(1, group)
        ]
        send, keep = project(gathered, weights)
        other = lax.ppermute(send, "head", [(0, 1), (1, 0)])
        parts = sum_parts(keep, other, group)
        parts = [parts[0]] + [
            swap(parts[offset], group, offset, count) for offset in range(1, group)
        ]
        return lay_out(parts, out_weight.shape[1])

    if group > 1:
        position_rows = []
        for offset in range(group):
            first = jnp.bitwise_xor(position, offset) * tokens
            part = lax.dynamic_slice_in_dim(mixed_heads, first, tokens, 0)
            position_rows.append(swap(part, group, offset, count) if offset else part)
        stacked = jnp.stack(position_rows)
        order = jnp.bitwise_xor(position, jnp.arange(group))
        stacked = jnp.take(stacked, order, axis=0)
        mixed_heads = jnp.swapaxes(stacked, 0, 1).reshape(tokens, heads * width)
    partial_sums = jnp.dot(
        mixed_heads,
        lax.all_gather(out_weight, "seq", axis=1, tiled=True),
        preferred_element_type=F32,
    )
    return lax.psum_scatter(
        partial_sums.astype(BF16), "head", scatter_dimension=1, tiled=True
    )


def solution(mesh):
    return jax.shard_map(
        per_device,
        mesh=mesh,
        in_specs=(
            P("seq", "head"),
            P(None, "seq", "head"),
            P(None, "seq", "head"),
            P(None, "head", "seq"),
            P("head", "seq"),
        ),
        out_specs=P("seq", "head"),
        check_vma=False,
    )
```

```python
import functools

import jax
import jax.numpy as jnp
from jax import lax
from jax.experimental import pallas as pl
from jax.experimental.pallas import tpu as pltpu
from jax.sharding import PartitionSpec as P


CHUNK = 128
EPS = 1e-06
F32 = jnp.float32
BF16 = jnp.bfloat16


def dot(a, b):
    return jnp.dot(a, b, preferred_element_type=F32)


def dot_t(a, b):
    return lax.dot_general(a, b, (((1,), (1,)), ((), ())), preferred_element_type=F32)


def split(x):
    high = x.astype(BF16)
    return high, (x - high.astype(F32)).astype(BF16)


def product3(left, right):
    left_high, left_low = split(left)
    right_high, right_low = split(right)
    lhs = jnp.concatenate([left_high, left_low], axis=1)
    rhs = jnp.concatenate(
        [
            jnp.concatenate([right_high, right_low], axis=1),
            jnp.concatenate([right_high, jnp.zeros_like(right_low)], axis=1),
        ],
        axis=0,
    )
    wide = dot(lhs, rhs)
    width = right.shape[1]
    return wide[:, :width] + wide[:, width:]


def iota(shape, axis):
    return lax.broadcasted_iota(jnp.int32, shape, axis)


def weave(first, second):
    half = first.shape[0] // 2
    return jnp.concatenate([first[:half], second[:half], first[half:], second[half:]], axis=0)


def weave_lanes(first, second):
    half = first.shape[1] // 2
    return jnp.concatenate(
        [first[:, :half], second[:, :half], first[:, half:], second[:, half:]], axis=1
    )


def place(position, offset):
    return jnp.bitwise_xor(position, offset)


VMEM = pl.BlockSpec(memory_space=pltpu.VMEM)
PARAMS = pltpu.CompilerParams(vmem_limit_bytes=12 * 2**20)


def held(*arrays):
    return [pltpu.with_memory_space_constraint(array, pltpu.VMEM) for array in arrays]


def times(chunk):
    half = chunk // 2
    row, col = iota((chunk, chunk), 0), iota((chunk, chunk), 1)
    return 2 * lax.rem(row, half) + row // half, 2 * lax.rem(col, half) + col // half


def beta_rows(tokens, width):
    return -(-4 * max(tokens // width, 1) // 16) * 16


def invert_kernel(heads, tokens, *refs):
    key_in, (inverse_ref, table_ref, a_buf) = refs[:-3], refs[-3:]
    width = key_in[0].shape[1] // heads
    chunk = min(CHUNK, tokens)
    per_source = tokens // chunk
    chunks = len(key_in) * per_source
    pieces = max(tokens // width, 1)
    row_time, col_time = times(chunk)
    levels = chunk.bit_length() - 1

    def joins(level):
        same = (row_time >> (level + 1)) == (col_time >> (level + 1))
        return same & (((row_time >> level) & 1) == 1) & (((col_time >> level) & 1) == 0)

    def one_head(head, carry):
        lanes = pl.ds(pl.multiple_of(head * width, width), width)
        for index in range(chunks):
            key_ref, first = key_in[index // per_source], (index % per_source) * chunk
            key = weave(
                key_ref[first : first + chunk, lanes],
                key_ref[tokens + first : tokens + first + chunk, lanes],
            )
            gram = dot_t(key, key)
            wide_row, wide_col = iota(gram.shape, 0), iota(gram.shape, 1)
            square = jnp.sum(jnp.where(wide_row == wide_col, gram, 0.0), axis=0, keepdims=True)
            scale_row = lax.rsqrt(square + EPS)
            halves = key_ref[2 * tokens :, lanes].astype(F32)
            piece, inside = first // width, first % width

            def strength(reflection):
                high = reflection * pieces + piece
                low = (2 + reflection) * pieces + piece
                both = halves[high : high + 1] + halves[low : low + 1]
                return both[:, inside : inside + chunk]

            beta_row = weave_lanes(strength(0), strength(1))
            both_row = beta_row * scale_row
            table = jnp.concatenate(
                [scale_row, beta_row, both_row, jnp.zeros((5, 2 * chunk), F32)], axis=0
            )
            table_ref[head, index] = table
            system = table.T[:, 2:3] * (gram * scale_row)
            for block in range(2):
                here = slice(block * chunk, (block + 1) * chunk)
                diagonal = system[here, here]
                a_buf[2 * index + block] = diagonal
                inverse_ref[head, index, block] = jnp.where(
                    row_time == col_time, 1.0, 0.0
                ) - jnp.where(joins(0), diagonal, 0.0)
            inverse_ref[head, index, 2] = system[chunk:, :chunk]
        every = [(index, block) for index in range(chunks) for block in range(2)]
        for level in range(1, levels):
            mask = joins(level)
            inner = [
                product3(
                    jnp.where(mask, a_buf[2 * index + block], 0.0),
                    inverse_ref[head, index, block],
                )
                for index, block in every
            ]
            for (index, block), value in zip(every, inner):
                held = inverse_ref[head, index, block]
                inverse_ref[head, index, block] = held - product3(held, value)
        inner = [
            product3(inverse_ref[head, index, 2], inverse_ref[head, index, 0])
            for index in range(chunks)
        ]
        for index in range(chunks):
            inverse_ref[head, index, 2] = -product3(inverse_ref[head, index, 1], inner[index])
        return carry

    lax.fori_loop(0, heads, one_head, 0)


def invert(keys, heads, tokens):
    chunk = min(CHUNK, tokens)
    chunks = len(keys) * tokens // chunk
    return pl.pallas_call(
        functools.partial(invert_kernel, heads, tokens),
        out_shape=(
            pltpu.VMEM((heads, chunks, 3, chunk, chunk), F32),
            pltpu.VMEM((heads, chunks, 8, 2 * chunk), F32),
        ),
        in_specs=[VMEM] * len(keys),
        out_specs=(VMEM, VMEM),
        scratch_shapes=[pltpu.VMEM((2 * chunks, chunk, chunk), F32)],
        compiler_params=PARAMS,
        name="invert",
    )(*held(*keys))


def slot_of(group, index, per_source):
    position = lax.rem(lax.axis_index("seq"), group)
    return place(position, index // per_source) * per_source + index % per_source


def state_kernel(group, *refs):
    key_in, rest_in = refs[:group], refs[group : 2 * group]
    inverse_ref, table_ref = refs[2 * group : 2 * group + 2]
    high_ref, low_ref, before_ref, state_ref, local_ref, step_buf = refs[2 * group + 2 :]
    heads, chunks, _, chunk, _ = inverse_ref.shape
    tokens = rest_in[0].shape[1]
    width = rest_in[0].shape[2] // heads
    per_source = tokens // chunk

    def one_head(head, carry):
        lanes = pl.ds(pl.multiple_of(head * width, width), width)
        for index in range(chunks):
            source, first = index // per_source, (index % per_source) * chunk
            key_ref, rest_ref = key_in[source], rest_in[source]
            key = weave(
                key_ref[first : first + chunk, lanes],
                key_ref[tokens + first : tokens + first + chunk, lanes],
            ).astype(F32)
            rows = slice(first, first + chunk)
            value = weave(rest_ref[0, rows, lanes], rest_ref[1, rows, lanes]).astype(F32)
            table = table_ref[head, index].T
            inverse = jnp.concatenate(
                [
                    jnp.concatenate(
                        [inverse_ref[head, index, 0], jnp.zeros((chunk, chunk), F32)], axis=1
                    ),
                    jnp.concatenate(
                        [inverse_ref[head, index, 2], inverse_ref[head, index, 1]], axis=1
                    ),
                ],
                axis=0,
            )
            right = jnp.concatenate([table[:, 2:3] * key, table[:, 1:2] * value], axis=1)
            high, low = split(dot3(inverse, *split(right)))
            high_ref[head, index] = high
            low_ref[head, index] = low
            step_buf[slot_of(group, index, per_source)] = dot3(
                (table[:, 0:1] * key).T, high, low
            )
        before = jnp.zeros((width, 2 * width), F32)
        for slot in range(chunks):
            narrow = before.astype(BF16)
            before_ref[head, slot] = narrow
            step = step_buf[slot]
            if slot:
                step = step - dot(step[:, :width].astype(BF16), narrow)
            before = before + step
        state_ref[head] = before.astype(BF16)
        local_ref[head] = before[:, width:].astype(BF16)
        return carry

    lax.fori_loop(0, heads, one_head, 0)


def dot3(left, high, low):
    left_high, left_low = split(left)
    return dot(left_high, high) + dot(left_low, high) + dot(left_high, low)


def carry_state(keys, rests, inverse, table):
    group = len(keys)
    heads, chunks, _, chunk, _ = inverse.shape
    width = rests[0].shape[2] // heads
    solved = pltpu.VMEM((heads, chunks, 2 * chunk, 2 * width), BF16)
    return pl.pallas_call(
        functools.partial(state_kernel, group),
        out_shape=(
            solved,
            solved,
            pltpu.VMEM((heads, chunks, width, 2 * width), BF16),
            pltpu.VMEM((heads, width, 2 * width), BF16),
            pltpu.VMEM((heads, width, width), BF16),
        ),
        in_specs=[VMEM] * (2 * group + 2),
        out_specs=(VMEM,) * 5,
        scratch_shapes=[pltpu.VMEM((chunks, width, 2 * width), F32)],
        compiler_params=PARAMS,
        name="carry_state",
    )(*held(*keys, *rests, inverse, table))


def read_kernel(group, *refs):
    key_in, rest_in = refs[:group], refs[group : 2 * group]
    table_ref, high_ref, low_ref, before_ref, out_ref, lift_ref = refs[2 * group :]
    heads, chunks, _, wide = table_ref.shape
    chunk = wide // 2
    half = chunk // 2
    tokens = rest_in[0].shape[1]
    width = rest_in[0].shape[2] // heads
    per_source = tokens // chunk
    token_row = iota((chunk, 2 * chunk), 0)
    token_col = iota((chunk, 2 * chunk), 1)
    token_col = (token_col // chunk) * half + lax.rem(token_col, half)

    def one_head(head, carry):
        lanes = pl.ds(pl.multiple_of(head * width, width), width)
        for index in range(chunks):
            source, first = index // per_source, (index % per_source) * chunk
            key_ref, rest_ref = key_in[source], rest_in[source]
            key = weave(
                key_ref[first : first + chunk, lanes],
                key_ref[tokens + first : tokens + first + chunk, lanes],
            )
            query = rest_ref[2, first : first + chunk, lanes]
            wide_query = query.astype(F32)
            scale = lax.rsqrt(jnp.sum(wide_query * wide_query, axis=1, keepdims=True) + EPS)
            scores = jnp.where(
                token_col <= token_row,
                dot_t(query, key) * (scale * table_ref[head, index, 0:1, :]),
                0.0,
            )
            applied = dot3(scores, high_ref[head, index], low_ref[head, index])
            lifted = scale * wide_query - applied[:, :width]
            slot = slot_of(group, index, per_source)
            moved = dot(lifted.astype(BF16), before_ref[head, slot])
            rows = pl.ds(pl.multiple_of(slot * chunk, chunk), chunk)
            out_ref[rows, lanes] = applied[:, width:] + moved[:, width:]
            lift_ref[rows, lanes] = (lifted - moved[:, :width]).astype(BF16)
        return carry

    lax.fori_loop(0, heads, one_head, 0)


def read(keys, rests, table, high, low, before):
    group = len(keys)
    _, tokens, wide = rests[0].shape
    return pl.pallas_call(
        functools.partial(read_kernel, group),
        out_shape=(
            pltpu.VMEM((group * tokens, wide), F32),
            pltpu.VMEM((group * tokens, wide), BF16),
        ),
        in_specs=[VMEM] * (2 * group + 4),
        out_specs=(VMEM, VMEM),
        compiler_params=PARAMS,
        name="read",
    )(*held(*keys, *rests, table, high, low, before))


def join_kernel(count, *refs):
    states, (local_ref, lift_ref, out_ref) = refs[:count], refs[count:]
    heads, width, _ = states[0].shape
    for head in range(heads):
        lanes = slice(head * width, (head + 1) * width)
        total = None
        for state in reversed(states):
            if total is None:
                total = state[head].astype(F32)
            else:
                step = state[head].astype(F32)
                total = (
                    total + step[:, width:] - dot(state[head, :, :width], total.astype(BF16))
                )
        out_ref[:, lanes] = (
            local_ref[:, lanes] + dot(lift_ref[:, lanes], total.astype(BF16))
        ).astype(BF16)


def join(states, local, lifted):
    return pl.pallas_call(
        functools.partial(join_kernel, len(states)),
        out_shape=pltpu.VMEM(local.shape, BF16),
        in_specs=[VMEM] * (len(states) + 2),
        out_specs=VMEM,
        compiler_params=PARAMS,
        name="join",
    )(*held(*states, local, lifted))


def compose(earlier, later):
    width = earlier.shape[1]
    moved = jnp.einsum("hab,hbc->hac", later[:, :, :width], earlier, preferred_element_type=F32)
    return (earlier.astype(F32) + later.astype(F32) - moved).astype(BF16)


def project_kernel(group, *refs):
    heads_in, weight_in, (send_ref, keep_ref) = refs[:group], refs[group:-2], refs[-2:]
    device = lax.axis_index("seq")
    core = lax.axis_index("head")
    position, plane = lax.rem(device, group), device // group
    wide = heads_in[0].shape[1]
    columns = weight_in[0].shape[1]
    side = keep_ref.shape[1] // columns
    inner = (plane == 1) | (plane == 2)
    lanes_of = {0: weight_in[0], 1: weight_in[1]}
    if len(weight_in) > 2:
        lanes_of[3] = weight_in[2]
        lanes_of[2] = weight_in[3:]
    for offset, source in lanes_of.items():
        owner = jnp.bitwise_xor(plane, offset)
        total = None
        for other in range(group):
            first = pl.multiple_of(place(position, other) * wide, wide)
            if offset == 2:
                weight = jnp.where(
                    inner, source[0][pl.ds(first, wide), :], source[1][pl.ds(first, wide), :]
                )
            else:
                weight = source[pl.ds(first, wide), :]
            part = dot(heads_in[other][...], weight)
            total = part if total is None else total + part
        result = total.astype(BF16)
        lanes = pl.ds(pl.multiple_of(lax.rem(owner, side) * columns, columns), columns)

        @pl.when(owner // side == core)
        def _():
            keep_ref[:, lanes] = result

        @pl.when(owner // side != core)
        def _():
            send_ref[:, lanes] = result


def project(heads, weights, planes):
    group = len(heads)
    rows = heads[0].shape[0]
    columns = weights[0].shape[1]
    shape = pltpu.VMEM((rows, columns * planes // 2), BF16)
    return pl.pallas_call(
        functools.partial(project_kernel, group),
        out_shape=(shape, shape),
        in_specs=[VMEM] * (group + len(weights)),
        out_specs=(VMEM, VMEM),
        compiler_params=PARAMS,
        name="project",
    )(*held(*heads, *weights))


def sum_kernel(group, keep_ref, other_ref, *outs):
    position = lax.rem(lax.axis_index("seq"), group)
    tokens = outs[0].shape[0]
    for offset in range(group):
        rows = pl.ds(pl.multiple_of(place(position, offset) * tokens, tokens), tokens)
        outs[offset][...] = (
            keep_ref[rows, :].astype(F32) + other_ref[rows, :].astype(F32)
        ).astype(BF16)


def sum_parts(keep, other, group):
    rows, columns = keep.shape
    return pl.pallas_call(
        functools.partial(sum_kernel, group),
        out_shape=[pltpu.VMEM((rows // group, columns), BF16)] * group,
        in_specs=[VMEM, VMEM],
        out_specs=[VMEM] * group,
        compiler_params=PARAMS,
        name="sum_parts",
    )(*held(keep, other))


def lay_kernel(group, columns, *refs):
    parts, out_ref, sems = refs[:group], refs[group], refs[group + 1]
    position = lax.rem(lax.axis_index("seq"), group)
    copies = []
    for offset in range(group):
        for index in range(parts[0].shape[1] // columns):
            first = (index * group + place(position, offset)) * columns
            copies.append(
                pltpu.make_async_copy(
                    parts[offset].at[:, index * columns : (index + 1) * columns],
                    out_ref.at[:, pl.ds(pl.multiple_of(first, columns), columns)],
                    sems.at[len(copies)],
                )
            )
    for copy in copies:
        copy.start()
    for copy in copies:
        copy.wait()


def lay_out(parts, columns):
    group = len(parts)
    rows, wide = parts[0].shape
    return pl.pallas_call(
        functools.partial(lay_kernel, group, columns),
        out_shape=jax.ShapeDtypeStruct((rows, group * wide), BF16),
        in_specs=[VMEM] * group,
        out_specs=pl.BlockSpec(memory_space=pl.ANY),
        scratch_shapes=[pltpu.SemaphoreType.DMA((group * wide // columns,))],
        compiler_params=PARAMS,
        name="lay_out",
    )(*held(*parts))


def swap(value, group, offset, count):
    pairs = [(i, (i // group) * group + ((i % group) ^ offset)) for i in range(count)]
    return lax.ppermute(value, "seq", pairs)


def per_device(queries, key_vectors, values, strengths, out_weight):
    count = lax.axis_size("seq")
    sides = lax.axis_size("head")
    heads = strengths.shape[1]
    tokens = queries.shape[0]
    width = queries.shape[1] // heads
    group = 1
    while group < 4 and heads % (2 * group) == 0 and count % (2 * group) == 0:
        group *= 2
    planes = count // group
    position = lax.axis_index("seq") % group
    mine = heads // group
    pieces = max(tokens // width, 1)
    high = lax.reduce_precision(strengths, 8, 7)
    beta = jnp.stack([high, strengths - high]).astype(BF16)
    beta = beta.reshape(4, heads, pieces, tokens // pieces)
    beta = jnp.pad(beta, ((0, 0), (0, 0), (0, 0), (0, width - tokens // pieces)))
    beta = jnp.swapaxes(beta, 1, 2).reshape(4 * pieces, heads * width)
    beta = jnp.pad(beta, ((0, beta_rows(tokens, width) - 4 * pieces), (0, 0)))
    packed = jnp.concatenate([key_vectors[0], key_vectors[1], beta], axis=0)

    keys, rests = [], []
    for offset in range(group):
        lane = jnp.bitwise_xor(position, offset) * mine * width
        key = lax.dynamic_slice_in_dim(packed, lane, mine * width, 1)
        rest = jnp.concatenate(
            [
                lax.dynamic_slice_in_dim(values, lane, mine * width, 2),
                lax.dynamic_slice_in_dim(queries, lane, mine * width, 1)[None],
            ],
            axis=0,
        )
        if offset:
            key = swap(key, group, offset, count)
            rest = swap(rest, group, offset, count)
        keys.append(key)
        rests.append(rest)

    split_out = sides == 2 and planes in (2, 4) and group > 1
    weights = [out_weight]
    if split_out:
        for offset in range(1, planes, 2):
            pairs = [(i, ((i // group) ^ offset) * group + i % group) for i in range(count)]
            weights.append(lax.ppermute(out_weight, "seq", pairs))

    inverse, table = invert(keys, mine, tokens)
    high, low, before, state, local_state = carry_state(keys, rests, inverse, table)
    local, lifted = read(keys, rests, table, high, low, before)

    def from_earlier(value, distance):
        pairs = [(i, i + distance * group) for i in range(count - distance * group)]
        return lax.ppermute(value, "seq", pairs)

    if planes <= 4:
        states = []
        for distance in range(1, planes):
            sent = state if distance + 1 < planes else local_state
            states.append(from_earlier(sent, distance))
    else:
        total = from_earlier(state, 1)
        distance = 1
        while distance < planes - 1:
            total = compose(from_earlier(total, distance), total)
            distance *= 2
        states = [total[:, :, width:]]
    if split_out and planes == 4:
        for held_weight, hops in ((weights[1], ((1, 2), (2, 1))), (weights[2], ((1, 0), (2, 3)))):
            pairs = [
                (source * group + i, target * group + i)
                for source, target in hops
                for i in range(group)
            ]
            weights.append(lax.ppermute(held_weight, "seq", pairs))

    mixed_heads = join(states, local, lifted)

    if split_out:
        gathered = [mixed_heads] + [
            swap(mixed_heads, group, offset, count) for offset in range(1, group)
        ]
        send, keep = project(gathered, weights, planes)
        other = lax.ppermute(send, "head", [(0, 1), (1, 0)])
        parts = sum_parts(keep, other, group)
        parts = [parts[0]] + [
            swap(parts[offset], group, offset, count) for offset in range(1, group)
        ]
        return lay_out(parts, out_weight.shape[1])

    if group > 1:
        position_rows = []
        for offset in range(group):
            first = jnp.bitwise_xor(position, offset) * tokens
            part = lax.dynamic_slice_in_dim(mixed_heads, first, tokens, 0)
            position_rows.append(swap(part, group, offset, count) if offset else part)
        stacked = jnp.stack(position_rows)
        order = jnp.bitwise_xor(position, jnp.arange(group))
        stacked = jnp.take(stacked, order, axis=0)
        mixed_heads = jnp.swapaxes(stacked, 0, 1).reshape(tokens, heads * width)
    partial_sums = jnp.dot(
        mixed_heads,
        lax.all_gather(out_weight, "seq", axis=1, tiled=True),
        preferred_element_type=F32,
    )
    return lax.psum_scatter(
        partial_sums.astype(BF16), "head", scatter_dimension=1, tiled=True
    )


def solution(mesh):
    return jax.shard_map(
        per_device,
        mesh=mesh,
        in_specs=(
            P("seq", "head"),
            P(None, "seq", "head"),
            P(None, "seq", "head"),
            P(None, "head", "seq"),
            P("head", "seq"),
        ),
        out_specs=P("seq", "head"),
        check_vma=False,
    )
```

```python
import functools

import jax
import jax.numpy as jnp
from jax import lax
from jax.experimental import pallas as pl
from jax.experimental.pallas import tpu as pltpu
from jax.sharding import PartitionSpec as P


CHUNK = 128
EPS = 1e-06
F32 = jnp.float32
BF16 = jnp.bfloat16


def dot(a, b):
    return jnp.dot(a, b, preferred_element_type=F32)


def dot_t(a, b):
    return lax.dot_general(a, b, (((1,), (1,)), ((), ())), preferred_element_type=F32)


def split(x):
    high = x.astype(BF16)
    return high, (x - high.astype(F32)).astype(BF16)


def product3(left, right):
    left_high, left_low = split(left)
    right_high, right_low = split(right)
    lhs = jnp.concatenate([left_high, left_low], axis=1)
    rhs = jnp.concatenate(
        [
            jnp.concatenate([right_high, right_low], axis=1),
            jnp.concatenate([right_high, jnp.zeros_like(right_low)], axis=1),
        ],
        axis=0,
    )
    wide = dot(lhs, rhs)
    width = right.shape[1]
    return wide[:, :width] + wide[:, width:]


def iota(shape, axis):
    return lax.broadcasted_iota(jnp.int32, shape, axis)


def weave(first, second):
    half = first.shape[0] // 2
    return jnp.concatenate([first[:half], second[:half], first[half:], second[half:]], axis=0)


def weave_lanes(first, second):
    half = first.shape[1] // 2
    return jnp.concatenate(
        [first[:, :half], second[:, :half], first[:, half:], second[:, half:]], axis=1
    )


def place(position, offset):
    return jnp.bitwise_xor(position, offset)


VMEM = pl.BlockSpec(memory_space=pltpu.VMEM)
PARAMS = pltpu.CompilerParams(vmem_limit_bytes=12 * 2**20)


def held(*arrays):
    return [pltpu.with_memory_space_constraint(array, pltpu.VMEM) for array in arrays]


def times(chunk):
    half = chunk // 2
    row, col = iota((chunk, chunk), 0), iota((chunk, chunk), 1)
    return 2 * lax.rem(row, half) + row // half, 2 * lax.rem(col, half) + col // half


def beta_rows(tokens, width):
    return -(-4 * max(tokens // width, 1) // 16) * 16


def invert_kernel(heads, tokens, *refs):
    key_in, (inverse_ref, table_ref, a_buf) = refs[:-3], refs[-3:]
    width = key_in[0].shape[1] // heads
    chunk = min(CHUNK, tokens)
    per_source = tokens // chunk
    chunks = len(key_in) * per_source
    pieces = max(tokens // width, 1)
    row_time, col_time = times(chunk)
    levels = chunk.bit_length() - 1

    def joins(level):
        same = (row_time >> (level + 1)) == (col_time >> (level + 1))
        return same & (((row_time >> level) & 1) == 1) & (((col_time >> level) & 1) == 0)

    def prepare(head, index):
        lanes = lanes_of(head, width)
        key_ref, first = key_in[index // per_source], (index % per_source) * chunk
        key = weave(
            key_ref[first : first + chunk, lanes],
            key_ref[tokens + first : tokens + first + chunk, lanes],
        )
        gram = dot_t(key, key)
        wide_row, wide_col = iota(gram.shape, 0), iota(gram.shape, 1)
        square = jnp.sum(jnp.where(wide_row == wide_col, gram, 0.0), axis=0, keepdims=True)
        scale_row = lax.rsqrt(square + EPS)
        halves = key_ref[2 * tokens :, lanes].astype(F32)
        piece, inside = first // width, first % width

        def strength(reflection):
            high = reflection * pieces + piece
            low = (2 + reflection) * pieces + piece
            both = halves[high : high + 1] + halves[low : low + 1]
            return both[:, inside : inside + chunk]

        beta_row = weave_lanes(strength(0), strength(1))
        both_row = beta_row * scale_row
        table = jnp.concatenate(
            [scale_row, beta_row, both_row, jnp.zeros((5, 2 * chunk), F32)], axis=0
        )
        table_ref[head, index] = table
        system = table.T[:, 2:3] * (gram * scale_row)
        for block in range(2):
            here = slice(block * chunk, (block + 1) * chunk)
            diagonal = system[here, here]
            a_buf[head, index, block] = diagonal
            inverse_ref[head, index, block] = jnp.where(
                row_time == col_time, 1.0, 0.0
            ) - jnp.where(joins(0), diagonal, 0.0)
        inverse_ref[head, index, 2] = system[chunk:, :chunk]

    def solve(units):
        for head, index in units:
            prepare(head, index)
        every = [(head, index, block) for head, index in units for block in range(2)]
        for level in range(1, levels):
            mask = joins(level)
            inner = [
                product3(jnp.where(mask, a_buf[one], 0.0), inverse_ref[one]) for one in every
            ]
            for one, value in zip(every, inner):
                known = inverse_ref[one]
                inverse_ref[one] = known - product3(known, value)
        inner = [
            product3(inverse_ref[head, index, 2], inverse_ref[head, index, 0])
            for head, index in units
        ]
        for (head, index), value in zip(units, inner):
            inverse_ref[head, index, 2] = -product3(inverse_ref[head, index, 1], value)

    if heads * chunks <= 8:
        solve([(head, index) for head in range(heads) for index in range(chunks)])
    else:

        def one_head(head, carry):
            solve([(head, index) for index in range(chunks)])
            return carry

        lax.fori_loop(0, heads, one_head, 0)


def lanes_of(head, width):
    if isinstance(head, int):
        return slice(head * width, (head + 1) * width)
    return pl.ds(pl.multiple_of(head * width, width), width)


def invert(keys, heads, tokens):
    chunk = min(CHUNK, tokens)
    chunks = len(keys) * tokens // chunk
    return pl.pallas_call(
        functools.partial(invert_kernel, heads, tokens),
        out_shape=(
            pltpu.VMEM((heads, chunks, 3, chunk, chunk), F32),
            pltpu.VMEM((heads, chunks, 8, 2 * chunk), F32),
        ),
        in_specs=[VMEM] * len(keys),
        out_specs=(VMEM, VMEM),
        scratch_shapes=[pltpu.VMEM((heads, chunks, 2, chunk, chunk), F32)],
        compiler_params=PARAMS,
        name="invert",
    )(*held(*keys))


def slot_of(group, index, per_source):
    position = lax.rem(lax.axis_index("seq"), group)
    return place(position, index // per_source) * per_source + index % per_source


def state_kernel(group, *refs):
    key_in, rest_in = refs[:group], refs[group : 2 * group]
    inverse_ref, table_ref = refs[2 * group : 2 * group + 2]
    high_ref, low_ref, step_ref, state_ref, local_ref = refs[2 * group + 2 :]
    heads, chunks, _, chunk, _ = inverse_ref.shape
    tokens = rest_in[0].shape[1]
    width = rest_in[0].shape[2] // heads
    per_source = tokens // chunk

    def one_head(head, carry):
        lanes = pl.ds(pl.multiple_of(head * width, width), width)
        for index in range(chunks):
            source, first = index // per_source, (index % per_source) * chunk
            key_ref, rest_ref = key_in[source], rest_in[source]
            key = weave(
                key_ref[first : first + chunk, lanes],
                key_ref[tokens + first : tokens + first + chunk, lanes],
            ).astype(F32)
            rows = slice(first, first + chunk)
            value = weave(rest_ref[0, rows, lanes], rest_ref[1, rows, lanes]).astype(F32)
            table = table_ref[head, index].T
            inverse = jnp.concatenate(
                [
                    jnp.concatenate(
                        [inverse_ref[head, index, 0], jnp.zeros((chunk, chunk), F32)], axis=1
                    ),
                    jnp.concatenate(
                        [inverse_ref[head, index, 2], inverse_ref[head, index, 1]], axis=1
                    ),
                ],
                axis=0,
            )
            right = jnp.concatenate([table[:, 2:3] * key, table[:, 1:2] * value], axis=1)
            high, low = split(dot3(inverse, *split(right)))
            high_ref[head, index] = high
            low_ref[head, index] = low
            step_ref[head, slot_of(group, index, per_source)] = dot3(
                (table[:, 0:1] * key).T, high, low
            )
        return carry

    lax.fori_loop(0, heads, one_head, 0)
    totals = [[step_ref[head, slot] for slot in range(chunks)] for head in range(heads)]
    while len(totals[0]) > 1:
        totals = [
            [after(one[i], one[i + 1]) for i in range(0, len(one) - 1, 2)]
            + one[len(one) - len(one) % 2 :]
            for one in totals
        ]
    for head, (total,) in enumerate(totals):
        state_ref[head] = total.astype(BF16)
        local_ref[head] = total[:, width:].astype(BF16)


def after(earlier, later):
    width = earlier.shape[0]
    return earlier + later - dot(later[:, :width].astype(BF16), earlier.astype(BF16))


def dot3(left, high, low):
    left_high, left_low = split(left)
    return dot(left_high, high) + dot(left_low, high) + dot(left_high, low)


def carry_state(keys, rests, inverse, table):
    group = len(keys)
    heads, chunks, _, chunk, _ = inverse.shape
    width = rests[0].shape[2] // heads
    solved = pltpu.VMEM((heads, chunks, 2 * chunk, 2 * width), BF16)
    return pl.pallas_call(
        functools.partial(state_kernel, group),
        out_shape=(
            solved,
            solved,
            pltpu.VMEM((heads, chunks, width, 2 * width), F32),
            pltpu.VMEM((heads, width, 2 * width), BF16),
            pltpu.VMEM((heads, width, width), BF16),
        ),
        in_specs=[VMEM] * (2 * group + 2),
        out_specs=(VMEM,) * 5,
        compiler_params=PARAMS,
        name="carry_state",
    )(*held(*keys, *rests, inverse, table))


def read_kernel(group, *refs):
    key_in, rest_in = refs[:group], refs[group : 2 * group]
    table_ref, high_ref, low_ref, step_ref, out_ref, lift_ref, before_buf = refs[2 * group :]
    heads, chunks, _, wide = table_ref.shape
    chunk = wide // 2
    half = chunk // 2
    tokens = rest_in[0].shape[1]
    width = rest_in[0].shape[2] // heads
    per_source = tokens // chunk
    token_row = iota((chunk, 2 * chunk), 0)
    token_col = iota((chunk, 2 * chunk), 1)
    token_col = (token_col // chunk) * half + lax.rem(token_col, half)
    totals = [step_ref[head, 0] for head in range(heads)]
    for head in range(heads):
        before_buf[head, 0] = jnp.zeros((width, 2 * width), BF16)
    for slot in range(1, chunks):
        for head in range(heads):
            before_buf[head, slot] = totals[head].astype(BF16)
        totals = [after(totals[head], step_ref[head, slot]) for head in range(heads)]

    def one_head(head, carry):
        lanes = pl.ds(pl.multiple_of(head * width, width), width)
        for index in range(chunks):
            source, first = index // per_source, (index % per_source) * chunk
            key_ref, rest_ref = key_in[source], rest_in[source]
            key = weave(
                key_ref[first : first + chunk, lanes],
                key_ref[tokens + first : tokens + first + chunk, lanes],
            )
            query = rest_ref[2, first : first + chunk, lanes]
            wide_query = query.astype(F32)
            scale = lax.rsqrt(jnp.sum(wide_query * wide_query, axis=1, keepdims=True) + EPS)
            scores = jnp.where(
                token_col <= token_row,
                dot_t(query, key) * (scale * table_ref[head, index, 0:1, :]),
                0.0,
            )
            applied = dot3(scores, high_ref[head, index], low_ref[head, index])
            lifted = scale * wide_query - applied[:, :width]
            slot = slot_of(group, index, per_source)
            moved = dot(lifted.astype(BF16), before_buf[head, slot])
            rows = pl.ds(pl.multiple_of(slot * chunk, chunk), chunk)
            out_ref[rows, lanes] = applied[:, width:] + moved[:, width:]
            lift_ref[rows, lanes] = (lifted - moved[:, :width]).astype(BF16)
        return carry

    lax.fori_loop(0, heads, one_head, 0)


def read(keys, rests, table, high, low, steps):
    group = len(keys)
    _, tokens, wide = rests[0].shape
    return pl.pallas_call(
        functools.partial(read_kernel, group),
        out_shape=(
            pltpu.VMEM((group * tokens, wide), F32),
            pltpu.VMEM((group * tokens, wide), BF16),
        ),
        in_specs=[VMEM] * (2 * group + 4),
        out_specs=(VMEM, VMEM),
        scratch_shapes=[pltpu.VMEM(steps.shape, BF16)],
        compiler_params=PARAMS,
        name="read",
    )(*held(*keys, *rests, table, high, low, steps))


def join_kernel(count, *refs):
    states, (local_ref, lift_ref, out_ref) = refs[:count], refs[count:]
    heads, width, _ = states[0].shape
    for head in range(heads):
        lanes = slice(head * width, (head + 1) * width)
        total = None
        for state in reversed(states):
            if total is None:
                total = state[head].astype(F32)
            else:
                step = state[head].astype(F32)
                total = (
                    total + step[:, width:] - dot(state[head, :, :width], total.astype(BF16))
                )
        out_ref[:, lanes] = (
            local_ref[:, lanes] + dot(lift_ref[:, lanes], total.astype(BF16))
        ).astype(BF16)


def join(states, local, lifted):
    return pl.pallas_call(
        functools.partial(join_kernel, len(states)),
        out_shape=pltpu.VMEM(local.shape, BF16),
        in_specs=[VMEM] * (len(states) + 2),
        out_specs=VMEM,
        compiler_params=PARAMS,
        name="join",
    )(*held(*states, local, lifted))


def compose(earlier, later):
    width = earlier.shape[1]
    moved = jnp.einsum("hab,hbc->hac", later[:, :, :width], earlier, preferred_element_type=F32)
    return (earlier.astype(F32) + later.astype(F32) - moved).astype(BF16)


def project_kernel(group, targets, *refs):
    heads_in, weight_in, (send_ref, keep_ref) = refs[:group], refs[group:-2], refs[-2:]
    device = lax.axis_index("seq")
    core = lax.axis_index("head")
    position, plane = lax.rem(device, group), device // group
    rows, wide = heads_in[0].shape
    tokens = rows // group
    columns = weight_in[0].shape[1]
    side = keep_ref.shape[1] // columns
    inner = (plane == 1) | (plane == 2)
    sources = {0: weight_in[0], 1: weight_in[1]}
    if len(weight_in) > 2:
        sources[3] = weight_in[2]
        sources[2] = weight_in[3:]

    def rows_of(source):
        firsts = [pl.multiple_of(place(position, t) * tokens, tokens) for t in targets]
        return jnp.concatenate([source[pl.ds(first, tokens), :] for first in firsts], axis=0)

    for offset, source in sources.items():
        owner = jnp.bitwise_xor(plane, offset)
        total = None
        for other in range(group):
            first = pl.multiple_of(place(position, other) * wide, wide)
            if offset == 2:
                weight = jnp.where(
                    inner, source[0][pl.ds(first, wide), :], source[1][pl.ds(first, wide), :]
                )
            else:
                weight = source[pl.ds(first, wide), :]
            part = dot(rows_of(heads_in[other]), weight)
            total = part if total is None else total + part
        result = total.astype(BF16)
        lanes = pl.ds(pl.multiple_of(lax.rem(owner, side) * columns, columns), columns)

        @pl.when(owner // side == core)
        def _():
            keep_ref[:, lanes] = result

        @pl.when(owner // side != core)
        def _():
            send_ref[:, lanes] = result


def project(heads, weights, planes, targets):
    group = len(heads)
    rows = heads[0].shape[0] // group * len(targets)
    columns = weights[0].shape[1]
    shape = pltpu.VMEM((rows, columns * planes // 2), BF16)
    return pl.pallas_call(
        functools.partial(project_kernel, group, targets),
        out_shape=(shape, shape),
        in_specs=[VMEM] * (group + len(weights)),
        out_specs=(VMEM, VMEM),
        compiler_params=PARAMS,
        name="project",
    )(*held(*heads, *weights))


def sum_kernel(keep_ref, other_ref, *outs):
    tokens = outs[0].shape[0]
    for index, out_ref in enumerate(outs):
        rows = slice(index * tokens, (index + 1) * tokens)
        out_ref[...] = (keep_ref[rows, :].astype(F32) + other_ref[rows, :].astype(F32)).astype(
            BF16
        )


def sum_parts(keep, other, count):
    rows, columns = keep.shape
    return pl.pallas_call(
        sum_kernel,
        out_shape=[pltpu.VMEM((rows // count, columns), BF16)] * count,
        in_specs=[VMEM, VMEM],
        out_specs=[VMEM] * count,
        compiler_params=PARAMS,
        name="sum_parts",
    )(*held(keep, other))


def lay_kernel(group, columns, *refs):
    parts, out_ref, sems = refs[:group], refs[group], refs[group + 1]
    position = lax.rem(lax.axis_index("seq"), group)
    copies = []
    for offset in range(group):
        for index in range(parts[0].shape[1] // columns):
            first = (index * group + place(position, offset)) * columns
            copies.append(
                pltpu.make_async_copy(
                    parts[offset].at[:, index * columns : (index + 1) * columns],
                    out_ref.at[:, pl.ds(pl.multiple_of(first, columns), columns)],
                    sems.at[len(copies)],
                )
            )
    for copy in copies:
        copy.start()
    for copy in copies:
        copy.wait()


def lay_out(parts, columns):
    group = len(parts)
    rows, wide = parts[0].shape
    return pl.pallas_call(
        functools.partial(lay_kernel, group, columns),
        out_shape=jax.ShapeDtypeStruct((rows, group * wide), BF16),
        in_specs=[VMEM] * group,
        out_specs=pl.BlockSpec(memory_space=pl.ANY),
        scratch_shapes=[pltpu.SemaphoreType.DMA((group * wide // columns,))],
        compiler_params=PARAMS,
        name="lay_out",
    )(*held(*parts))


def swap(value, group, offset, count):
    pairs = [(i, (i // group) * group + ((i % group) ^ offset)) for i in range(count)]
    return lax.ppermute(value, "seq", pairs)


def per_device(queries, key_vectors, values, strengths, out_weight):
    count = lax.axis_size("seq")
    sides = lax.axis_size("head")
    heads = strengths.shape[1]
    tokens = queries.shape[0]
    width = queries.shape[1] // heads
    group = 1
    while group < 4 and heads % (2 * group) == 0 and count % (2 * group) == 0:
        group *= 2
    planes = count // group
    position = lax.axis_index("seq") % group
    mine = heads // group
    pieces = max(tokens // width, 1)
    high = lax.reduce_precision(strengths, 8, 7)
    beta = jnp.stack([high, strengths - high]).astype(BF16)
    beta = beta.reshape(4, heads, pieces, tokens // pieces)
    beta = jnp.pad(beta, ((0, 0), (0, 0), (0, 0), (0, width - tokens // pieces)))
    beta = jnp.swapaxes(beta, 1, 2).reshape(4 * pieces, heads * width)
    beta = jnp.pad(beta, ((0, beta_rows(tokens, width) - 4 * pieces), (0, 0)))
    packed = jnp.concatenate([key_vectors[0], key_vectors[1], beta], axis=0)

    keys, rests = [], []
    for offset in range(group):
        lane = jnp.bitwise_xor(position, offset) * mine * width
        key = lax.dynamic_slice_in_dim(packed, lane, mine * width, 1)
        rest = jnp.concatenate(
            [
                lax.dynamic_slice_in_dim(values, lane, mine * width, 2),
                lax.dynamic_slice_in_dim(queries, lane, mine * width, 1)[None],
            ],
            axis=0,
        )
        if offset:
            key = swap(key, group, offset, count)
            rest = swap(rest, group, offset, count)
        keys.append(key)
        rests.append(rest)

    split_out = sides == 2 and planes in (2, 4) and group > 1
    weights = [out_weight]
    if split_out:
        for offset in range(1, planes, 2):
            pairs = [(i, ((i // group) ^ offset) * group + i % group) for i in range(count)]
            weights.append(lax.ppermute(out_weight, "seq", pairs))

    inverse, table = invert(keys, mine, tokens)
    high, low, steps, state, local_state = carry_state(keys, rests, inverse, table)
    local, lifted = read(keys, rests, table, high, low, steps)

    def from_earlier(value, distance):
        pairs = [(i, i + distance * group) for i in range(count - distance * group)]
        return lax.ppermute(value, "seq", pairs)

    if planes <= 4:
        states = []
        for distance in range(1, planes):
            sent = state if distance + 1 < planes else local_state
            states.append(from_earlier(sent, distance))
    else:
        total = from_earlier(state, 1)
        distance = 1
        while distance < planes - 1:
            total = compose(from_earlier(total, distance), total)
            distance *= 2
        states = [total[:, :, width:]]
    if split_out and planes == 4:
        for held_weight, hops in ((weights[1], ((1, 2), (2, 1))), (weights[2], ((1, 0), (2, 3)))):
            pairs = [
                (source * group + i, target * group + i)
                for source, target in hops
                for i in range(group)
            ]
            weights.append(lax.ppermute(held_weight, "seq", pairs))

    mixed_heads = join(states, local, lifted)

    if split_out:
        gathered = [mixed_heads] + [
            swap(mixed_heads, group, offset, count) for offset in range(1, group)
        ]
        order = tuple(reversed(range(group)))
        order = order[:1] + order[2:-1] + order[1:2] + order[-1:] if group > 2 else order
        parts = [None] * group
        halves = []
        for targets in (order[: group // 2], order[group // 2 :]):
            send, keep = project(gathered, weights, planes, targets)
            other = lax.ppermute(send, "head", [(0, 1), (1, 0)])
            halves.append((targets, keep, other))
        for targets, keep, other in halves:
            for offset, part in zip(targets, sum_parts(keep, other, len(targets))):
                parts[offset] = swap(part, group, offset, count) if offset else part
        return lay_out(parts, out_weight.shape[1])

    if group > 1:
        position_rows = []
        for offset in range(group):
            first = jnp.bitwise_xor(position, offset) * tokens
            part = lax.dynamic_slice_in_dim(mixed_heads, first, tokens, 0)
            position_rows.append(swap(part, group, offset, count) if offset else part)
        stacked = jnp.stack(position_rows)
        order = jnp.bitwise_xor(position, jnp.arange(group))
        stacked = jnp.take(stacked, order, axis=0)
        mixed_heads = jnp.swapaxes(stacked, 0, 1).reshape(tokens, heads * width)
    partial_sums = jnp.dot(
        mixed_heads,
        lax.all_gather(out_weight, "seq", axis=1, tiled=True),
        preferred_element_type=F32,
    )
    return lax.psum_scatter(
        partial_sums.astype(BF16), "head", scatter_dimension=1, tiled=True
    )


def solution(mesh):
    return jax.shard_map(
        per_device,
        mesh=mesh,
        in_specs=(
            P("seq", "head"),
            P(None, "seq", "head"),
            P(None, "seq", "head"),
            P(None, "head", "seq"),
            P("head", "seq"),
        ),
        out_specs=P("seq", "head"),
        check_vma=False,
    )
```

```python
import functools

import jax
import jax.numpy as jnp
from jax import lax
from jax.experimental import pallas as pl
from jax.experimental.pallas import tpu as pltpu
from jax.sharding import PartitionSpec as P


CHUNK = 128
EPS = 1e-06
F32 = jnp.float32
BF16 = jnp.bfloat16


def dot(a, b):
    return jnp.dot(a, b, preferred_element_type=F32)


def dot_t(a, b):
    return lax.dot_general(a, b, (((1,), (1,)), ((), ())), preferred_element_type=F32)


def split(x):
    high = x.astype(BF16)
    return high, (x - high.astype(F32)).astype(BF16)


def product3(left, right):
    left_high, left_low = split(left)
    right_high, right_low = split(right)
    lhs = jnp.concatenate([left_high, left_low], axis=1)
    rhs = jnp.concatenate(
        [
            jnp.concatenate([right_high, right_low], axis=1),
            jnp.concatenate([right_high, jnp.zeros_like(right_low)], axis=1),
        ],
        axis=0,
    )
    wide = dot(lhs, rhs)
    width = right.shape[1]
    return wide[:, :width] + wide[:, width:]


def iota(shape, axis):
    return lax.broadcasted_iota(jnp.int32, shape, axis)


def weave(first, second):
    half = first.shape[0] // 2
    return jnp.concatenate([first[:half], second[:half], first[half:], second[half:]], axis=0)


def weave_lanes(first, second):
    half = first.shape[1] // 2
    return jnp.concatenate(
        [first[:, :half], second[:, :half], first[:, half:], second[:, half:]], axis=1
    )


def place(position, offset):
    return jnp.bitwise_xor(position, offset)


VMEM = pl.BlockSpec(memory_space=pltpu.VMEM)
PARAMS = pltpu.CompilerParams(vmem_limit_bytes=12 * 2**20)


def held(*arrays):
    return [pltpu.with_memory_space_constraint(array, pltpu.VMEM) for array in arrays]


def times(chunk):
    half = chunk // 2
    row, col = iota((chunk, chunk), 0), iota((chunk, chunk), 1)
    return 2 * lax.rem(row, half) + row // half, 2 * lax.rem(col, half) + col // half


def beta_rows(tokens, width):
    return -(-4 * max(tokens // width, 1) // 16) * 16


def invert_kernel(heads, tokens, *refs):
    key_in, (inverse_ref, table_ref, a_buf) = refs[:-3], refs[-3:]
    width = key_in[0].shape[1] // heads
    chunk = min(CHUNK, tokens)
    per_source = tokens // chunk
    chunks = len(key_in) * per_source
    pieces = max(tokens // width, 1)
    row_time, col_time = times(chunk)
    levels = chunk.bit_length() - 1

    def joins(level):
        same = (row_time >> (level + 1)) == (col_time >> (level + 1))
        return same & (((row_time >> level) & 1) == 1) & (((col_time >> level) & 1) == 0)

    def prepare(head, index):
        lanes = lanes_of(head, width)
        key_ref, first = key_in[index // per_source], (index % per_source) * chunk
        key = woven_key(key_ref, tokens, first, chunk, lanes)
        gram = dot_t(key, key)
        wide_row, wide_col = iota(gram.shape, 0), iota(gram.shape, 1)
        square = jnp.sum(jnp.where(wide_row == wide_col, gram, 0.0), axis=0, keepdims=True)
        scale_row = lax.rsqrt(square + EPS)
        halves = key_ref[2 * tokens :, lanes].astype(F32)
        piece, inside = first // width, first % width

        def strength(reflection):
            high = reflection * pieces + piece
            low = (2 + reflection) * pieces + piece
            both = halves[high : high + 1] + halves[low : low + 1]
            return both[:, inside : inside + chunk]

        beta_row = weave_lanes(strength(0), strength(1))
        both_row = beta_row * scale_row
        table = jnp.concatenate(
            [scale_row, beta_row, both_row, jnp.zeros((5, 2 * chunk), F32)], axis=0
        )
        table_ref[head, index] = table
        system = table.T[:, 2:3] * (gram * scale_row)
        for block in range(2):
            here = slice(block * chunk, (block + 1) * chunk)
            diagonal = system[here, here]
            a_buf[head, index, block] = diagonal
            inverse_ref[head, index, block] = jnp.where(
                row_time == col_time, 1.0, 0.0
            ) - jnp.where(joins(0), diagonal, 0.0)
        inverse_ref[head, index, 2] = system[chunk:, :chunk]

    def solve(units):
        for head, index in units:
            prepare(head, index)
        every = [(head, index, block) for head, index in units for block in range(2)]
        for level in range(1, levels):
            mask = joins(level)
            inner = [
                product3(jnp.where(mask, a_buf[one], 0.0), inverse_ref[one]) for one in every
            ]
            for one, value in zip(every, inner):
                known = inverse_ref[one]
                inverse_ref[one] = known - product3(known, value)
        inner = [
            product3(inverse_ref[head, index, 2], inverse_ref[head, index, 0])
            for head, index in units
        ]
        for (head, index), value in zip(units, inner):
            inverse_ref[head, index, 2] = -product3(inverse_ref[head, index, 1], value)

    every_unit(heads, chunks, solve)


def lanes_of(head, width):
    if isinstance(head, int):
        return slice(head * width, (head + 1) * width)
    return pl.ds(pl.multiple_of(head * width, width), width)


def invert(keys, heads, tokens):
    chunk = min(CHUNK, tokens)
    chunks = len(keys) * tokens // chunk
    return pl.pallas_call(
        functools.partial(invert_kernel, heads, tokens),
        out_shape=(
            pltpu.VMEM((heads, chunks, 3, chunk, chunk), F32),
            pltpu.VMEM((heads, chunks, 8, 2 * chunk), F32),
        ),
        in_specs=[VMEM] * len(keys),
        out_specs=(VMEM, VMEM),
        scratch_shapes=[pltpu.VMEM((heads, chunks, 2, chunk, chunk), F32)],
        compiler_params=PARAMS,
        name="invert",
    )(*held(*keys))


def slot_of(group, index, per_source):
    position = lax.rem(lax.axis_index("seq"), group)
    return place(position, index // per_source) * per_source + index % per_source


def every_unit(heads, chunks, body):
    if heads * chunks <= 8:
        body([(head, index) for head in range(heads) for index in range(chunks)])
    else:

        def one_head(head, carry):
            body([(head, index) for index in range(chunks)])
            return carry

        lax.fori_loop(0, heads, one_head, 0)


def woven_key(key_ref, tokens, first, chunk, lanes):
    return weave(
        key_ref[first : first + chunk, lanes],
        key_ref[tokens + first : tokens + first + chunk, lanes],
    )


def state_kernel(group, parts, *refs):
    key_in, rest_in = refs[:group], refs[group : 2 * group]
    inverse_in = refs[2 * group : 2 * group + parts]
    table_in = refs[2 * group + parts : 2 * group + 2 * parts]
    high_ref, low_ref, step_ref, state_ref, local_ref = refs[2 * group + 2 * parts :]
    heads, per_part, _, chunk, _ = inverse_in[0].shape
    chunks = parts * per_part
    tokens = rest_in[0].shape[1]
    width = rest_in[0].shape[2] // heads
    per_source = tokens // chunk

    def solve(units):
        for head, index in units:
            lanes = lanes_of(head, width)
            part, inside = index // per_part, index % per_part
            source, first = index // per_source, (index % per_source) * chunk
            key_ref, rest_ref = key_in[source], rest_in[source]
            key = woven_key(key_ref, tokens, first, chunk, lanes).astype(F32)
            rows = slice(first, first + chunk)
            value = weave(rest_ref[0, rows, lanes], rest_ref[1, rows, lanes]).astype(F32)
            table = table_in[part][head, inside].T
            inverse = jnp.concatenate(
                [
                    jnp.concatenate(
                        [inverse_in[part][head, inside, 0], jnp.zeros((chunk, chunk), F32)],
                        axis=1,
                    ),
                    jnp.concatenate(
                        [inverse_in[part][head, inside, 2], inverse_in[part][head, inside, 1]],
                        axis=1,
                    ),
                ],
                axis=0,
            )
            right = jnp.concatenate([table[:, 2:3] * key, table[:, 1:2] * value], axis=1)
            high, low = split(table[:, 0:1] * dot3(inverse, *split(right)))
            high_ref[head, index] = high
            low_ref[head, index] = low
        for head, index in units:
            source, first = index // per_source, (index % per_source) * chunk
            turned = woven_key(key_in[source], tokens, first, chunk, lanes_of(head, width)).T
            step_ref[head, slot_of(group, index, per_source)] = dot(
                turned, high_ref[head, index]
            ) + dot(turned, low_ref[head, index])

    every_unit(heads, chunks, solve)
    totals = [[step_ref[head, slot] for slot in range(chunks)] for head in range(heads)]
    while len(totals[0]) > 1:
        totals = [
            [after(one[i], one[i + 1]) for i in range(0, len(one) - 1, 2)]
            + one[len(one) - len(one) % 2 :]
            for one in totals
        ]
    for head, (total,) in enumerate(totals):
        state_ref[head] = total.astype(BF16)
        local_ref[head] = total[:, width:].astype(BF16)


def after(earlier, later):
    width = earlier.shape[0]
    return earlier + later - dot(later[:, :width].astype(BF16), earlier.astype(BF16))


def dot3(left, high, low):
    left_high, left_low = split(left)
    return dot(left_high, high) + dot(left_low, high) + dot(left_high, low)


def carry_state(keys, rests, inverses, tables):
    group, parts = len(keys), len(inverses)
    heads, per_part, _, chunk, _ = inverses[0].shape
    chunks = parts * per_part
    width = rests[0].shape[2] // heads
    solved = pltpu.VMEM((heads, chunks, 2 * chunk, 2 * width), BF16)
    return pl.pallas_call(
        functools.partial(state_kernel, group, parts),
        out_shape=(
            solved,
            solved,
            pltpu.VMEM((heads, chunks, width, 2 * width), F32),
            pltpu.VMEM((heads, width, 2 * width), BF16),
            pltpu.VMEM((heads, width, width), BF16),
        ),
        in_specs=[VMEM] * (2 * group + 2 * parts),
        out_specs=(VMEM,) * 5,
        compiler_params=PARAMS,
        name="carry_state",
    )(*held(*keys, *rests, *inverses, *tables))


def read_kernel(group, *refs):
    key_in, rest_in = refs[:group], refs[group : 2 * group]
    high_ref, low_ref, step_ref, out_ref, lift_ref, before_buf = refs[2 * group :]
    heads, chunks, wide, _ = high_ref.shape
    chunk = wide // 2
    half = chunk // 2
    tokens = rest_in[0].shape[1]
    width = rest_in[0].shape[2] // heads
    per_source = tokens // chunk
    token_row = iota((chunk, 2 * chunk), 0)
    token_col = iota((chunk, 2 * chunk), 1)
    token_col = (token_col // chunk) * half + lax.rem(token_col, half)
    totals = [step_ref[head, 0] for head in range(heads)]
    for head in range(heads):
        before_buf[head, 0] = jnp.zeros((width, 2 * width), BF16)
    for slot in range(1, chunks):
        for head in range(heads):
            before_buf[head, slot] = totals[head].astype(BF16)
        totals = [after(totals[head], step_ref[head, slot]) for head in range(heads)]

    def answer(units):
        for head, index in units:
            lanes = lanes_of(head, width)
            source, first = index // per_source, (index % per_source) * chunk
            key = woven_key(key_in[source], tokens, first, chunk, lanes)
            query = rest_in[source][2, first : first + chunk, lanes]
            wide_query = query.astype(F32)
            scale = lax.rsqrt(jnp.sum(wide_query * wide_query, axis=1, keepdims=True) + EPS)
            scores = jnp.where(token_col <= token_row, dot_t(query, key) * scale, 0.0)
            applied = dot3(scores, high_ref[head, index], low_ref[head, index])
            lifted = scale * wide_query - applied[:, :width]
            slot = slot_of(group, index, per_source)
            moved = dot(lifted.astype(BF16), before_buf[head, slot])
            rows = pl.ds(pl.multiple_of(slot * chunk, chunk), chunk)
            out_ref[rows, lanes] = applied[:, width:] + moved[:, width:]
            lift_ref[rows, lanes] = (lifted - moved[:, :width]).astype(BF16)

    every_unit(heads, chunks, answer)


def read(keys, rests, high, low, steps):
    group = len(keys)
    _, tokens, wide = rests[0].shape
    return pl.pallas_call(
        functools.partial(read_kernel, group),
        out_shape=(
            pltpu.VMEM((group * tokens, wide), F32),
            pltpu.VMEM((group * tokens, wide), BF16),
        ),
        in_specs=[VMEM] * (2 * group + 3),
        out_specs=(VMEM, VMEM),
        scratch_shapes=[pltpu.VMEM(steps.shape, BF16)],
        compiler_params=PARAMS,
        name="read",
    )(*held(*keys, *rests, high, low, steps))


def join_kernel(count, *refs):
    states, (local_ref, lift_ref, out_ref) = refs[:count], refs[count:]
    heads, width, _ = states[0].shape
    for head in range(heads):
        lanes = slice(head * width, (head + 1) * width)
        total = None
        for state in reversed(states):
            if total is None:
                total = state[head].astype(F32)
            else:
                step = state[head].astype(F32)
                total = (
                    total + step[:, width:] - dot(state[head, :, :width], total.astype(BF16))
                )
        out_ref[:, lanes] = (
            local_ref[:, lanes] + dot(lift_ref[:, lanes], total.astype(BF16))
        ).astype(BF16)


def join(states, local, lifted):
    return pl.pallas_call(
        functools.partial(join_kernel, len(states)),
        out_shape=pltpu.VMEM(local.shape, BF16),
        in_specs=[VMEM] * (len(states) + 2),
        out_specs=VMEM,
        compiler_params=PARAMS,
        name="join",
    )(*held(*states, local, lifted))


def compose(earlier, later):
    width = earlier.shape[1]
    moved = jnp.einsum("hab,hbc->hac", later[:, :, :width], earlier, preferred_element_type=F32)
    return (earlier.astype(F32) + later.astype(F32) - moved).astype(BF16)


def weight_rows(weights, offset, inner, first, count):
    rows = pl.ds(first, count)
    if offset == 2:
        return jnp.where(inner, weights[3][rows, :], weights[4][rows, :])
    return weights[{0: 0, 1: 1, 3: 2}[offset]][rows, :]


def where_am_i(group):
    device = lax.axis_index("seq")
    return lax.rem(device, group), device // group


def target_rows(source, group, targets):
    position, _ = where_am_i(group)
    tokens = source.shape[0] // group
    firsts = [pl.multiple_of(place(position, t) * tokens, tokens) for t in targets]
    return jnp.concatenate([source[pl.ds(first, tokens), :] for first in firsts], axis=0)


def begin_kernel(group, halves, early, *refs):
    heads_in, weight_in, totals = refs[: len(early[0])], refs[len(early[0]) : -2], refs[-2:]
    position, _ = where_am_i(group)
    wide = heads_in[0].shape[1]
    columns = weight_in[0].shape[1]
    for targets, total_ref in zip(halves, totals):
        for number, offset in enumerate(early[1]):
            total = None
            for member, source in zip(early[0], heads_in):
                first = pl.multiple_of(place(position, member) * wide, wide)
                part = dot(
                    target_rows(source, group, targets),
                    weight_rows(weight_in, offset, None, first, wide),
                )
                total = part if total is None else total + part
            total_ref[:, number * columns : (number + 1) * columns] = total


def project_kernel(group, targets, early, offsets, *refs):
    heads_in, weight_in = refs[:group], refs[group:-3]
    total_ref, send_ref, keep_ref = refs[-3:]
    core = lax.axis_index("head")
    position, plane = where_am_i(group)
    wide = heads_in[0].shape[1]
    columns = weight_in[0].shape[1]
    side = keep_ref.shape[1] // columns
    inner = (plane == 1) | (plane == 2)
    for offset in offsets:
        owner = jnp.bitwise_xor(plane, offset)
        total = None
        members = range(group)
        if offset in early[1]:
            number = early[1].index(offset)
            members = [member for member in members if member not in early[0]]
        for member in members:
            first = pl.multiple_of(place(position, member) * wide, wide)
            part = dot(
                target_rows(heads_in[member], group, targets),
                weight_rows(weight_in, offset, inner, first, wide),
            )
            total = part if total is None else total + part
        if offset in early[1]:
            total = total + total_ref[:, number * columns : (number + 1) * columns]
        result = total.astype(BF16)
        lanes = pl.ds(pl.multiple_of(lax.rem(owner, side) * columns, columns), columns)

        @pl.when(owner // side == core)
        def _():
            keep_ref[:, lanes] = result

        @pl.when(owner // side != core)
        def _():
            send_ref[:, lanes] = result


def begin_projection(heads, weights, halves, early):
    group = len(heads)
    tokens = heads[0].shape[0] // group
    columns = weights[0].shape[1]
    here = [heads[member] for member in early[0]] + list(weights[: len(early[1])])
    return pl.pallas_call(
        functools.partial(begin_kernel, group, halves, early),
        out_shape=[
            pltpu.VMEM((tokens * len(targets), columns * len(early[1])), F32)
            for targets in halves
        ],
        in_specs=[VMEM] * len(here),
        out_specs=[VMEM] * 2,
        compiler_params=PARAMS,
        name="begin_projection",
    )(*held(*here))


def project(heads, weights, planes, targets, early, total):
    group = len(heads)
    rows = heads[0].shape[0] // group * len(targets)
    columns = weights[0].shape[1]
    offsets = (0, 1, 3, 2) if planes == 4 else (0, 1)
    shape = pltpu.VMEM((rows, columns * planes // 2), BF16)
    return pl.pallas_call(
        functools.partial(project_kernel, group, targets, early, offsets),
        out_shape=(shape, shape),
        in_specs=[VMEM] * (group + len(weights) + 1),
        out_specs=(VMEM, VMEM),
        compiler_params=PARAMS,
        name="project",
    )(*held(*heads, *weights, total))


def sum_kernel(keep_ref, other_ref, *outs):
    tokens = outs[0].shape[0]
    for index, out_ref in enumerate(outs):
        rows = slice(index * tokens, (index + 1) * tokens)
        out_ref[...] = (keep_ref[rows, :].astype(F32) + other_ref[rows, :].astype(F32)).astype(
            BF16
        )


def sum_parts(keep, other, count):
    rows, columns = keep.shape
    return pl.pallas_call(
        sum_kernel,
        out_shape=[pltpu.VMEM((rows // count, columns), BF16)] * count,
        in_specs=[VMEM, VMEM],
        out_specs=[VMEM] * count,
        compiler_params=PARAMS,
        name="sum_parts",
    )(*held(keep, other))


def lay_kernel(group, columns, *refs):
    parts, out_ref, sems = refs[:group], refs[group], refs[group + 1]
    position = lax.rem(lax.axis_index("seq"), group)
    copies = []
    for offset in range(group):
        for index in range(parts[0].shape[1] // columns):
            first = (index * group + place(position, offset)) * columns
            copies.append(
                pltpu.make_async_copy(
                    parts[offset].at[:, index * columns : (index + 1) * columns],
                    out_ref.at[:, pl.ds(pl.multiple_of(first, columns), columns)],
                    sems.at[len(copies)],
                )
            )
    for copy in copies:
        copy.start()
    for copy in copies:
        copy.wait()


def lay_out(parts, columns):
    group = len(parts)
    rows, wide = parts[0].shape
    return pl.pallas_call(
        functools.partial(lay_kernel, group, columns),
        out_shape=jax.ShapeDtypeStruct((rows, group * wide), BF16),
        in_specs=[VMEM] * group,
        out_specs=pl.BlockSpec(memory_space=pl.ANY),
        scratch_shapes=[pltpu.SemaphoreType.DMA((group * wide // columns,))],
        compiler_params=PARAMS,
        name="lay_out",
    )(*held(*parts))


def swap(value, group, offset, count):
    pairs = [(i, (i // group) * group + ((i % group) ^ offset)) for i in range(count)]
    return lax.ppermute(value, "seq", pairs)


def per_device(queries, key_vectors, values, strengths, out_weight):
    count = lax.axis_size("seq")
    sides = lax.axis_size("head")
    heads = strengths.shape[1]
    tokens = queries.shape[0]
    width = queries.shape[1] // heads
    group = 1
    while group < 4 and heads % (2 * group) == 0 and count % (2 * group) == 0:
        group *= 2
    planes = count // group
    position = lax.axis_index("seq") % group
    mine = heads // group
    pieces = max(tokens // width, 1)
    high = lax.reduce_precision(strengths, 8, 7)
    beta = jnp.stack([high, strengths - high]).astype(BF16)
    beta = beta.reshape(4, heads, pieces, tokens // pieces)
    beta = jnp.pad(beta, ((0, 0), (0, 0), (0, 0), (0, width - tokens // pieces)))
    beta = jnp.swapaxes(beta, 1, 2).reshape(4 * pieces, heads * width)
    beta = jnp.pad(beta, ((0, beta_rows(tokens, width) - 4 * pieces), (0, 0)))
    packed = jnp.concatenate([key_vectors[0], key_vectors[1], beta], axis=0)

    keys, rests = [], []
    for offset in range(group):
        lane = jnp.bitwise_xor(position, offset) * mine * width
        key = lax.dynamic_slice_in_dim(packed, lane, mine * width, 1)
        rest = jnp.concatenate(
            [
                lax.dynamic_slice_in_dim(values, lane, mine * width, 2),
                lax.dynamic_slice_in_dim(queries, lane, mine * width, 1)[None],
            ],
            axis=0,
        )
        if offset:
            key = swap(key, group, offset, count)
            rest = swap(rest, group, offset, count)
        keys.append(key)
        rests.append(rest)

    split_out = sides == 2 and planes in (2, 4) and group > 1
    weights = [out_weight]
    if split_out:
        for offset in range(1, planes, 2):
            pairs = [(i, ((i // group) ^ offset) * group + i % group) for i in range(count)]
            weights.append(lax.ppermute(out_weight, "seq", pairs))

    near = max(group // 2, 1)
    solved = []
    for part in (keys[:near], keys[near:]):
        if part:
            solved.append(invert(part, mine, tokens))
    inverses, tables = zip(*solved)
    high, low, steps, state, local_state = carry_state(keys, rests, inverses, tables)
    local, lifted = read(keys, rests, high, low, steps)

    def from_earlier(value, distance):
        pairs = [(i, i + distance * group) for i in range(count - distance * group)]
        return lax.ppermute(value, "seq", pairs)

    if planes <= 4:
        states = []
        for distance in range(1, planes):
            sent = state if distance + 1 < planes else local_state
            states.append(from_earlier(sent, distance))
    else:
        total = from_earlier(state, 1)
        distance = 1
        while distance < planes - 1:
            total = compose(from_earlier(total, distance), total)
            distance *= 2
        states = [total[:, :, width:]]
    if split_out and planes == 4:
        for held_weight, hops in ((weights[1], ((1, 2), (2, 1))), (weights[2], ((1, 0), (2, 3)))):
            pairs = [
                (source * group + i, target * group + i)
                for source, target in hops
                for i in range(group)
            ]
            weights.append(lax.ppermute(held_weight, "seq", pairs))

    mixed_heads = join(states, local, lifted)

    if split_out:
        order = tuple(reversed(range(group)))
        order = order[:1] + order[2:-1] + order[1:2] + order[-1:] if group > 2 else order
        row_halves = (order[: group // 2], order[group // 2 :])
        early = (tuple(range(group - 1)), (0, 1, 3) if planes == 4 else (0, 1))
        parts = [None] * group
        gathered = [mixed_heads]
        for offset in range(1, group):
            gathered.append(swap(mixed_heads, group, offset, count))
        totals = begin_projection(gathered, weights, row_halves, early)
        halves = []
        for targets, total in zip(row_halves, totals):
            send, keep = project(gathered, weights, planes, targets, early, total)
            other = lax.ppermute(send, "head", [(0, 1), (1, 0)])
            halves.append((targets, keep, other))
        for targets, keep, other in halves:
            for offset, part in zip(targets, sum_parts(keep, other, len(targets))):
                parts[offset] = swap(part, group, offset, count) if offset else part
        return lay_out(parts, out_weight.shape[1])

    if group > 1:
        position_rows = []
        for offset in range(group):
            first = jnp.bitwise_xor(position, offset) * tokens
            part = lax.dynamic_slice_in_dim(mixed_heads, first, tokens, 0)
            position_rows.append(swap(part, group, offset, count) if offset else part)
        stacked = jnp.stack(position_rows)
        order = jnp.bitwise_xor(position, jnp.arange(group))
        stacked = jnp.take(stacked, order, axis=0)
        mixed_heads = jnp.swapaxes(stacked, 0, 1).reshape(tokens, heads * width)
    partial_sums = jnp.dot(
        mixed_heads,
        lax.all_gather(out_weight, "seq", axis=1, tiled=True),
        preferred_element_type=F32,
    )
    return lax.psum_scatter(
        partial_sums.astype(BF16), "head", scatter_dimension=1, tiled=True
    )


def solution(mesh):
    return jax.shard_map(
        per_device,
        mesh=mesh,
        in_specs=(
            P("seq", "head"),
            P(None, "seq", "head"),
            P(None, "seq", "head"),
            P(None, "head", "seq"),
            P("head", "seq"),
        ),
        out_specs=P("seq", "head"),
        check_vma=False,
    )
```

```python
import functools

import jax
import jax.numpy as jnp
from jax import lax
from jax.experimental import pallas as pl
from jax.experimental.pallas import tpu as pltpu
from jax.sharding import PartitionSpec as P


CHUNK = 128
EPS = 1e-06
F32 = jnp.float32
BF16 = jnp.bfloat16


def dot(a, b):
    return jnp.dot(a, b, preferred_element_type=F32)


def dot_t(a, b):
    return lax.dot_general(a, b, (((1,), (1,)), ((), ())), preferred_element_type=F32)


def split(x):
    high = x.astype(BF16)
    return high, (x - high.astype(F32)).astype(BF16)


def product3(left, right):
    left_high, left_low = split(left)
    right_high, right_low = split(right)
    lhs = jnp.concatenate([left_high, left_low], axis=1)
    rhs = jnp.concatenate(
        [
            jnp.concatenate([right_high, right_low], axis=1),
            jnp.concatenate([right_high, jnp.zeros_like(right_low)], axis=1),
        ],
        axis=0,
    )
    wide = dot(lhs, rhs)
    width = right.shape[1]
    return wide[:, :width] + wide[:, width:]


def iota(shape, axis):
    return lax.broadcasted_iota(jnp.int32, shape, axis)


def weave(first, second):
    half = first.shape[0] // 2
    return jnp.concatenate([first[:half], second[:half], first[half:], second[half:]], axis=0)


def weave_lanes(first, second):
    half = first.shape[1] // 2
    return jnp.concatenate(
        [first[:, :half], second[:, :half], first[:, half:], second[:, half:]], axis=1
    )


def place(position, offset):
    return jnp.bitwise_xor(position, offset)


VMEM = pl.BlockSpec(memory_space=pltpu.VMEM)
PARAMS = pltpu.CompilerParams(vmem_limit_bytes=12 * 2**20)


def held(*arrays):
    return [pltpu.with_memory_space_constraint(array, pltpu.VMEM) for array in arrays]


def times(chunk):
    half = chunk // 2
    row, col = iota((chunk, chunk), 0), iota((chunk, chunk), 1)
    return 2 * lax.rem(row, half) + row // half, 2 * lax.rem(col, half) + col // half


def beta_rows(tokens, width):
    return -(-4 * max(tokens // width, 1) // 16) * 16


def pack_kernel(group, key_ref, beta_ref, *outs):
    _, heads, tokens = beta_ref.shape
    mine = heads // group
    wide = outs[0].shape[1]
    width = wide // mine
    pieces = max(tokens // width, 1)
    inside = tokens // pieces
    position, _ = where_am_i(group)
    for offset, out_ref in enumerate(outs):
        member = place(position, offset)
        lanes = pl.ds(pl.multiple_of(member * wide, wide), wide)
        for reflection in range(2):
            out_ref[reflection * tokens : (reflection + 1) * tokens, :] = key_ref[
                reflection, :, lanes
            ]
        rows = []
        for reflection in range(2):
            for piece in range(pieces):
                cuts = []
                for head in range(mine):
                    cut = beta_ref[reflection, pl.ds(member * mine + head, 1), :]
                    cuts.append(cut[:, piece * inside : (piece + 1) * inside])
                    if inside < width:
                        cuts.append(jnp.zeros((1, width - inside), F32))
                rows.append(jnp.concatenate(cuts, axis=1) if len(cuts) > 1 else cuts[0])
        both = jnp.concatenate(rows, axis=0)
        high = both.astype(BF16).astype(F32)
        spare = jnp.zeros((out_ref.shape[0] - 2 * tokens - 2 * len(rows), wide), F32)
        out_ref[2 * tokens :, :] = jnp.concatenate([high, both - high, spare], axis=0).astype(BF16)


def pack_keys(key_vectors, strengths, group):
    _, tokens, wide = key_vectors.shape
    width = wide // strengths.shape[1]
    shape = (2 * tokens + beta_rows(tokens, width), wide // group)
    return pl.pallas_call(
        functools.partial(pack_kernel, group),
        out_shape=[pltpu.VMEM(shape, BF16)] * group,
        in_specs=[VMEM] * 2,
        out_specs=[VMEM] * group,
        compiler_params=PARAMS,
        name="pack_keys",
    )(*held(key_vectors, strengths))


def invert_kernel(heads, tokens, *refs):
    key_in, (inverse_ref, table_ref, a_buf) = refs[:-3], refs[-3:]
    width = key_in[0].shape[1] // heads
    chunk = min(CHUNK, tokens)
    per_source = tokens // chunk
    chunks = len(key_in) * per_source
    pieces = max(tokens // width, 1)
    row_time, col_time = times(chunk)
    levels = chunk.bit_length() - 1

    def joins(level):
        same = (row_time >> (level + 1)) == (col_time >> (level + 1))
        return same & (((row_time >> level) & 1) == 1) & (((col_time >> level) & 1) == 0)

    def prepare(head, index):
        lanes = lanes_of(head, width)
        key_ref, first = key_in[index // per_source], (index % per_source) * chunk
        key = woven_key(key_ref, tokens, first, chunk, lanes)
        gram = dot_t(key, key)
        wide_row, wide_col = iota(gram.shape, 0), iota(gram.shape, 1)
        square = jnp.sum(jnp.where(wide_row == wide_col, gram, 0.0), axis=0, keepdims=True)
        scale_row = lax.rsqrt(square + EPS)
        halves = key_ref[2 * tokens :, lanes].astype(F32)
        piece, inside = first // width, first % width

        def strength(reflection):
            high = reflection * pieces + piece
            low = (2 + reflection) * pieces + piece
            both = halves[high : high + 1] + halves[low : low + 1]
            return both[:, inside : inside + chunk]

        beta_row = weave_lanes(strength(0), strength(1))
        both_row = beta_row * scale_row
        table = jnp.concatenate(
            [scale_row, beta_row, both_row, jnp.zeros((5, 2 * chunk), F32)], axis=0
        )
        table_ref[head, index] = table
        system = table.T[:, 2:3] * (gram * scale_row)
        for block in range(2):
            here = slice(block * chunk, (block + 1) * chunk)
            diagonal = system[here, here]
            a_buf[head, index, block] = diagonal
            inverse_ref[head, index, block] = jnp.where(
                row_time == col_time, 1.0, 0.0
            ) - jnp.where(joins(0), diagonal, 0.0)
        inverse_ref[head, index, 2] = system[chunk:, :chunk]

    def solve(units):
        for head, index in units:
            prepare(head, index)
        every = [(head, index, block) for head, index in units for block in range(2)]
        for level in range(1, levels):
            mask = joins(level)
            inner = [
                product3(jnp.where(mask, a_buf[one], 0.0), inverse_ref[one]) for one in every
            ]
            for one, value in zip(every, inner):
                known = inverse_ref[one]
                inverse_ref[one] = known - product3(known, value)
        inner = [
            product3(inverse_ref[head, index, 2], inverse_ref[head, index, 0])
            for head, index in units
        ]
        for (head, index), value in zip(units, inner):
            inverse_ref[head, index, 2] = -product3(inverse_ref[head, index, 1], value)

    every_unit(heads, chunks, solve)


def lanes_of(head, width):
    if isinstance(head, int):
        return slice(head * width, (head + 1) * width)
    return pl.ds(pl.multiple_of(head * width, width), width)


def invert(keys, heads, tokens):
    chunk = min(CHUNK, tokens)
    chunks = len(keys) * tokens // chunk
    return pl.pallas_call(
        functools.partial(invert_kernel, heads, tokens),
        out_shape=(
            pltpu.VMEM((heads, chunks, 3, chunk, chunk), F32),
            pltpu.VMEM((heads, chunks, 8, 2 * chunk), F32),
        ),
        in_specs=[VMEM] * len(keys),
        out_specs=(VMEM, VMEM),
        scratch_shapes=[pltpu.VMEM((heads, chunks, 2, chunk, chunk), F32)],
        compiler_params=PARAMS,
        name="invert",
    )(*held(*keys))


def slot_of(group, index, per_source):
    position = lax.rem(lax.axis_index("seq"), group)
    return place(position, index // per_source) * per_source + index % per_source


def every_unit(heads, chunks, body):
    if heads * chunks <= 8:
        body([(head, index) for head in range(heads) for index in range(chunks)])
    else:

        def one_head(head, carry):
            body([(head, index) for index in range(chunks)])
            return carry

        lax.fori_loop(0, heads, one_head, 0)


def woven_key(key_ref, tokens, first, chunk, lanes):
    return weave(
        key_ref[first : first + chunk, lanes],
        key_ref[tokens + first : tokens + first + chunk, lanes],
    )


def state_kernel(group, parts, *refs):
    key_in, rest_in = refs[:group], refs[group : 2 * group]
    inverse_in = refs[2 * group : 2 * group + parts]
    table_in = refs[2 * group + parts : 2 * group + 2 * parts]
    high_ref, low_ref, step_ref, state_ref, local_ref = refs[2 * group + 2 * parts :]
    heads, per_part, _, chunk, _ = inverse_in[0].shape
    chunks = parts * per_part
    tokens = rest_in[0].shape[1]
    width = rest_in[0].shape[2] // heads
    per_source = tokens // chunk

    def solve(units):
        for head, index in units:
            lanes = lanes_of(head, width)
            part, inside = index // per_part, index % per_part
            source, first = index // per_source, (index % per_source) * chunk
            key_ref, rest_ref = key_in[source], rest_in[source]
            key = woven_key(key_ref, tokens, first, chunk, lanes).astype(F32)
            rows = slice(first, first + chunk)
            value = weave(rest_ref[0, rows, lanes], rest_ref[1, rows, lanes]).astype(F32)
            table = table_in[part][head, inside].T
            inverse = jnp.concatenate(
                [
                    jnp.concatenate(
                        [inverse_in[part][head, inside, 0], jnp.zeros((chunk, chunk), F32)],
                        axis=1,
                    ),
                    jnp.concatenate(
                        [inverse_in[part][head, inside, 2], inverse_in[part][head, inside, 1]],
                        axis=1,
                    ),
                ],
                axis=0,
            )
            right = jnp.concatenate([table[:, 2:3] * key, table[:, 1:2] * value], axis=1)
            high, low = split(table[:, 0:1] * dot3(inverse, *split(right)))
            high_ref[head, index] = high
            low_ref[head, index] = low
        for head, index in units:
            source, first = index // per_source, (index % per_source) * chunk
            turned = woven_key(key_in[source], tokens, first, chunk, lanes_of(head, width)).T
            step_ref[head, slot_of(group, index, per_source)] = dot(
                turned, high_ref[head, index]
            ) + dot(turned, low_ref[head, index])

    every_unit(heads, chunks, solve)
    totals = [[step_ref[head, slot] for slot in range(chunks)] for head in range(heads)]
    while len(totals[0]) > 1:
        totals = [
            [after(one[i], one[i + 1]) for i in range(0, len(one) - 1, 2)]
            + one[len(one) - len(one) % 2 :]
            for one in totals
        ]
    for head, (total,) in enumerate(totals):
        state_ref[head] = total.astype(BF16)
        local_ref[head] = total[:, width:].astype(BF16)


def after(earlier, later):
    width = earlier.shape[0]
    return earlier + later - dot(later[:, :width].astype(BF16), earlier.astype(BF16))


def dot3(left, high, low):
    left_high, left_low = split(left)
    return dot(left_high, high) + dot(left_low, high) + dot(left_high, low)


def carry_state(keys, rests, inverses, tables):
    group, parts = len(keys), len(inverses)
    heads, per_part, _, chunk, _ = inverses[0].shape
    chunks = parts * per_part
    width = rests[0].shape[2] // heads
    solved = pltpu.VMEM((heads, chunks, 2 * chunk, 2 * width), BF16)
    return pl.pallas_call(
        functools.partial(state_kernel, group, parts),
        out_shape=(
            solved,
            solved,
            pltpu.VMEM((heads, chunks, width, 2 * width), F32),
            pltpu.VMEM((heads, width, 2 * width), BF16),
            pltpu.VMEM((heads, width, width), BF16),
        ),
        in_specs=[VMEM] * (2 * group + 2 * parts),
        out_specs=(VMEM,) * 5,
        compiler_params=PARAMS,
        name="carry_state",
    )(*held(*keys, *rests, *inverses, *tables))


def read_kernel(group, *refs):
    key_in, rest_in = refs[:group], refs[group : 2 * group]
    high_ref, low_ref, step_ref, out_ref, lift_ref, before_buf = refs[2 * group :]
    heads, chunks, wide, _ = high_ref.shape
    chunk = wide // 2
    half = chunk // 2
    tokens = rest_in[0].shape[0]
    width = rest_in[0].shape[1] // heads
    per_source = tokens // chunk
    token_row = iota((chunk, 2 * chunk), 0)
    token_col = iota((chunk, 2 * chunk), 1)
    token_col = (token_col // chunk) * half + lax.rem(token_col, half)
    totals = [step_ref[head, 0] for head in range(heads)]
    for head in range(heads):
        before_buf[head, 0] = jnp.zeros((width, 2 * width), BF16)
    for slot in range(1, chunks):
        for head in range(heads):
            before_buf[head, slot] = totals[head].astype(BF16)
        totals = [after(totals[head], step_ref[head, slot]) for head in range(heads)]

    def answer(units):
        for head, index in units:
            lanes = lanes_of(head, width)
            source, first = index // per_source, (index % per_source) * chunk
            key = woven_key(key_in[source], tokens, first, chunk, lanes)
            query = rest_in[source][first : first + chunk, lanes]
            wide_query = query.astype(F32)
            scale = lax.rsqrt(jnp.sum(wide_query * wide_query, axis=1, keepdims=True) + EPS)
            scores = jnp.where(token_col <= token_row, dot_t(query, key) * scale, 0.0)
            applied = dot3(scores, high_ref[head, index], low_ref[head, index])
            lifted = scale * wide_query - applied[:, :width]
            slot = slot_of(group, index, per_source)
            moved = dot(lifted.astype(BF16), before_buf[head, slot])
            rows = pl.ds(pl.multiple_of(slot * chunk, chunk), chunk)
            out_ref[rows, lanes] = applied[:, width:] + moved[:, width:]
            lift_ref[rows, lanes] = (lifted - moved[:, :width]).astype(BF16)

    every_unit(heads, chunks, answer)


def read(keys, rests, high, low, steps):
    group = len(keys)
    tokens, wide = rests[0].shape
    return pl.pallas_call(
        functools.partial(read_kernel, group),
        out_shape=(
            pltpu.VMEM((group * tokens, wide), F32),
            pltpu.VMEM((group * tokens, wide), BF16),
        ),
        in_specs=[VMEM] * (2 * group + 3),
        out_specs=(VMEM, VMEM),
        scratch_shapes=[pltpu.VMEM(steps.shape, BF16)],
        compiler_params=PARAMS,
        name="read",
    )(*held(*keys, *rests, high, low, steps))


def join_kernel(count, *refs):
    states, (local_ref, lift_ref, out_ref) = refs[:count], refs[count:]
    heads, width, _ = states[0].shape
    for head in range(heads):
        lanes = slice(head * width, (head + 1) * width)
        total = None
        for state in reversed(states):
            if total is None:
                total = state[head].astype(F32)
            else:
                step = state[head].astype(F32)
                total = (
                    total + step[:, width:] - dot(state[head, :, :width], total.astype(BF16))
                )
        out_ref[:, lanes] = (
            local_ref[:, lanes] + dot(lift_ref[:, lanes], total.astype(BF16))
        ).astype(BF16)


def join(states, local, lifted):
    return pl.pallas_call(
        functools.partial(join_kernel, len(states)),
        out_shape=pltpu.VMEM(local.shape, BF16),
        in_specs=[VMEM] * (len(states) + 2),
        out_specs=VMEM,
        compiler_params=PARAMS,
        name="join",
    )(*held(*states, local, lifted))


def compose(earlier, later):
    width = earlier.shape[1]
    moved = jnp.einsum("hab,hbc->hac", later[:, :, :width], earlier, preferred_element_type=F32)
    return (earlier.astype(F32) + later.astype(F32) - moved).astype(BF16)


def weight_rows(weights, offset, inner, first, count):
    rows = pl.ds(first, count)
    if offset == 2:
        return jnp.where(inner, weights[3][rows, :], weights[4][rows, :])
    return weights[{0: 0, 1: 1, 3: 2}[offset]][rows, :]


def where_am_i(group):
    device = lax.axis_index("seq")
    return lax.rem(device, group), device // group


def target_rows(source, group, targets):
    position, _ = where_am_i(group)
    tokens = source.shape[0] // group
    firsts = [pl.multiple_of(place(position, t) * tokens, tokens) for t in targets]
    return jnp.concatenate([source[pl.ds(first, tokens), :] for first in firsts], axis=0)


def begin_kernel(group, halves, early, *refs):
    heads_in, weight_in, totals = refs[: len(early[0])], refs[len(early[0]) : -2], refs[-2:]
    position, _ = where_am_i(group)
    wide = heads_in[0].shape[1]
    columns = weight_in[0].shape[1]
    for targets, total_ref in zip(halves, totals):
        for number, offset in enumerate(early[1]):
            total = None
            for member, source in zip(early[0], heads_in):
                first = pl.multiple_of(place(position, member) * wide, wide)
                part = dot(
                    target_rows(source, group, targets),
                    weight_rows(weight_in, offset, None, first, wide),
                )
                total = part if total is None else total + part
            total_ref[:, number * columns : (number + 1) * columns] = total


def project_kernel(group, targets, early, offsets, *refs):
    heads_in, weight_in = refs[:group], refs[group:-3]
    total_ref, send_ref, keep_ref = refs[-3:]
    core = lax.axis_index("head")
    position, plane = where_am_i(group)
    wide = heads_in[0].shape[1]
    columns = weight_in[0].shape[1]
    side = keep_ref.shape[1] // columns
    inner = (plane == 1) | (plane == 2)
    for offset in offsets:
        owner = jnp.bitwise_xor(plane, offset)
        total = None
        members = range(group)
        if offset in early[1]:
            number = early[1].index(offset)
            members = [member for member in members if member not in early[0]]
        for member in members:
            first = pl.multiple_of(place(position, member) * wide, wide)
            part = dot(
                target_rows(heads_in[member], group, targets),
                weight_rows(weight_in, offset, inner, first, wide),
            )
            total = part if total is None else total + part
        if offset in early[1]:
            total = total + total_ref[:, number * columns : (number + 1) * columns]
        result = total.astype(BF16)
        lanes = pl.ds(pl.multiple_of(lax.rem(owner, side) * columns, columns), columns)

        @pl.when(owner // side == core)
        def _():
            keep_ref[:, lanes] = result

        @pl.when(owner // side != core)
        def _():
            send_ref[:, lanes] = result


def begin_projection(heads, weights, halves, early):
    group = len(heads)
    tokens = heads[0].shape[0] // group
    columns = weights[0].shape[1]
    here = [heads[member] for member in early[0]] + list(weights[: len(early[1])])
    return pl.pallas_call(
        functools.partial(begin_kernel, group, halves, early),
        out_shape=[
            pltpu.VMEM((tokens * len(targets), columns * len(early[1])), F32)
            for targets in halves
        ],
        in_specs=[VMEM] * len(here),
        out_specs=[VMEM] * 2,
        compiler_params=PARAMS,
        name="begin_projection",
    )(*held(*here))


def project(heads, weights, planes, targets, early, total):
    group = len(heads)
    rows = heads[0].shape[0] // group * len(targets)
    columns = weights[0].shape[1]
    offsets = (0, 1, 3, 2) if planes == 4 else (0, 1)
    shape = pltpu.VMEM((rows, columns * planes // 2), BF16)
    return pl.pallas_call(
        functools.partial(project_kernel, group, targets, early, offsets),
        out_shape=(shape, shape),
        in_specs=[VMEM] * (group + len(weights) + 1),
        out_specs=(VMEM, VMEM),
        compiler_params=PARAMS,
        name="project",
    )(*held(*heads, *weights, total))


def sum_kernel(keep_ref, other_ref, *outs):
    tokens = outs[0].shape[0]
    for index, out_ref in enumerate(outs):
        rows = slice(index * tokens, (index + 1) * tokens)
        out_ref[...] = (keep_ref[rows, :].astype(F32) + other_ref[rows, :].astype(F32)).astype(
            BF16
        )


def sum_parts(keep, other, count):
    rows, columns = keep.shape
    return pl.pallas_call(
        sum_kernel,
        out_shape=[pltpu.VMEM((rows // count, columns), BF16)] * count,
        in_specs=[VMEM, VMEM],
        out_specs=[VMEM] * count,
        compiler_params=PARAMS,
        name="sum_parts",
    )(*held(keep, other))


def lay_kernel(group, columns, *refs):
    parts, out_ref, sems = refs[:group], refs[group], refs[group + 1]
    position = lax.rem(lax.axis_index("seq"), group)
    copies = []
    for offset in range(group):
        for index in range(parts[0].shape[1] // columns):
            first = (index * group + place(position, offset)) * columns
            copies.append(
                pltpu.make_async_copy(
                    parts[offset].at[:, index * columns : (index + 1) * columns],
                    out_ref.at[:, pl.ds(pl.multiple_of(first, columns), columns)],
                    sems.at[len(copies)],
                )
            )
    for copy in copies:
        copy.start()
    for copy in copies:
        copy.wait()


def lay_out(parts, columns):
    group = len(parts)
    rows, wide = parts[0].shape
    return pl.pallas_call(
        functools.partial(lay_kernel, group, columns),
        out_shape=jax.ShapeDtypeStruct((rows, group * wide), BF16),
        in_specs=[VMEM] * group,
        out_specs=pl.BlockSpec(memory_space=pl.ANY),
        scratch_shapes=[pltpu.SemaphoreType.DMA((group * wide // columns,))],
        compiler_params=PARAMS,
        name="lay_out",
    )(*held(*parts))


def swap(value, group, offset, count):
    pairs = [(i, (i // group) * group + ((i % group) ^ offset)) for i in range(count)]
    return lax.ppermute(value, "seq", pairs)


def per_device(queries, key_vectors, values, strengths, out_weight):
    count = lax.axis_size("seq")
    sides = lax.axis_size("head")
    heads = strengths.shape[1]
    tokens = queries.shape[0]
    width = queries.shape[1] // heads
    group = 1
    while group < 4 and heads % (2 * group) == 0 and count % (2 * group) == 0:
        group *= 2
    planes = count // group
    position = lax.axis_index("seq") % group
    mine = heads // group
    keys = list(pack_keys(key_vectors, strengths, group))
    vals, asks = [], []
    for offset in range(group):
        lane = jnp.bitwise_xor(position, offset) * mine * width
        value = lax.dynamic_slice_in_dim(values, lane, mine * width, 2)
        ask = lax.dynamic_slice_in_dim(queries, lane, mine * width, 1)
        if offset:
            keys[offset] = swap(keys[offset], group, offset, count)
            value = swap(value, group, offset, count)
            ask = swap(ask, group, offset, count)
        vals.append(value)
        asks.append(ask)

    split_out = sides == 2 and planes in (2, 4) and group > 1
    weights = [out_weight]
    if split_out:
        for offset in range(1, planes, 2):
            pairs = [(i, ((i // group) ^ offset) * group + i % group) for i in range(count)]
            weights.append(lax.ppermute(out_weight, "seq", pairs))

    near = max(group // 2, 1)
    solved = []
    for part in (keys[:near], keys[near:]):
        if part:
            solved.append(invert(part, mine, tokens))
    inverses, tables = zip(*solved)
    high, low, steps, state, local_state = carry_state(keys, vals, inverses, tables)
    local, lifted = read(keys, asks, high, low, steps)

    def from_earlier(value, distance):
        pairs = [(i, i + distance * group) for i in range(count - distance * group)]
        return lax.ppermute(value, "seq", pairs)

    if planes <= 4:
        states = []
        for distance in range(1, planes):
            sent = state if distance + 1 < planes else local_state
            states.append(from_earlier(sent, distance))
    else:
        total = from_earlier(state, 1)
        distance = 1
        while distance < planes - 1:
            total = compose(from_earlier(total, distance), total)
            distance *= 2
        states = [total[:, :, width:]]
    if split_out and planes == 4:
        for held_weight, hops in ((weights[1], ((1, 2), (2, 1))), (weights[2], ((1, 0), (2, 3)))):
            pairs = [
                (source * group + i, target * group + i)
                for source, target in hops
                for i in range(group)
            ]
            weights.append(lax.ppermute(held_weight, "seq", pairs))

    mixed_heads = join(states, local, lifted)

    if split_out:
        order = tuple(reversed(range(group)))
        order = order[:1] + order[2:-1] + order[1:2] + order[-1:] if group > 2 else order
        row_halves = (order[: group // 2], order[group // 2 :])
        early = (tuple(range(group - 1)), (0, 1, 3) if planes == 4 else (0, 1))
        parts = [None] * group
        gathered = [mixed_heads]
        for offset in range(1, group):
            gathered.append(swap(mixed_heads, group, offset, count))
        totals = begin_projection(gathered, weights, row_halves, early)
        halves = []
        for targets, total in zip(row_halves, totals):
            send, keep = project(gathered, weights, planes, targets, early, total)
            other = lax.ppermute(send, "head", [(0, 1), (1, 0)])
            halves.append((targets, keep, other))
        for targets, keep, other in halves:
            for offset, part in zip(targets, sum_parts(keep, other, len(targets))):
                parts[offset] = swap(part, group, offset, count) if offset else part
        return lay_out(parts, out_weight.shape[1])

    if group > 1:
        position_rows = []
        for offset in range(group):
            first = jnp.bitwise_xor(position, offset) * tokens
            part = lax.dynamic_slice_in_dim(mixed_heads, first, tokens, 0)
            position_rows.append(swap(part, group, offset, count) if offset else part)
        stacked = jnp.stack(position_rows)
        order = jnp.bitwise_xor(position, jnp.arange(group))
        stacked = jnp.take(stacked, order, axis=0)
        mixed_heads = jnp.swapaxes(stacked, 0, 1).reshape(tokens, heads * width)
    partial_sums = jnp.dot(
        mixed_heads,
        lax.all_gather(out_weight, "seq", axis=1, tiled=True),
        preferred_element_type=F32,
    )
    return lax.psum_scatter(
        partial_sums.astype(BF16), "head", scatter_dimension=1, tiled=True
    )


def solution(mesh):
    return jax.shard_map(
        per_device,
        mesh=mesh,
        in_specs=(
            P("seq", "head"),
            P(None, "seq", "head"),
            P(None, "seq", "head"),
            P(None, "head", "seq"),
            P("head", "seq"),
        ),
        out_specs=P("seq", "head"),
        check_vma=False,
    )
```

```python
import functools

import jax
import jax.numpy as jnp
from jax import lax
from jax.experimental import pallas as pl
from jax.experimental.pallas import tpu as pltpu
from jax.sharding import PartitionSpec as P


CHUNK = 128
EPS = 1e-06
F32 = jnp.float32
BF16 = jnp.bfloat16


def dot(a, b):
    return jnp.dot(a, b, preferred_element_type=F32)


def dot_t(a, b):
    return lax.dot_general(a, b, (((1,), (1,)), ((), ())), preferred_element_type=F32)


def split(x):
    high = x.astype(BF16)
    return high, (x - high.astype(F32)).astype(BF16)


def product3(left, right):
    left_high, left_low = split(left)
    right_high, right_low = split(right)
    lhs = jnp.concatenate([left_high, left_low], axis=1)
    rhs = jnp.concatenate(
        [
            jnp.concatenate([right_high, right_low], axis=1),
            jnp.concatenate([right_high, jnp.zeros_like(right_low)], axis=1),
        ],
        axis=0,
    )
    wide = dot(lhs, rhs)
    width = right.shape[1]
    return wide[:, :width] + wide[:, width:]


def iota(shape, axis):
    return lax.broadcasted_iota(jnp.int32, shape, axis)


def weave(first, second):
    half = first.shape[0] // 2
    return jnp.concatenate([first[:half], second[:half], first[half:], second[half:]], axis=0)


def weave_lanes(first, second):
    half = first.shape[1] // 2
    return jnp.concatenate(
        [first[:, :half], second[:, :half], first[:, half:], second[:, half:]], axis=1
    )


def place(position, offset):
    return jnp.bitwise_xor(position, offset)


VMEM = pl.BlockSpec(memory_space=pltpu.VMEM)
PARAMS = pltpu.CompilerParams(vmem_limit_bytes=12 * 2**20)


def held(*arrays):
    return [pltpu.with_memory_space_constraint(array, pltpu.VMEM) for array in arrays]


def times(chunk):
    half = chunk // 2
    row, col = iota((chunk, chunk), 0), iota((chunk, chunk), 1)
    return 2 * lax.rem(row, half) + row // half, 2 * lax.rem(col, half) + col // half


def beta_rows(tokens, width):
    return -(-4 * max(tokens // width, 1) // 16) * 16


def pack_kernel(group, key_ref, value_ref, query_ref, strength_ref, *refs):
    key_outs, rest_outs, (beta_ref, sems) = refs[:group], refs[group : 2 * group], refs[-2:]
    _, heads, tokens = beta_ref.shape
    mine = heads // group
    wide = key_outs[0].shape[1]
    width = wide // mine
    pieces = max(tokens // width, 1)
    inside = tokens // pieces
    position, _ = where_am_i(group)
    first_copy = pltpu.make_async_copy(strength_ref, beta_ref, sems.at[0])
    pairs = []
    for offset in range(group):
        lanes = pl.ds(pl.multiple_of(place(position, offset) * wide, wide), wide)
        for reflection in range(2):
            rows = pl.ds(reflection * tokens, tokens)
            pairs.append((key_ref.at[reflection, :, lanes], key_outs[offset].at[rows, :]))
    for offset in range(group):
        lanes = pl.ds(pl.multiple_of(place(position, offset) * wide, wide), wide)
        for reflection in range(2):
            pairs.append(
                (value_ref.at[reflection, :, lanes], rest_outs[offset].at[reflection])
            )
        pairs.append((query_ref.at[:, lanes], rest_outs[offset].at[2]))
    copies = [
        pltpu.make_async_copy(source, target, sems.at[1 + number])
        for number, (source, target) in enumerate(pairs)
    ]
    first_copy.start()
    for copy in copies:
        copy.start()
    first_copy.wait()
    for offset, out_ref in enumerate(key_outs):
        member = place(position, offset)
        rows = []
        for reflection in range(2):
            for piece in range(pieces):
                cuts = []
                for head in range(mine):
                    cut = beta_ref[reflection, pl.ds(member * mine + head, 1), :]
                    cuts.append(cut[:, piece * inside : (piece + 1) * inside])
                    if inside < width:
                        cuts.append(jnp.zeros((1, width - inside), F32))
                rows.append(jnp.concatenate(cuts, axis=1) if len(cuts) > 1 else cuts[0])
        both = jnp.concatenate(rows, axis=0)
        high = both.astype(BF16).astype(F32)
        spare = jnp.zeros((out_ref.shape[0] - 2 * tokens - 2 * len(rows), wide), F32)
        out_ref[2 * tokens :, :] = jnp.concatenate([high, both - high, spare], axis=0).astype(BF16)
    for copy in copies:
        copy.wait()


def pack(queries, key_vectors, values, strengths, group):
    _, tokens, wide = key_vectors.shape
    width = wide // strengths.shape[1]
    shape = (2 * tokens + beta_rows(tokens, width), wide // group)
    out = pl.pallas_call(
        functools.partial(pack_kernel, group),
        out_shape=[pltpu.VMEM(shape, BF16)] * group
        + [pltpu.VMEM((3, tokens, wide // group), BF16)] * group,
        in_specs=[pl.BlockSpec(memory_space=pltpu.HBM)] * 4,
        out_specs=[VMEM] * (2 * group),
        scratch_shapes=[
            pltpu.VMEM(strengths.shape, F32),
            pltpu.SemaphoreType.DMA((1 + 5 * group,)),
        ],
        compiler_params=PARAMS,
        name="pack",
    )(
        *(
            pltpu.with_memory_space_constraint(array, pltpu.HBM)
            for array in (key_vectors, values, queries, strengths)
        )
    )
    return list(out[:group]), list(out[group:])


def invert_kernel(heads, tokens, *refs):
    key_in, (inverse_ref, table_ref, a_buf) = refs[:-3], refs[-3:]
    width = key_in[0].shape[1] // heads
    chunk = min(CHUNK, tokens)
    per_source = tokens // chunk
    chunks = len(key_in) * per_source
    pieces = max(tokens // width, 1)
    row_time, col_time = times(chunk)
    levels = chunk.bit_length() - 1

    def joins(level):
        same = (row_time >> (level + 1)) == (col_time >> (level + 1))
        return same & (((row_time >> level) & 1) == 1) & (((col_time >> level) & 1) == 0)

    def prepare(head, index):
        lanes = lanes_of(head, width)
        key_ref, first = key_in[index // per_source], (index % per_source) * chunk
        key = woven_key(key_ref, tokens, first, chunk, lanes)
        gram = dot_t(key, key)
        wide_row, wide_col = iota(gram.shape, 0), iota(gram.shape, 1)
        square = jnp.sum(jnp.where(wide_row == wide_col, gram, 0.0), axis=0, keepdims=True)
        scale_row = lax.rsqrt(square + EPS)
        halves = key_ref[2 * tokens :, lanes].astype(F32)
        piece, inside = first // width, first % width

        def strength(reflection):
            high = reflection * pieces + piece
            low = (2 + reflection) * pieces + piece
            both = halves[high : high + 1] + halves[low : low + 1]
            return both[:, inside : inside + chunk]

        beta_row = weave_lanes(strength(0), strength(1))
        both_row = beta_row * scale_row
        table = jnp.concatenate(
            [scale_row, beta_row, both_row, jnp.zeros((5, 2 * chunk), F32)], axis=0
        )
        table_ref[head, index] = table
        system = table.T[:, 2:3] * (gram * scale_row)
        for block in range(2):
            here = slice(block * chunk, (block + 1) * chunk)
            diagonal = system[here, here]
            a_buf[head, index, block] = diagonal
            inverse_ref[head, index, block] = jnp.where(
                row_time == col_time, 1.0, 0.0
            ) - jnp.where(joins(0), diagonal, 0.0)
        inverse_ref[head, index, 2] = system[chunk:, :chunk]

    def solve(units):
        for head, index in units:
            prepare(head, index)
        every = [(head, index, block) for head, index in units for block in range(2)]
        for level in range(1, levels):
            mask = joins(level)
            inner = [
                product3(jnp.where(mask, a_buf[one], 0.0), inverse_ref[one]) for one in every
            ]
            for one, value in zip(every, inner):
                known = inverse_ref[one]
                inverse_ref[one] = known - product3(known, value)
        inner = [
            product3(inverse_ref[head, index, 2], inverse_ref[head, index, 0])
            for head, index in units
        ]
        for (head, index), value in zip(units, inner):
            inverse_ref[head, index, 2] = -product3(inverse_ref[head, index, 1], value)

    every_unit(heads, chunks, solve)


def lanes_of(head, width):
    if isinstance(head, int):
        return slice(head * width, (head + 1) * width)
    return pl.ds(pl.multiple_of(head * width, width), width)


def invert(keys, heads, tokens):
    chunk = min(CHUNK, tokens)
    chunks = len(keys) * tokens // chunk
    return pl.pallas_call(
        functools.partial(invert_kernel, heads, tokens),
        out_shape=(
            pltpu.VMEM((heads, chunks, 3, chunk, chunk), F32),
            pltpu.VMEM((heads, chunks, 8, 2 * chunk), F32),
        ),
        in_specs=[VMEM] * len(keys),
        out_specs=(VMEM, VMEM),
        scratch_shapes=[pltpu.VMEM((heads, chunks, 2, chunk, chunk), F32)],
        compiler_params=PARAMS,
        name="invert",
    )(*held(*keys))


def slot_of(group, index, per_source):
    position = lax.rem(lax.axis_index("seq"), group)
    return place(position, index // per_source) * per_source + index % per_source


def every_unit(heads, chunks, body):
    if heads * chunks <= 8:
        body([(head, index) for head in range(heads) for index in range(chunks)])
    else:

        def one_head(head, carry):
            body([(head, index) for index in range(chunks)])
            return carry

        lax.fori_loop(0, heads, one_head, 0)


def woven_key(key_ref, tokens, first, chunk, lanes):
    return weave(
        key_ref[first : first + chunk, lanes],
        key_ref[tokens + first : tokens + first + chunk, lanes],
    )


def state_kernel(group, parts, *refs):
    key_in, rest_in = refs[:group], refs[group : 2 * group]
    inverse_in = refs[2 * group : 2 * group + parts]
    table_in = refs[2 * group + parts : 2 * group + 2 * parts]
    high_ref, low_ref, step_ref, state_ref, local_ref = refs[2 * group + 2 * parts :]
    heads, per_part, _, chunk, _ = inverse_in[0].shape
    chunks = parts * per_part
    tokens = rest_in[0].shape[1]
    width = rest_in[0].shape[2] // heads
    per_source = tokens // chunk

    def solve(units):
        for head, index in units:
            lanes = lanes_of(head, width)
            part, inside = index // per_part, index % per_part
            source, first = index // per_source, (index % per_source) * chunk
            key_ref, rest_ref = key_in[source], rest_in[source]
            key = woven_key(key_ref, tokens, first, chunk, lanes).astype(F32)
            rows = slice(first, first + chunk)
            value = weave(rest_ref[0, rows, lanes], rest_ref[1, rows, lanes]).astype(F32)
            table = table_in[part][head, inside].T
            inverse = jnp.concatenate(
                [
                    jnp.concatenate(
                        [inverse_in[part][head, inside, 0], jnp.zeros((chunk, chunk), F32)],
                        axis=1,
                    ),
                    jnp.concatenate(
                        [inverse_in[part][head, inside, 2], inverse_in[part][head, inside, 1]],
                        axis=1,
                    ),
                ],
                axis=0,
            )
            right = jnp.concatenate([table[:, 2:3] * key, table[:, 1:2] * value], axis=1)
            high, low = split(table[:, 0:1] * dot3(inverse, *split(right)))
            high_ref[head, index] = high
            low_ref[head, index] = low
        for head, index in units:
            source, first = index // per_source, (index % per_source) * chunk
            turned = woven_key(key_in[source], tokens, first, chunk, lanes_of(head, width)).T
            step_ref[head, slot_of(group, index, per_source)] = dot(
                turned, high_ref[head, index]
            ) + dot(turned, low_ref[head, index])

    every_unit(heads, chunks, solve)
    totals = [[step_ref[head, slot] for slot in range(chunks)] for head in range(heads)]
    while len(totals[0]) > 1:
        totals = [
            [after(one[i], one[i + 1]) for i in range(0, len(one) - 1, 2)]
            + one[len(one) - len(one) % 2 :]
            for one in totals
        ]
    for head, (total,) in enumerate(totals):
        state_ref[head] = total.astype(BF16)
        local_ref[head] = total[:, width:].astype(BF16)


def after(earlier, later):
    width = earlier.shape[0]
    return earlier + later - dot(later[:, :width].astype(BF16), earlier.astype(BF16))


def dot3(left, high, low):
    left_high, left_low = split(left)
    return dot(left_high, high) + dot(left_low, high) + dot(left_high, low)


def carry_state(keys, rests, inverses, tables):
    group, parts = len(keys), len(inverses)
    heads, per_part, _, chunk, _ = inverses[0].shape
    chunks = parts * per_part
    width = rests[0].shape[2] // heads
    solved = pltpu.VMEM((heads, chunks, 2 * chunk, 2 * width), BF16)
    return pl.pallas_call(
        functools.partial(state_kernel, group, parts),
        out_shape=(
            solved,
            solved,
            pltpu.VMEM((heads, chunks, width, 2 * width), F32),
            pltpu.VMEM((heads, width, 2 * width), BF16),
            pltpu.VMEM((heads, width, width), BF16),
        ),
        in_specs=[VMEM] * (2 * group + 2 * parts),
        out_specs=(VMEM,) * 5,
        compiler_params=PARAMS,
        name="carry_state",
    )(*held(*keys, *rests, *inverses, *tables))


def read_kernel(group, *refs):
    key_in, rest_in = refs[:group], refs[group : 2 * group]
    high_ref, low_ref, step_ref, out_ref, lift_ref, before_buf = refs[2 * group :]
    heads, chunks, wide, _ = high_ref.shape
    chunk = wide // 2
    half = chunk // 2
    tokens = rest_in[0].shape[1]
    width = rest_in[0].shape[2] // heads
    per_source = tokens // chunk
    token_row = iota((chunk, 2 * chunk), 0)
    token_col = iota((chunk, 2 * chunk), 1)
    token_col = (token_col // chunk) * half + lax.rem(token_col, half)
    totals = [step_ref[head, 0] for head in range(heads)]
    for head in range(heads):
        before_buf[head, 0] = jnp.zeros((width, 2 * width), BF16)
    for slot in range(1, chunks):
        for head in range(heads):
            before_buf[head, slot] = totals[head].astype(BF16)
        totals = [after(totals[head], step_ref[head, slot]) for head in range(heads)]

    def answer(units):
        for head, index in units:
            lanes = lanes_of(head, width)
            source, first = index // per_source, (index % per_source) * chunk
            key = woven_key(key_in[source], tokens, first, chunk, lanes)
            query = rest_in[source][2, first : first + chunk, lanes]
            wide_query = query.astype(F32)
            scale = lax.rsqrt(jnp.sum(wide_query * wide_query, axis=1, keepdims=True) + EPS)
            scores = jnp.where(token_col <= token_row, dot_t(query, key) * scale, 0.0)
            applied = dot3(scores, high_ref[head, index], low_ref[head, index])
            lifted = scale * wide_query - applied[:, :width]
            slot = slot_of(group, index, per_source)
            moved = dot(lifted.astype(BF16), before_buf[head, slot])
            rows = pl.ds(pl.multiple_of(slot * chunk, chunk), chunk)
            out_ref[rows, lanes] = applied[:, width:] + moved[:, width:]
            lift_ref[rows, lanes] = (lifted - moved[:, :width]).astype(BF16)

    every_unit(heads, chunks, answer)


def read(keys, rests, high, low, steps):
    group = len(keys)
    _, tokens, wide = rests[0].shape
    return pl.pallas_call(
        functools.partial(read_kernel, group),
        out_shape=(
            pltpu.VMEM((group * tokens, wide), F32),
            pltpu.VMEM((group * tokens, wide), BF16),
        ),
        in_specs=[VMEM] * (2 * group + 3),
        out_specs=(VMEM, VMEM),
        scratch_shapes=[pltpu.VMEM(steps.shape, BF16)],
        compiler_params=PARAMS,
        name="read",
    )(*held(*keys, *rests, high, low, steps))


def join_kernel(count, *refs):
    states, (local_ref, lift_ref, out_ref) = refs[:count], refs[count:]
    heads, width, _ = states[0].shape
    for head in range(heads):
        lanes = slice(head * width, (head + 1) * width)
        total = None
        for state in reversed(states):
            if total is None:
                total = state[head].astype(F32)
            else:
                step = state[head].astype(F32)
                total = (
                    total + step[:, width:] - dot(state[head, :, :width], total.astype(BF16))
                )
        out_ref[:, lanes] = (
            local_ref[:, lanes] + dot(lift_ref[:, lanes], total.astype(BF16))
        ).astype(BF16)


def join(states, local, lifted):
    return pl.pallas_call(
        functools.partial(join_kernel, len(states)),
        out_shape=pltpu.VMEM(local.shape, BF16),
        in_specs=[VMEM] * (len(states) + 2),
        out_specs=VMEM,
        compiler_params=PARAMS,
        name="join",
    )(*held(*states, local, lifted))


def compose(earlier, later):
    width = earlier.shape[1]
    moved = jnp.einsum("hab,hbc->hac", later[:, :, :width], earlier, preferred_element_type=F32)
    return (earlier.astype(F32) + later.astype(F32) - moved).astype(BF16)


def weight_rows(weights, offset, inner, first, count):
    rows = pl.ds(first, count)
    if offset < 2:
        return weights[offset][rows, :]
    if offset == 2:
        return jnp.where(inner, weights[5][rows, :], weights[6][rows, :])
    far = jnp.concatenate([weights[3][rows, :], weights[4][rows, :]], axis=1)
    return jnp.where(inner, weights[2][rows, :], far)


def where_am_i(group):
    device = lax.axis_index("seq")
    return lax.rem(device, group), device // group


def target_rows(source, group, targets):
    position, _ = where_am_i(group)
    tokens = source.shape[0] // group
    firsts = [pl.multiple_of(place(position, t) * tokens, tokens) for t in targets]
    return jnp.concatenate([source[pl.ds(first, tokens), :] for first in firsts], axis=0)


def begin_kernel(group, halves, early, *refs):
    heads_in, weight_in, totals = refs[: len(early[0])], refs[len(early[0]) : -2], refs[-2:]
    position, _ = where_am_i(group)
    wide = heads_in[0].shape[1]
    columns = weight_in[0].shape[1]
    for targets, total_ref in zip(halves, totals):
        for number, offset in enumerate(early[1]):
            total = None
            for member, source in zip(early[0], heads_in):
                first = pl.multiple_of(place(position, member) * wide, wide)
                part = dot(
                    target_rows(source, group, targets),
                    weight_rows(weight_in, offset, None, first, wide),
                )
                total = part if total is None else total + part
            total_ref[:, number * columns : (number + 1) * columns] = total


def project_kernel(group, targets, early, offsets, *refs):
    heads_in, weight_in = refs[:group], refs[group:-3]
    total_ref, send_ref, keep_ref = refs[-3:]
    core = lax.axis_index("head")
    position, plane = where_am_i(group)
    wide = heads_in[0].shape[1]
    columns = weight_in[0].shape[1]
    side = keep_ref.shape[1] // columns
    inner = (plane == 1) | (plane == 2)
    for offset in offsets:
        owner = jnp.bitwise_xor(plane, offset)
        total = None
        members = range(group)
        if offset in early[1]:
            number = early[1].index(offset)
            members = [member for member in members if member not in early[0]]
        for member in members:
            first = pl.multiple_of(place(position, member) * wide, wide)
            part = dot(
                target_rows(heads_in[member], group, targets),
                weight_rows(weight_in, offset, inner, first, wide),
            )
            total = part if total is None else total + part
        if offset in early[1]:
            total = total + total_ref[:, number * columns : (number + 1) * columns]
        result = total.astype(BF16)
        lanes = pl.ds(pl.multiple_of(lax.rem(owner, side) * columns, columns), columns)

        @pl.when(owner // side == core)
        def _():
            keep_ref[:, lanes] = result

        @pl.when(owner // side != core)
        def _():
            send_ref[:, lanes] = result


def begin_projection(heads, weights, halves, early):
    group = len(heads)
    tokens = heads[0].shape[0] // group
    columns = weights[0].shape[1]
    here = [heads[member] for member in early[0]] + list(weights[: len(early[1])])
    return pl.pallas_call(
        functools.partial(begin_kernel, group, halves, early),
        out_shape=[
            pltpu.VMEM((tokens * len(targets), columns * len(early[1])), F32)
            for targets in halves
        ],
        in_specs=[VMEM] * len(here),
        out_specs=[VMEM] * 2,
        compiler_params=PARAMS,
        name="begin_projection",
    )(*held(*here))


def project(heads, weights, planes, targets, early, total):
    group = len(heads)
    rows = heads[0].shape[0] // group * len(targets)
    columns = weights[0].shape[1]
    offsets = (0, 1, 3, 2) if planes == 4 else (0, 1)
    shape = pltpu.VMEM((rows, columns * planes // 2), BF16)
    return pl.pallas_call(
        functools.partial(project_kernel, group, targets, early, offsets),
        out_shape=(shape, shape),
        in_specs=[VMEM] * (group + len(weights) + 1),
        out_specs=(VMEM, VMEM),
        compiler_params=PARAMS,
        name="project",
    )(*held(*heads, *weights, total))


def sum_kernel(keep_ref, other_ref, *outs):
    tokens = outs[0].shape[0]
    for index, out_ref in enumerate(outs):
        rows = slice(index * tokens, (index + 1) * tokens)
        out_ref[...] = (keep_ref[rows, :].astype(F32) + other_ref[rows, :].astype(F32)).astype(
            BF16
        )


def sum_parts(keep, other, count):
    rows, columns = keep.shape
    return pl.pallas_call(
        sum_kernel,
        out_shape=[pltpu.VMEM((rows // count, columns), BF16)] * count,
        in_specs=[VMEM, VMEM],
        out_specs=[VMEM] * count,
        compiler_params=PARAMS,
        name="sum_parts",
    )(*held(keep, other))


def lay_kernel(group, columns, *refs):
    parts, out_ref, sems = refs[:group], refs[group], refs[group + 1]
    position = lax.rem(lax.axis_index("seq"), group)
    copies = []
    for offset in range(group):
        for index in range(parts[0].shape[1] // columns):
            first = (index * group + place(position, offset)) * columns
            copies.append(
                pltpu.make_async_copy(
                    parts[offset].at[:, index * columns : (index + 1) * columns],
                    out_ref.at[:, pl.ds(pl.multiple_of(first, columns), columns)],
                    sems.at[len(copies)],
                )
            )
    for copy in copies:
        copy.start()
    for copy in copies:
        copy.wait()


def lay_out(parts, columns):
    group = len(parts)
    rows, wide = parts[0].shape
    return pl.pallas_call(
        functools.partial(lay_kernel, group, columns),
        out_shape=jax.ShapeDtypeStruct((rows, group * wide), BF16),
        in_specs=[VMEM] * group,
        out_specs=pl.BlockSpec(memory_space=pl.ANY),
        scratch_shapes=[pltpu.SemaphoreType.DMA((group * wide // columns,))],
        compiler_params=PARAMS,
        name="lay_out",
    )(*held(*parts))


def swap(value, group, offset, count):
    pairs = [(i, (i // group) * group + ((i % group) ^ offset)) for i in range(count)]
    return lax.ppermute(value, "seq", pairs)


def per_device(queries, key_vectors, values, strengths, out_weight):
    count = lax.axis_size("seq")
    sides = lax.axis_size("head")
    heads = strengths.shape[1]
    tokens = queries.shape[0]
    width = queries.shape[1] // heads
    group = 1
    while group < 4 and heads % (2 * group) == 0 and count % (2 * group) == 0:
        group *= 2
    planes = count // group
    position = lax.axis_index("seq") % group
    mine = heads // group
    keys, rests = pack(queries, key_vectors, values, strengths, group)
    for offset in range(1, group):
        keys[offset] = swap(keys[offset], group, offset, count)
        rests[offset] = swap(rests[offset], group, offset, count)

    def between_planes(value, pairs):
        return lax.ppermute(
            value,
            "seq",
            [
                (source * group + i, target * group + i)
                for source, target in pairs
                for i in range(group)
            ],
        )

    split_out = sides == 2 and planes in (2, 4) and group > 1
    columns = out_weight.shape[1]
    weights = [out_weight]
    if split_out:
        swapped = [(plane, plane ^ 1) for plane in range(planes)]
        weights.append(between_planes(out_weight, swapped))
    if split_out and planes == 4:
        outer = ((0, 3), (3, 0))
        weights.append(between_planes(out_weight, ((1, 2), (2, 1))))
        weights.append(between_planes(out_weight[:, : columns // 2], outer))

    near = max(group // 2, 1)
    solved = []
    for part in (keys[:near], keys[near:]):
        if part:
            solved.append(invert(part, mine, tokens))
    inverses, tables = zip(*solved)
    high, low, steps, state, local_state = carry_state(keys, rests, inverses, tables)
    local, lifted = read(keys, rests, high, low, steps)

    def from_earlier(value, distance):
        pairs = [(i, i + distance * group) for i in range(count - distance * group)]
        return lax.ppermute(value, "seq", pairs)

    if planes <= 4:
        states = []
        for distance in range(1, planes):
            sent = state if distance + 1 < planes else local_state
            states.append(from_earlier(sent, distance))
    else:
        total = from_earlier(state, 1)
        distance = 1
        while distance < planes - 1:
            total = compose(from_earlier(total, distance), total)
            distance *= 2
        states = [total[:, :, width:]]
    if split_out and planes == 4:
        late = between_planes(out_weight[:, columns // 2 :], outer)
        weights += [
            late,
            between_planes(weights[1], ((1, 2), (2, 1))),
            between_planes(weights[2], ((1, 0), (2, 3))),
        ]

    mixed_heads = join(states, local, lifted)

    if split_out:
        order = tuple(range(1, group)) + (0,)
        row_halves = (order[: group // 2], order[group // 2 :])
        early = (tuple(range(group - 1)), (0, 1))
        parts = [None] * group
        gathered = [mixed_heads]
        for offset in range(1, group):
            gathered.append(swap(mixed_heads, group, offset, count))
        totals = begin_projection(gathered, weights, row_halves, early)
        halves = []
        for targets, total in zip(row_halves, totals):
            send, keep = project(gathered, weights, planes, targets, early, total)
            other = lax.ppermute(send, "head", [(0, 1), (1, 0)])
            halves.append((targets, keep, other))
        for targets, keep, other in halves:
            for offset, part in zip(targets, sum_parts(keep, other, len(targets))):
                parts[offset] = swap(part, group, offset, count) if offset else part
        return lay_out(parts, out_weight.shape[1])

    if group > 1:
        position_rows = []
        for offset in range(group):
            first = jnp.bitwise_xor(position, offset) * tokens
            part = lax.dynamic_slice_in_dim(mixed_heads, first, tokens, 0)
            position_rows.append(swap(part, group, offset, count) if offset else part)
        stacked = jnp.stack(position_rows)
        order = jnp.bitwise_xor(position, jnp.arange(group))
        stacked = jnp.take(stacked, order, axis=0)
        mixed_heads = jnp.swapaxes(stacked, 0, 1).reshape(tokens, heads * width)
    partial_sums = jnp.dot(
        mixed_heads,
        lax.all_gather(out_weight, "seq", axis=1, tiled=True),
        preferred_element_type=F32,
    )
    return lax.psum_scatter(
        partial_sums.astype(BF16), "head", scatter_dimension=1, tiled=True
    )


def solution(mesh):
    return jax.shard_map(
        per_device,
        mesh=mesh,
        in_specs=(
            P("seq", "head"),
            P(None, "seq", "head"),
            P(None, "seq", "head"),
            P(None, "head", "seq"),
            P("head", "seq"),
        ),
        out_specs=P("seq", "head"),
        check_vma=False,
    )
```

```python
import functools

import jax
import jax.numpy as jnp
from jax import lax
from jax.experimental import pallas as pl
from jax.experimental.pallas import tpu as pltpu
from jax.sharding import PartitionSpec as P


CHUNK = 128
EPS = 1e-06
F32 = jnp.float32
BF16 = jnp.bfloat16


def dot(a, b):
    return jnp.dot(a, b, preferred_element_type=F32)


def dot_t(a, b):
    return lax.dot_general(a, b, (((1,), (1,)), ((), ())), preferred_element_type=F32)


def split(x):
    high = x.astype(BF16)
    return high, (x - high.astype(F32)).astype(BF16)


def product3(left, right):
    left_high, left_low = split(left)
    right_high, right_low = split(right)
    lhs = jnp.concatenate([left_high, left_low], axis=1)
    rhs = jnp.concatenate(
        [
            jnp.concatenate([right_high, right_low], axis=1),
            jnp.concatenate([right_high, jnp.zeros_like(right_low)], axis=1),
        ],
        axis=0,
    )
    wide = dot(lhs, rhs)
    width = right.shape[1]
    return wide[:, :width] + wide[:, width:]


def iota(shape, axis):
    return lax.broadcasted_iota(jnp.int32, shape, axis)


def weave(first, second):
    half = first.shape[0] // 2
    return jnp.concatenate([first[:half], second[:half], first[half:], second[half:]], axis=0)


def weave_lanes(first, second):
    half = first.shape[1] // 2
    return jnp.concatenate(
        [first[:, :half], second[:, :half], first[:, half:], second[:, half:]], axis=1
    )


def place(position, offset):
    return jnp.bitwise_xor(position, offset)


VMEM = pl.BlockSpec(memory_space=pltpu.VMEM)
PARAMS = pltpu.CompilerParams(vmem_limit_bytes=12 * 2**20)


def held(*arrays):
    return [pltpu.with_memory_space_constraint(array, pltpu.VMEM) for array in arrays]


def times(chunk):
    half = chunk // 2
    row, col = iota((chunk, chunk), 0), iota((chunk, chunk), 1)
    return 2 * lax.rem(row, half) + row // half, 2 * lax.rem(col, half) + col // half


def beta_rows(tokens, width):
    return -(-4 * max(tokens // width, 1) // 16) * 16


def pack_kernel(group, key_ref, value_ref, query_ref, strength_ref, *refs):
    key_outs, rest_outs, (beta_ref, sems) = refs[:group], refs[group : 2 * group], refs[-2:]
    _, heads, tokens = beta_ref.shape
    mine = heads // group
    wide = key_outs[0].shape[1]
    width = wide // mine
    pieces = max(tokens // width, 1)
    inside = tokens // pieces
    position, _ = where_am_i(group)
    first_copy = pltpu.make_async_copy(strength_ref, beta_ref, sems.at[0])
    pairs = []
    for offset in range(group):
        lanes = pl.ds(pl.multiple_of(place(position, offset) * wide, wide), wide)
        for reflection in range(2):
            rows = pl.ds(reflection * tokens, tokens)
            pairs.append((key_ref.at[reflection, :, lanes], key_outs[offset].at[rows, :]))
    for offset in range(group):
        lanes = pl.ds(pl.multiple_of(place(position, offset) * wide, wide), wide)
        for reflection in range(2):
            pairs.append(
                (value_ref.at[reflection, :, lanes], rest_outs[offset].at[reflection])
            )
        pairs.append((query_ref.at[:, lanes], rest_outs[offset].at[2]))
    copies = [
        pltpu.make_async_copy(source, target, sems.at[1 + number])
        for number, (source, target) in enumerate(pairs)
    ]
    first_copy.start()
    for copy in copies:
        copy.start()
    first_copy.wait()
    for offset, out_ref in enumerate(key_outs):
        member = place(position, offset)
        rows = []
        for reflection in range(2):
            for piece in range(pieces):
                cuts = []
                for head in range(mine):
                    cut = beta_ref[reflection, pl.ds(member * mine + head, 1), :]
                    cuts.append(cut[:, piece * inside : (piece + 1) * inside])
                    if inside < width:
                        cuts.append(jnp.zeros((1, width - inside), F32))
                rows.append(jnp.concatenate(cuts, axis=1) if len(cuts) > 1 else cuts[0])
        both = jnp.concatenate(rows, axis=0)
        high = both.astype(BF16).astype(F32)
        spare = jnp.zeros((out_ref.shape[0] - 2 * tokens - 2 * len(rows), wide), F32)
        out_ref[2 * tokens :, :] = jnp.concatenate([high, both - high, spare], axis=0).astype(BF16)
    for copy in copies:
        copy.wait()


def pack(queries, key_vectors, values, strengths, group):
    _, tokens, wide = key_vectors.shape
    width = wide // strengths.shape[1]
    shape = (2 * tokens + beta_rows(tokens, width), wide // group)
    out = pl.pallas_call(
        functools.partial(pack_kernel, group),
        out_shape=[pltpu.VMEM(shape, BF16)] * group
        + [pltpu.VMEM((3, tokens, wide // group), BF16)] * group,
        in_specs=[pl.BlockSpec(memory_space=pltpu.HBM)] * 4,
        out_specs=[VMEM] * (2 * group),
        scratch_shapes=[
            pltpu.VMEM(strengths.shape, F32),
            pltpu.SemaphoreType.DMA((1 + 5 * group,)),
        ],
        compiler_params=PARAMS,
        name="pack",
    )(
        *(
            pltpu.with_memory_space_constraint(array, pltpu.HBM)
            for array in (key_vectors, values, queries, strengths)
        )
    )
    return list(out[:group]), list(out[group:])


def invert_kernel(heads, tokens, *refs):
    key_in, (inverse_ref, table_ref, a_buf) = refs[:-3], refs[-3:]
    width = key_in[0].shape[1] // heads
    chunk = min(CHUNK, tokens)
    per_source = tokens // chunk
    chunks = len(key_in) * per_source
    pieces = max(tokens // width, 1)
    row_time, col_time = times(chunk)
    levels = chunk.bit_length() - 1

    def joins(level):
        same = (row_time >> (level + 1)) == (col_time >> (level + 1))
        return same & (((row_time >> level) & 1) == 1) & (((col_time >> level) & 1) == 0)

    def prepare(head, index):
        lanes = lanes_of(head, width)
        key_ref, first = key_in[index // per_source], (index % per_source) * chunk
        key = woven_key(key_ref, tokens, first, chunk, lanes)
        gram = dot_t(key, key)
        wide_row, wide_col = iota(gram.shape, 0), iota(gram.shape, 1)
        square = jnp.sum(jnp.where(wide_row == wide_col, gram, 0.0), axis=0, keepdims=True)
        scale_row = lax.rsqrt(square + EPS)
        halves = key_ref[2 * tokens :, lanes].astype(F32)
        piece, inside = first // width, first % width

        def strength(reflection):
            high = reflection * pieces + piece
            low = (2 + reflection) * pieces + piece
            both = halves[high : high + 1] + halves[low : low + 1]
            return both[:, inside : inside + chunk]

        beta_row = weave_lanes(strength(0), strength(1))
        both_row = beta_row * scale_row
        table = jnp.concatenate(
            [scale_row, beta_row, both_row, jnp.zeros((5, 2 * chunk), F32)], axis=0
        )
        table_ref[head, index] = table
        system = table.T[:, 2:3] * (gram * scale_row)
        for block in range(2):
            here = slice(block * chunk, (block + 1) * chunk)
            diagonal = system[here, here]
            a_buf[head, index, block] = diagonal
            inverse_ref[head, index, block] = jnp.where(
                row_time == col_time, 1.0, 0.0
            ) - jnp.where(joins(0), diagonal, 0.0)
        inverse_ref[head, index, 2] = system[chunk:, :chunk]

    def solve(units):
        for head, index in units:
            prepare(head, index)
        every = [(head, index, block) for head, index in units for block in range(2)]
        for level in range(1, levels):
            mask = joins(level)
            inner = [
                product3(jnp.where(mask, a_buf[one], 0.0), inverse_ref[one]) for one in every
            ]
            for one, value in zip(every, inner):
                known = inverse_ref[one]
                inverse_ref[one] = known - product3(known, value)
        inner = [
            product3(inverse_ref[head, index, 2], inverse_ref[head, index, 0])
            for head, index in units
        ]
        for (head, index), value in zip(units, inner):
            inverse_ref[head, index, 2] = -product3(inverse_ref[head, index, 1], value)

    every_unit(heads, chunks, solve)


def lanes_of(head, width):
    if isinstance(head, int):
        return slice(head * width, (head + 1) * width)
    return pl.ds(pl.multiple_of(head * width, width), width)


def invert(keys, heads, tokens):
    chunk = min(CHUNK, tokens)
    chunks = len(keys) * tokens // chunk
    return pl.pallas_call(
        functools.partial(invert_kernel, heads, tokens),
        out_shape=(
            pltpu.VMEM((heads, chunks, 3, chunk, chunk), F32),
            pltpu.VMEM((heads, chunks, 8, 2 * chunk), F32),
        ),
        in_specs=[VMEM] * len(keys),
        out_specs=(VMEM, VMEM),
        scratch_shapes=[pltpu.VMEM((heads, chunks, 2, chunk, chunk), F32)],
        compiler_params=PARAMS,
        name="invert",
    )(*held(*keys))


def slot_of(group, index, per_source):
    position = lax.rem(lax.axis_index("seq"), group)
    return place(position, index // per_source) * per_source + index % per_source


def every_unit(heads, chunks, body):
    if heads * chunks <= 8:
        body([(head, index) for head in range(heads) for index in range(chunks)])
    else:

        def one_head(head, carry):
            body([(head, index) for index in range(chunks)])
            return carry

        lax.fori_loop(0, heads, one_head, 0)


def woven_key(key_ref, tokens, first, chunk, lanes):
    return weave(
        key_ref[first : first + chunk, lanes],
        key_ref[tokens + first : tokens + first + chunk, lanes],
    )


def state_kernel(group, parts, *refs):
    key_in, rest_in = refs[:group], refs[group : 2 * group]
    inverse_in = refs[2 * group : 2 * group + parts]
    table_in = refs[2 * group + parts : 2 * group + 2 * parts]
    high_ref, low_ref, step_ref, state_ref, local_ref = refs[2 * group + 2 * parts :]
    heads, per_part, _, chunk, _ = inverse_in[0].shape
    chunks = parts * per_part
    tokens = rest_in[0].shape[1]
    width = rest_in[0].shape[2] // heads
    per_source = tokens // chunk

    def solve(units):
        for head, index in units:
            lanes = lanes_of(head, width)
            part, inside = index // per_part, index % per_part
            source, first = index // per_source, (index % per_source) * chunk
            key_ref, rest_ref = key_in[source], rest_in[source]
            key = woven_key(key_ref, tokens, first, chunk, lanes).astype(F32)
            rows = slice(first, first + chunk)
            value = weave(rest_ref[0, rows, lanes], rest_ref[1, rows, lanes]).astype(F32)
            table = table_in[part][head, inside].T
            inverse = jnp.concatenate(
                [
                    jnp.concatenate(
                        [inverse_in[part][head, inside, 0], jnp.zeros((chunk, chunk), F32)],
                        axis=1,
                    ),
                    jnp.concatenate(
                        [inverse_in[part][head, inside, 2], inverse_in[part][head, inside, 1]],
                        axis=1,
                    ),
                ],
                axis=0,
            )
            right = jnp.concatenate([table[:, 2:3] * key, table[:, 1:2] * value], axis=1)
            high, low = split(table[:, 0:1] * dot3(inverse, *split(right)))
            high_ref[head, index] = high
            low_ref[head, index] = low
        for head, index in units:
            source, first = index // per_source, (index % per_source) * chunk
            turned = woven_key(key_in[source], tokens, first, chunk, lanes_of(head, width)).T
            step_ref[head, slot_of(group, index, per_source)] = dot(
                turned, high_ref[head, index]
            ) + dot(turned, low_ref[head, index])

    every_unit(heads, chunks, solve)
    totals = [[step_ref[head, slot] for slot in range(chunks)] for head in range(heads)]
    while len(totals[0]) > 1:
        totals = [
            [after(one[i], one[i + 1]) for i in range(0, len(one) - 1, 2)]
            + one[len(one) - len(one) % 2 :]
            for one in totals
        ]
    for head, (total,) in enumerate(totals):
        state_ref[head] = total.astype(BF16)
        local_ref[head] = total[:, width:].astype(BF16)


def after(earlier, later):
    width = earlier.shape[0]
    return earlier + later - dot(later[:, :width].astype(BF16), earlier.astype(BF16))


def dot3(left, high, low):
    left_high, left_low = split(left)
    return dot(left_high, high) + dot(left_low, high) + dot(left_high, low)


def carry_state(keys, rests, inverses, tables):
    group, parts = len(keys), len(inverses)
    heads, per_part, _, chunk, _ = inverses[0].shape
    chunks = parts * per_part
    width = rests[0].shape[2] // heads
    solved = pltpu.VMEM((heads, chunks, 2 * chunk, 2 * width), BF16)
    return pl.pallas_call(
        functools.partial(state_kernel, group, parts),
        out_shape=(
            solved,
            solved,
            pltpu.VMEM((heads, chunks, width, 2 * width), F32),
            pltpu.VMEM((heads, width, 2 * width), BF16),
            pltpu.VMEM((heads, width, width), BF16),
        ),
        in_specs=[VMEM] * (2 * group + 2 * parts),
        out_specs=(VMEM,) * 5,
        compiler_params=PARAMS,
        name="carry_state",
    )(*held(*keys, *rests, *inverses, *tables))


def read_kernel(group, *refs):
    key_in, rest_in = refs[:group], refs[group : 2 * group]
    high_ref, low_ref, step_ref, out_ref, lift_ref = refs[2 * group : -3]
    before_buf, local_buf, lift_buf = refs[-3:]
    heads, chunks, wide, _ = high_ref.shape
    chunk = wide // 2
    half = chunk // 2
    tokens = rest_in[0].shape[1]
    width = rest_in[0].shape[2] // heads
    per_source = tokens // chunk
    token_row = iota((chunk, 2 * chunk), 0)
    token_col = iota((chunk, 2 * chunk), 1)
    token_col = (token_col // chunk) * half + lax.rem(token_col, half)

    def answer(units):
        for head, index in units:
            lanes = lanes_of(head, width)
            source, first = index // per_source, (index % per_source) * chunk
            key = woven_key(key_in[source], tokens, first, chunk, lanes)
            query = rest_in[source][2, first : first + chunk, lanes]
            wide_query = query.astype(F32)
            scale = lax.rsqrt(jnp.sum(wide_query * wide_query, axis=1, keepdims=True) + EPS)
            scores = jnp.where(token_col <= token_row, dot_t(query, key) * scale, 0.0)
            applied = dot3(scores, high_ref[head, index], low_ref[head, index])
            local_buf[head, index] = applied[:, width:]
            lift_buf[head, index] = scale * wide_query - applied[:, :width]

    every_unit(heads, chunks, answer)
    totals = [step_ref[head, 0] for head in range(heads)]
    for head in range(heads):
        before_buf[head, 0] = jnp.zeros((width, 2 * width), BF16)
    for slot in range(1, chunks):
        for head in range(heads):
            before_buf[head, slot] = totals[head].astype(BF16)
        if slot + 1 < chunks:
            totals = [after(totals[head], step_ref[head, slot]) for head in range(heads)]

    def correct(units):
        for head, index in units:
            lanes = lanes_of(head, width)
            slot = slot_of(group, index, per_source)
            lifted = lift_buf[head, index]
            moved = dot(lifted.astype(BF16), before_buf[head, slot])
            rows = pl.ds(pl.multiple_of(slot * chunk, chunk), chunk)
            out_ref[rows, lanes] = local_buf[head, index] + moved[:, width:]
            lift_ref[rows, lanes] = (lifted - moved[:, :width]).astype(BF16)

    every_unit(heads, chunks, correct)


def read(keys, rests, high, low, steps):
    group = len(keys)
    _, tokens, wide = rests[0].shape
    chunk, width = high.shape[2] // 2, steps.shape[2]
    return pl.pallas_call(
        functools.partial(read_kernel, group),
        out_shape=(
            pltpu.VMEM((group * tokens, wide), F32),
            pltpu.VMEM((group * tokens, wide), BF16),
        ),
        in_specs=[VMEM] * (2 * group + 3),
        out_specs=(VMEM, VMEM),
        scratch_shapes=[
            pltpu.VMEM(steps.shape, BF16),
            pltpu.VMEM(steps.shape[:2] + (chunk, width), F32),
            pltpu.VMEM(steps.shape[:2] + (chunk, width), F32),
        ],
        compiler_params=PARAMS,
        name="read",
    )(*held(*keys, *rests, high, low, steps))


def join_kernel(count, *refs):
    states, (local_ref, lift_ref, out_ref) = refs[:count], refs[count:]
    heads, width, _ = states[0].shape
    for head in range(heads):
        lanes = slice(head * width, (head + 1) * width)
        total = None
        for state in reversed(states):
            if total is None:
                total = state[head].astype(F32)
            else:
                step = state[head].astype(F32)
                total = (
                    total + step[:, width:] - dot(state[head, :, :width], total.astype(BF16))
                )
        out_ref[:, lanes] = (
            local_ref[:, lanes] + dot(lift_ref[:, lanes], total.astype(BF16))
        ).astype(BF16)


def join(states, local, lifted):
    return pl.pallas_call(
        functools.partial(join_kernel, len(states)),
        out_shape=pltpu.VMEM(local.shape, BF16),
        in_specs=[VMEM] * (len(states) + 2),
        out_specs=VMEM,
        compiler_params=PARAMS,
        name="join",
    )(*held(*states, local, lifted))


def compose(earlier, later):
    width = earlier.shape[1]
    moved = jnp.einsum("hab,hbc->hac", later[:, :, :width], earlier, preferred_element_type=F32)
    return (earlier.astype(F32) + later.astype(F32) - moved).astype(BF16)


def weight_rows(weights, offset, inner, first, count):
    rows = pl.ds(first, count)
    if offset == 2:
        return jnp.where(inner, weights[3][rows, :], weights[4][rows, :])
    return weights[{0: 0, 1: 1, 3: 2}[offset]][rows, :]


def where_am_i(group):
    device = lax.axis_index("seq")
    return lax.rem(device, group), device // group


def target_rows(source, group, targets):
    position, _ = where_am_i(group)
    tokens = source.shape[0] // group
    firsts = [pl.multiple_of(place(position, t) * tokens, tokens) for t in targets]
    return jnp.concatenate([source[pl.ds(first, tokens), :] for first in firsts], axis=0)


def begin_kernel(group, halves, early, *refs):
    heads_in, weight_in, totals = refs[: len(early[0])], refs[len(early[0]) : -2], refs[-2:]
    position, _ = where_am_i(group)
    wide = heads_in[0].shape[1]
    columns = weight_in[0].shape[1]
    for targets, total_ref in zip(halves, totals):
        for number, offset in enumerate(early[1]):
            total = None
            for member, source in zip(early[0], heads_in):
                first = pl.multiple_of(place(position, member) * wide, wide)
                part = dot(
                    target_rows(source, group, targets),
                    weight_rows(weight_in, offset, None, first, wide),
                )
                total = part if total is None else total + part
            total_ref[:, number * columns : (number + 1) * columns] = total


def project_kernel(group, targets, early, offsets, *refs):
    heads_in, weight_in = refs[:group], refs[group:-3]
    total_ref, send_ref, keep_ref = refs[-3:]
    core = lax.axis_index("head")
    position, plane = where_am_i(group)
    wide = heads_in[0].shape[1]
    columns = weight_in[0].shape[1]
    side = keep_ref.shape[1] // columns
    inner = (plane == 1) | (plane == 2)
    for offset in offsets:
        owner = jnp.bitwise_xor(plane, offset)
        total = None
        members = range(group)
        if offset in early[1]:
            number = early[1].index(offset)
            members = [member for member in members if member not in early[0]]
        for member in members:
            first = pl.multiple_of(place(position, member) * wide, wide)
            part = dot(
                target_rows(heads_in[member], group, targets),
                weight_rows(weight_in, offset, inner, first, wide),
            )
            total = part if total is None else total + part
        if offset in early[1]:
            total = total + total_ref[:, number * columns : (number + 1) * columns]
        result = total.astype(BF16)
        lanes = pl.ds(pl.multiple_of(lax.rem(owner, side) * columns, columns), columns)

        @pl.when(owner // side == core)
        def _():
            keep_ref[:, lanes] = result

        @pl.when(owner // side != core)
        def _():
            send_ref[:, lanes] = result


def begin_projection(heads, weights, halves, early):
    group = len(heads)
    tokens = heads[0].shape[0] // group
    columns = weights[0].shape[1]
    here = [heads[member] for member in early[0]] + list(weights[: len(early[1])])
    return pl.pallas_call(
        functools.partial(begin_kernel, group, halves, early),
        out_shape=[
            pltpu.VMEM((tokens * len(targets), columns * len(early[1])), F32)
            for targets in halves
        ],
        in_specs=[VMEM] * len(here),
        out_specs=[VMEM] * 2,
        compiler_params=PARAMS,
        name="begin_projection",
    )(*held(*here))


def project(heads, weights, planes, targets, early, total):
    group = len(heads)
    rows = heads[0].shape[0] // group * len(targets)
    columns = weights[0].shape[1]
    offsets = (0, 1, 3, 2) if planes == 4 else (0, 1)
    shape = pltpu.VMEM((rows, columns * planes // 2), BF16)
    return pl.pallas_call(
        functools.partial(project_kernel, group, targets, early, offsets),
        out_shape=(shape, shape),
        in_specs=[VMEM] * (group + len(weights) + 1),
        out_specs=(VMEM, VMEM),
        compiler_params=PARAMS,
        name="project",
    )(*held(*heads, *weights, total))


def sum_kernel(keep_ref, other_ref, *outs):
    tokens = outs[0].shape[0]
    for index, out_ref in enumerate(outs):
        rows = slice(index * tokens, (index + 1) * tokens)
        out_ref[...] = (keep_ref[rows, :].astype(F32) + other_ref[rows, :].astype(F32)).astype(
            BF16
        )


def sum_parts(keep, other, count):
    rows, columns = keep.shape
    return pl.pallas_call(
        sum_kernel,
        out_shape=[pltpu.VMEM((rows // count, columns), BF16)] * count,
        in_specs=[VMEM, VMEM],
        out_specs=[VMEM] * count,
        compiler_params=PARAMS,
        name="sum_parts",
    )(*held(keep, other))


def lay_kernel(group, columns, *refs):
    parts, out_ref, sems = refs[:group], refs[group], refs[group + 1]
    position = lax.rem(lax.axis_index("seq"), group)
    copies = []
    for offset in range(group):
        for index in range(parts[0].shape[1] // columns):
            first = (index * group + place(position, offset)) * columns
            copies.append(
                pltpu.make_async_copy(
                    parts[offset].at[:, index * columns : (index + 1) * columns],
                    out_ref.at[:, pl.ds(pl.multiple_of(first, columns), columns)],
                    sems.at[len(copies)],
                )
            )
    for copy in copies:
        copy.start()
    for copy in copies:
        copy.wait()


def lay_out(parts, columns):
    group = len(parts)
    rows, wide = parts[0].shape
    return pl.pallas_call(
        functools.partial(lay_kernel, group, columns),
        out_shape=jax.ShapeDtypeStruct((rows, group * wide), BF16),
        in_specs=[VMEM] * group,
        out_specs=pl.BlockSpec(memory_space=pl.ANY),
        scratch_shapes=[pltpu.SemaphoreType.DMA((group * wide // columns,))],
        compiler_params=PARAMS,
        name="lay_out",
    )(*held(*parts))


def swap(value, group, offset, count):
    pairs = [(i, (i // group) * group + ((i % group) ^ offset)) for i in range(count)]
    return lax.ppermute(value, "seq", pairs)


def per_device(queries, key_vectors, values, strengths, out_weight):
    count = lax.axis_size("seq")
    sides = lax.axis_size("head")
    heads = strengths.shape[1]
    tokens = queries.shape[0]
    width = queries.shape[1] // heads
    group = 1
    while group < 4 and heads % (2 * group) == 0 and count % (2 * group) == 0:
        group *= 2
    planes = count // group
    position = lax.axis_index("seq") % group
    mine = heads // group
    keys, rests = pack(queries, key_vectors, values, strengths, group)
    for offset in range(1, group):
        keys[offset] = swap(keys[offset], group, offset, count)
        rests[offset] = swap(rests[offset], group, offset, count)

    def between_planes(value, pairs):
        return lax.ppermute(
            value,
            "seq",
            [
                (source * group + i, target * group + i)
                for source, target in pairs
                for i in range(group)
            ],
        )

    split_out = sides == 2 and planes in (2, 4) and group > 1
    weights = [out_weight]
    if split_out:
        for offset in range(1, planes, 2):
            swapped = [(plane, plane ^ offset) for plane in range(planes)]
            weights.append(between_planes(out_weight, swapped))

    near = max(group // 2, 1)
    solved = []
    for part in (keys[:near], keys[near:]):
        if part:
            solved.append(invert(part, mine, tokens))
    inverses, tables = zip(*solved)
    high, low, steps, state, local_state = carry_state(keys, rests, inverses, tables)
    local, lifted = read(keys, rests, high, low, steps)

    def from_earlier(value, distance):
        pairs = [(i, i + distance * group) for i in range(count - distance * group)]
        return lax.ppermute(value, "seq", pairs)

    if planes <= 4:
        states = []
        for distance in range(1, planes):
            sent = state if distance + 1 < planes else local_state
            states.append(from_earlier(sent, distance))
    else:
        total = from_earlier(state, 1)
        distance = 1
        while distance < planes - 1:
            total = compose(from_earlier(total, distance), total)
            distance *= 2
        states = [total[:, :, width:]]
    if split_out and planes == 4:
        weights += [
            between_planes(weights[1], ((1, 2), (2, 1))),
            between_planes(weights[2], ((1, 0), (2, 3))),
        ]

    mixed_heads = join(states, local, lifted)

    if split_out:
        order = tuple(range(1, group)) + (0,)
        row_halves = (order[: group // 2], order[group // 2 :])
        early = (tuple(range(group - 1)), (0, 1, 3) if planes == 4 else (0, 1))
        parts = [None] * group
        gathered = [mixed_heads]
        for offset in range(1, group):
            gathered.append(swap(mixed_heads, group, offset, count))
        totals = begin_projection(gathered, weights, row_halves, early)
        halves = []
        for targets, total in zip(row_halves, totals):
            send, keep = project(gathered, weights, planes, targets, early, total)
            other = lax.ppermute(send, "head", [(0, 1), (1, 0)])
            halves.append((targets, keep, other))
        for targets, keep, other in halves:
            for offset, part in zip(targets, sum_parts(keep, other, len(targets))):
                parts[offset] = swap(part, group, offset, count) if offset else part
        return lay_out(parts, out_weight.shape[1])

    if group > 1:
        position_rows = []
        for offset in range(group):
            first = jnp.bitwise_xor(position, offset) * tokens
            part = lax.dynamic_slice_in_dim(mixed_heads, first, tokens, 0)
            position_rows.append(swap(part, group, offset, count) if offset else part)
        stacked = jnp.stack(position_rows)
        order = jnp.bitwise_xor(position, jnp.arange(group))
        stacked = jnp.take(stacked, order, axis=0)
        mixed_heads = jnp.swapaxes(stacked, 0, 1).reshape(tokens, heads * width)
    partial_sums = jnp.dot(
        mixed_heads,
        lax.all_gather(out_weight, "seq", axis=1, tiled=True),
        preferred_element_type=F32,
    )
    return lax.psum_scatter(
        partial_sums.astype(BF16), "head", scatter_dimension=1, tiled=True
    )


def solution(mesh):
    return jax.shard_map(
        per_device,
        mesh=mesh,
        in_specs=(
            P("seq", "head"),
            P(None, "seq", "head"),
            P(None, "seq", "head"),
            P(None, "head", "seq"),
            P("head", "seq"),
        ),
        out_specs=P("seq", "head"),
        check_vma=False,
    )
```

```python
import functools

import jax
import jax.numpy as jnp
from jax import lax
from jax.experimental import pallas as pl
from jax.experimental.pallas import tpu as pltpu
from jax.sharding import PartitionSpec as P


CHUNK = 128
EPS = 1e-06
F32 = jnp.float32
BF16 = jnp.bfloat16


def dot(a, b):
    return jnp.dot(a, b, preferred_element_type=F32)


def dot_t(a, b):
    return lax.dot_general(a, b, (((1,), (1,)), ((), ())), preferred_element_type=F32)


def split(x):
    high = x.astype(BF16)
    return high, (x - high.astype(F32)).astype(BF16)


def product3(left, right):
    left_high, left_low = split(left)
    right_high, right_low = split(right)
    lhs = jnp.concatenate([left_high, left_low], axis=1)
    rhs = jnp.concatenate(
        [
            jnp.concatenate([right_high, right_low], axis=1),
            jnp.concatenate([right_high, jnp.zeros_like(right_low)], axis=1),
        ],
        axis=0,
    )
    wide = dot(lhs, rhs)
    width = right.shape[1]
    return wide[:, :width] + wide[:, width:]


def iota(shape, axis):
    return lax.broadcasted_iota(jnp.int32, shape, axis)


def weave(first, second):
    half = first.shape[0] // 2
    return jnp.concatenate([first[:half], second[:half], first[half:], second[half:]], axis=0)


def weave_lanes(first, second):
    half = first.shape[1] // 2
    return jnp.concatenate(
        [first[:, :half], second[:, :half], first[:, half:], second[:, half:]], axis=1
    )


def place(position, offset):
    return jnp.bitwise_xor(position, offset)


VMEM = pl.BlockSpec(memory_space=pltpu.VMEM)
PARAMS = pltpu.CompilerParams(vmem_limit_bytes=12 * 2**20)


def held(*arrays):
    return [pltpu.with_memory_space_constraint(array, pltpu.VMEM) for array in arrays]


def times(chunk):
    half = chunk // 2
    row, col = iota((chunk, chunk), 0), iota((chunk, chunk), 1)
    return 2 * lax.rem(row, half) + row // half, 2 * lax.rem(col, half) + col // half


def beta_rows(tokens, width):
    return -(-4 * max(tokens // width, 1) // 16) * 16


def pack_kernel(group, key_ref, value_ref, query_ref, strength_ref, *refs):
    key_outs, rest_outs, (beta_ref, sems) = refs[:group], refs[group : 2 * group], refs[-2:]
    _, heads, tokens = beta_ref.shape
    mine = heads // group
    wide = key_outs[0].shape[1]
    width = wide // mine
    pieces = max(tokens // width, 1)
    inside = tokens // pieces
    position, _ = where_am_i(group)
    first_copy = pltpu.make_async_copy(strength_ref, beta_ref, sems.at[0])
    pairs = []
    for offset in range(group):
        lanes = pl.ds(pl.multiple_of(place(position, offset) * wide, wide), wide)
        for reflection in range(2):
            rows = pl.ds(reflection * tokens, tokens)
            pairs.append((key_ref.at[reflection, :, lanes], key_outs[offset].at[rows, :]))
    for offset in range(group):
        lanes = pl.ds(pl.multiple_of(place(position, offset) * wide, wide), wide)
        for reflection in range(2):
            pairs.append(
                (value_ref.at[reflection, :, lanes], rest_outs[offset].at[reflection])
            )
        pairs.append((query_ref.at[:, lanes], rest_outs[offset].at[2]))
    copies = [
        pltpu.make_async_copy(source, target, sems.at[1 + number])
        for number, (source, target) in enumerate(pairs)
    ]
    first_copy.start()
    for copy in copies:
        copy.start()
    first_copy.wait()
    for offset, out_ref in enumerate(key_outs):
        member = place(position, offset)
        rows = []
        for reflection in range(2):
            for piece in range(pieces):
                cuts = []
                for head in range(mine):
                    cut = beta_ref[reflection, pl.ds(member * mine + head, 1), :]
                    cuts.append(cut[:, piece * inside : (piece + 1) * inside])
                    if inside < width:
                        cuts.append(jnp.zeros((1, width - inside), F32))
                rows.append(jnp.concatenate(cuts, axis=1) if len(cuts) > 1 else cuts[0])
        both = jnp.concatenate(rows, axis=0)
        high = both.astype(BF16).astype(F32)
        spare = jnp.zeros((out_ref.shape[0] - 2 * tokens - 2 * len(rows), wide), F32)
        out_ref[2 * tokens :, :] = jnp.concatenate([high, both - high, spare], axis=0).astype(BF16)
    for copy in copies:
        copy.wait()


def pack(queries, key_vectors, values, strengths, group):
    _, tokens, wide = key_vectors.shape
    width = wide // strengths.shape[1]
    shape = (2 * tokens + beta_rows(tokens, width), wide // group)
    out = pl.pallas_call(
        functools.partial(pack_kernel, group),
        out_shape=[pltpu.VMEM(shape, BF16)] * group
        + [pltpu.VMEM((3, tokens, wide // group), BF16)] * group,
        in_specs=[pl.BlockSpec(memory_space=pltpu.HBM)] * 4,
        out_specs=[VMEM] * (2 * group),
        scratch_shapes=[
            pltpu.VMEM(strengths.shape, F32),
            pltpu.SemaphoreType.DMA((1 + 5 * group,)),
        ],
        compiler_params=PARAMS,
        name="pack",
    )(
        *(
            pltpu.with_memory_space_constraint(array, pltpu.HBM)
            for array in (key_vectors, values, queries, strengths)
        )
    )
    return list(out[:group]), list(out[group:])


def invert_kernel(heads, tokens, *refs):
    key_in, (inverse_ref, table_ref, a_buf) = refs[:-3], refs[-3:]
    width = key_in[0].shape[1] // heads
    chunk = min(CHUNK, tokens)
    per_source = tokens // chunk
    chunks = len(key_in) * per_source
    pieces = max(tokens // width, 1)
    row_time, col_time = times(chunk)
    levels = chunk.bit_length() - 1

    def joins(level):
        same = (row_time >> (level + 1)) == (col_time >> (level + 1))
        return same & (((row_time >> level) & 1) == 1) & (((col_time >> level) & 1) == 0)

    def prepare(head, index):
        lanes = lanes_of(head, width)
        key_ref, first = key_in[index // per_source], (index % per_source) * chunk
        key = woven_key(key_ref, tokens, first, chunk, lanes)
        gram = dot_t(key, key)
        wide_row, wide_col = iota(gram.shape, 0), iota(gram.shape, 1)
        square = jnp.sum(jnp.where(wide_row == wide_col, gram, 0.0), axis=0, keepdims=True)
        scale_row = lax.rsqrt(square + EPS)
        halves = key_ref[2 * tokens :, lanes].astype(F32)
        piece, inside = first // width, first % width

        def strength(reflection):
            high = reflection * pieces + piece
            low = (2 + reflection) * pieces + piece
            both = halves[high : high + 1] + halves[low : low + 1]
            return both[:, inside : inside + chunk]

        beta_row = weave_lanes(strength(0), strength(1))
        both_row = beta_row * scale_row
        table = jnp.concatenate(
            [scale_row, beta_row, both_row, jnp.zeros((5, 2 * chunk), F32)], axis=0
        )
        table_ref[head, index] = table
        system = table.T[:, 2:3] * (gram * scale_row)
        for block in range(2):
            here = slice(block * chunk, (block + 1) * chunk)
            diagonal = system[here, here]
            a_buf[head, index, block] = diagonal
            inverse_ref[head, index, block] = jnp.where(
                row_time == col_time, 1.0, 0.0
            ) - jnp.where(joins(0), diagonal, 0.0)
        inverse_ref[head, index, 2] = system[chunk:, :chunk]

    def solve(units):
        for head, index in units:
            prepare(head, index)
        every = [(head, index, block) for head, index in units for block in range(2)]
        for level in range(1, levels):
            mask = joins(level)
            inner = [
                product3(jnp.where(mask, a_buf[one], 0.0), inverse_ref[one]) for one in every
            ]
            for one, value in zip(every, inner):
                known = inverse_ref[one]
                inverse_ref[one] = known - product3(known, value)
        inner = [
            product3(inverse_ref[head, index, 2], inverse_ref[head, index, 0])
            for head, index in units
        ]
        for (head, index), value in zip(units, inner):
            inverse_ref[head, index, 2] = -product3(inverse_ref[head, index, 1], value)

    every_unit(heads, chunks, solve)


def lanes_of(head, width):
    if isinstance(head, int):
        return slice(head * width, (head + 1) * width)
    return pl.ds(pl.multiple_of(head * width, width), width)


def invert(keys, heads, tokens):
    chunk = min(CHUNK, tokens)
    chunks = len(keys) * tokens // chunk
    return pl.pallas_call(
        functools.partial(invert_kernel, heads, tokens),
        out_shape=(
            pltpu.VMEM((heads, chunks, 3, chunk, chunk), F32),
            pltpu.VMEM((heads, chunks, 8, 2 * chunk), F32),
        ),
        in_specs=[VMEM] * len(keys),
        out_specs=(VMEM, VMEM),
        scratch_shapes=[pltpu.VMEM((heads, chunks, 2, chunk, chunk), F32)],
        compiler_params=PARAMS,
        name="invert",
    )(*held(*keys))


def slot_of(group, index, per_source):
    position = lax.rem(lax.axis_index("seq"), group)
    return place(position, index // per_source) * per_source + index % per_source


def every_unit(heads, chunks, body):
    if heads * chunks <= 8:
        body([(head, index) for head in range(heads) for index in range(chunks)])
    else:

        def one_head(head, carry):
            body([(head, index) for index in range(chunks)])
            return carry

        lax.fori_loop(0, heads, one_head, 0)


def woven_key(key_ref, tokens, first, chunk, lanes):
    return weave(
        key_ref[first : first + chunk, lanes],
        key_ref[tokens + first : tokens + first + chunk, lanes],
    )


def state_kernel(group, parts, *refs):
    key_in, rest_in = refs[:group], refs[group : 2 * group]
    inverse_in = refs[2 * group : 2 * group + parts]
    table_in = refs[2 * group + parts : 2 * group + 2 * parts]
    high_ref, low_ref, step_ref, state_ref, local_ref = refs[2 * group + 2 * parts :]
    heads, per_part, _, chunk, _ = inverse_in[0].shape
    chunks = parts * per_part
    tokens = rest_in[0].shape[1]
    width = rest_in[0].shape[2] // heads
    per_source = tokens // chunk

    def solve(units):
        for head, index in units:
            lanes = lanes_of(head, width)
            part, inside = index // per_part, index % per_part
            source, first = index // per_source, (index % per_source) * chunk
            key_ref, rest_ref = key_in[source], rest_in[source]
            key = woven_key(key_ref, tokens, first, chunk, lanes).astype(F32)
            rows = slice(first, first + chunk)
            value = weave(rest_ref[0, rows, lanes], rest_ref[1, rows, lanes]).astype(F32)
            table = table_in[part][head, inside].T
            inverse = jnp.concatenate(
                [
                    jnp.concatenate(
                        [inverse_in[part][head, inside, 0], jnp.zeros((chunk, chunk), F32)],
                        axis=1,
                    ),
                    jnp.concatenate(
                        [inverse_in[part][head, inside, 2], inverse_in[part][head, inside, 1]],
                        axis=1,
                    ),
                ],
                axis=0,
            )
            right = jnp.concatenate([table[:, 2:3] * key, table[:, 1:2] * value], axis=1)
            high, low = split(table[:, 0:1] * dot3(inverse, *split(right)))
            high_ref[head, index] = high
            low_ref[head, index] = low
        for head, index in units:
            source, first = index // per_source, (index % per_source) * chunk
            turned = woven_key(key_in[source], tokens, first, chunk, lanes_of(head, width)).T
            step_ref[head, slot_of(group, index, per_source)] = dot(
                turned, high_ref[head, index]
            ) + dot(turned, low_ref[head, index])

    every_unit(heads, chunks, solve)
    totals = [[step_ref[head, slot] for slot in range(chunks)] for head in range(heads)]
    while len(totals[0]) > 1:
        totals = [
            [after(one[i], one[i + 1]) for i in range(0, len(one) - 1, 2)]
            + one[len(one) - len(one) % 2 :]
            for one in totals
        ]
    for head, (total,) in enumerate(totals):
        state_ref[head] = total.astype(BF16)
        local_ref[head] = total[:, width:].astype(BF16)


def after(earlier, later):
    width = earlier.shape[0]
    return earlier + later - dot(later[:, :width].astype(BF16), earlier.astype(BF16))


def dot3(left, high, low):
    left_high, left_low = split(left)
    return dot(left_high, high) + dot(left_low, high) + dot(left_high, low)


def carry_state(keys, rests, inverses, tables):
    group, parts = len(keys), len(inverses)
    heads, per_part, _, chunk, _ = inverses[0].shape
    chunks = parts * per_part
    width = rests[0].shape[2] // heads
    solved = pltpu.VMEM((heads, chunks, 2 * chunk, 2 * width), BF16)
    return pl.pallas_call(
        functools.partial(state_kernel, group, parts),
        out_shape=(
            solved,
            solved,
            pltpu.VMEM((heads, chunks, width, 2 * width), F32),
            pltpu.VMEM((heads, width, 2 * width), BF16),
            pltpu.VMEM((heads, width, width), BF16),
        ),
        in_specs=[VMEM] * (2 * group + 2 * parts),
        out_specs=(VMEM,) * 5,
        compiler_params=PARAMS,
        name="carry_state",
    )(*held(*keys, *rests, *inverses, *tables))


def read_kernel(group, *refs):
    key_in, rest_in = refs[:group], refs[group : 2 * group]
    high_ref, low_ref, step_ref, out_ref, lift_ref = refs[2 * group : -3]
    before_buf, local_buf, lift_buf = refs[-3:]
    heads, chunks, wide, _ = high_ref.shape
    chunk = wide // 2
    half = chunk // 2
    tokens = rest_in[0].shape[1]
    width = rest_in[0].shape[2] // heads
    per_source = tokens // chunk
    token_row = iota((chunk, 2 * chunk), 0)
    token_col = iota((chunk, 2 * chunk), 1)
    token_col = (token_col // chunk) * half + lax.rem(token_col, half)

    def answer(units):
        for head, index in units:
            lanes = lanes_of(head, width)
            source, first = index // per_source, (index % per_source) * chunk
            key = woven_key(key_in[source], tokens, first, chunk, lanes)
            query = rest_in[source][2, first : first + chunk, lanes]
            wide_query = query.astype(F32)
            scale = lax.rsqrt(jnp.sum(wide_query * wide_query, axis=1, keepdims=True) + EPS)
            scores = jnp.where(token_col <= token_row, dot_t(query, key) * scale, 0.0)
            applied = dot3(scores, high_ref[head, index], low_ref[head, index])
            local_buf[head, index] = applied[:, width:]
            lift_buf[head, index] = scale * wide_query - applied[:, :width]

    every_unit(heads, chunks, answer)
    totals = [step_ref[head, 0] for head in range(heads)]
    for head in range(heads):
        before_buf[head, 0] = jnp.zeros((width, 2 * width), BF16)
    for slot in range(1, chunks):
        for head in range(heads):
            before_buf[head, slot] = totals[head].astype(BF16)
        if slot + 1 < chunks:
            totals = [after(totals[head], step_ref[head, slot]) for head in range(heads)]

    def correct(units):
        for head, index in units:
            lanes = lanes_of(head, width)
            slot = slot_of(group, index, per_source)
            lifted = lift_buf[head, index]
            moved = dot(lifted.astype(BF16), before_buf[head, slot])
            rows = pl.ds(pl.multiple_of(slot * chunk, chunk), chunk)
            out_ref[rows, lanes] = local_buf[head, index] + moved[:, width:]
            lift_ref[rows, lanes] = (lifted - moved[:, :width]).astype(BF16)

    every_unit(heads, chunks, correct)


def read(keys, rests, high, low, steps):
    group = len(keys)
    _, tokens, wide = rests[0].shape
    chunk, width = high.shape[2] // 2, steps.shape[2]
    return pl.pallas_call(
        functools.partial(read_kernel, group),
        out_shape=(
            pltpu.VMEM((group * tokens, wide), F32),
            pltpu.VMEM((group * tokens, wide), BF16),
        ),
        in_specs=[VMEM] * (2 * group + 3),
        out_specs=(VMEM, VMEM),
        scratch_shapes=[
            pltpu.VMEM(steps.shape, BF16),
            pltpu.VMEM(steps.shape[:2] + (chunk, width), F32),
            pltpu.VMEM(steps.shape[:2] + (chunk, width), F32),
        ],
        compiler_params=PARAMS,
        name="read",
    )(*held(*keys, *rests, high, low, steps))


def join_kernel(count, splits, *refs):
    states, (local_ref, lift_ref), outs = refs[:count], refs[count : count + 2], refs[count + 2 :]
    heads, width, _ = states[0].shape
    group = sum(len(split) for split in splits)
    tokens = local_ref.shape[0] // group
    position, _ = where_am_i(group)
    for head in range(heads):
        lanes = slice(head * width, (head + 1) * width)
        total = None
        for state in reversed(states):
            if total is None:
                total = state[head].astype(F32)
            else:
                step = state[head].astype(F32)
                total = (
                    total + step[:, width:] - dot(state[head, :, :width], total.astype(BF16))
                )
        total = total.astype(BF16)
        for split_of, out_ref in zip(splits, outs):
            for number, offset in enumerate(split_of):
                rows = pl.ds(pl.multiple_of(place(position, offset) * tokens, tokens), tokens)
                out_ref[number * tokens : (number + 1) * tokens, lanes] = (
                    local_ref[rows, lanes] + dot(lift_ref[rows, lanes], total)
                ).astype(BF16)


def join(states, local, lifted, splits):
    group = sum(len(split) for split in splits)
    rows, wide = local.shape
    return pl.pallas_call(
        functools.partial(join_kernel, len(states), splits),
        out_shape=[pltpu.VMEM((rows // group * len(split), wide), BF16) for split in splits],
        in_specs=[VMEM] * (len(states) + 2),
        out_specs=[VMEM] * len(splits),
        compiler_params=PARAMS,
        name="join",
    )(*held(*states, local, lifted))


def compose(earlier, later):
    width = earlier.shape[1]
    moved = jnp.einsum("hab,hbc->hac", later[:, :, :width], earlier, preferred_element_type=F32)
    return (earlier.astype(F32) + later.astype(F32) - moved).astype(BF16)


def weight_rows(weights, offset, inner, first, count):
    rows = pl.ds(first, count)
    if offset == 2:
        return jnp.where(inner, weights[3][rows, :], weights[4][rows, :])
    return weights[{0: 0, 1: 1, 3: 2}[offset]][rows, :]


def where_am_i(group):
    device = lax.axis_index("seq")
    return lax.rem(device, group), device // group


def project_kernel(group, orders, offsets, *refs):
    heads_in, weight_in, (send_ref, keep_ref) = refs[:group], refs[group:-2], refs[-2:]
    core = lax.axis_index("head")
    position, plane = where_am_i(group)
    rows, wide = heads_in[0].shape
    tokens = rows // len(orders[0])
    columns = weight_in[0].shape[1]
    side = keep_ref.shape[1] // columns
    inner = (plane == 1) | (plane == 2)
    for offset in offsets:
        owner = jnp.bitwise_xor(plane, offset)
        total = None
        for member in range(group):
            first = pl.multiple_of(place(position, member) * wide, wide)
            blocks = [
                heads_in[member][at * tokens : (at + 1) * tokens, :] for at in orders[member]
            ]
            part = dot(
                jnp.concatenate(blocks, axis=0),
                weight_rows(weight_in, offset, inner, first, wide),
            )
            total = part if total is None else total + part
        result = total.astype(BF16)
        lanes = pl.ds(pl.multiple_of(lax.rem(owner, side) * columns, columns), columns)

        @pl.when(owner // side == core)
        def _():
            keep_ref[:, lanes] = result

        @pl.when(owner // side != core)
        def _():
            send_ref[:, lanes] = result


def project(heads, weights, planes, orders):
    group = len(heads)
    rows = heads[0].shape[0]
    columns = weights[0].shape[1]
    offsets = (0, 1, 3, 2) if planes == 4 else (0, 1)
    shape = pltpu.VMEM((rows, columns * planes // 2), BF16)
    return pl.pallas_call(
        functools.partial(project_kernel, group, orders, offsets),
        out_shape=(shape, shape),
        in_specs=[VMEM] * (group + len(weights)),
        out_specs=(VMEM, VMEM),
        compiler_params=PARAMS,
        name="project",
    )(*held(*heads, *weights))


def sum_kernel(keep_ref, other_ref, *outs):
    tokens = outs[0].shape[0]
    for index, out_ref in enumerate(outs):
        rows = slice(index * tokens, (index + 1) * tokens)
        out_ref[...] = (keep_ref[rows, :].astype(F32) + other_ref[rows, :].astype(F32)).astype(
            BF16
        )


def sum_parts(keep, other, count):
    rows, columns = keep.shape
    return pl.pallas_call(
        sum_kernel,
        out_shape=[pltpu.VMEM((rows // count, columns), BF16)] * count,
        in_specs=[VMEM, VMEM],
        out_specs=[VMEM] * count,
        compiler_params=PARAMS,
        name="sum_parts",
    )(*held(keep, other))


def lay_kernel(group, columns, *refs):
    parts, out_ref, sems = refs[:group], refs[group], refs[group + 1]
    position = lax.rem(lax.axis_index("seq"), group)
    copies = []
    for offset in range(group):
        for index in range(parts[0].shape[1] // columns):
            first = (index * group + place(position, offset)) * columns
            copies.append(
                pltpu.make_async_copy(
                    parts[offset].at[:, index * columns : (index + 1) * columns],
                    out_ref.at[:, pl.ds(pl.multiple_of(first, columns), columns)],
                    sems.at[len(copies)],
                )
            )
    for copy in copies:
        copy.start()
    for copy in copies:
        copy.wait()


def lay_out(parts, columns):
    group = len(parts)
    rows, wide = parts[0].shape
    return pl.pallas_call(
        functools.partial(lay_kernel, group, columns),
        out_shape=jax.ShapeDtypeStruct((rows, group * wide), BF16),
        in_specs=[VMEM] * group,
        out_specs=pl.BlockSpec(memory_space=pl.ANY),
        scratch_shapes=[pltpu.SemaphoreType.DMA((group * wide // columns,))],
        compiler_params=PARAMS,
        name="lay_out",
    )(*held(*parts))


def swap(value, group, offset, count):
    pairs = [(i, (i // group) * group + ((i % group) ^ offset)) for i in range(count)]
    return lax.ppermute(value, "seq", pairs)


def per_device(queries, key_vectors, values, strengths, out_weight):
    count = lax.axis_size("seq")
    sides = lax.axis_size("head")
    heads = strengths.shape[1]
    tokens = queries.shape[0]
    width = queries.shape[1] // heads
    group = 1
    while group < 4 and heads % (2 * group) == 0 and count % (2 * group) == 0:
        group *= 2
    planes = count // group
    position = lax.axis_index("seq") % group
    mine = heads // group
    keys, rests = pack(queries, key_vectors, values, strengths, group)
    for offset in range(1, group):
        keys[offset] = swap(keys[offset], group, offset, count)
        rests[offset] = swap(rests[offset], group, offset, count)

    def between_planes(value, pairs):
        return lax.ppermute(
            value,
            "seq",
            [
                (source * group + i, target * group + i)
                for source, target in pairs
                for i in range(group)
            ],
        )

    split_out = sides == 2 and planes in (2, 4) and group > 1
    weights = [out_weight]
    if split_out:
        for offset in range(1, planes, 2):
            swapped = [(plane, plane ^ offset) for plane in range(planes)]
            weights.append(between_planes(out_weight, swapped))

    near = max(group // 2, 1)
    solved = []
    for part in (keys[:near], keys[near:]):
        if part:
            solved.append(invert(part, mine, tokens))
    inverses, tables = zip(*solved)
    high, low, steps, state, local_state = carry_state(keys, rests, inverses, tables)
    local, lifted = read(keys, rests, high, low, steps)

    def from_earlier(value, distance):
        pairs = [(i, i + distance * group) for i in range(count - distance * group)]
        return lax.ppermute(value, "seq", pairs)

    if planes <= 4:
        states = []
        for distance in range(1, planes):
            sent = state if distance + 1 < planes else local_state
            states.append(from_earlier(sent, distance))
    else:
        total = from_earlier(state, 1)
        distance = 1
        while distance < planes - 1:
            total = compose(from_earlier(total, distance), total)
            distance *= 2
        states = [total[:, :, width:]]
    if split_out and planes == 4:
        weights += [
            between_planes(weights[1], ((1, 2), (2, 1))),
            between_planes(weights[2], ((1, 0), (2, 3))),
        ]

    if split_out:
        row_halves = ((3, 1), (2, 0)) if group == 4 else ((1,), (0,))
        ready = join(states, local, lifted, row_halves)
        parts = [None] * group
        gathered, orders = [], []
        for targets in row_halves:
            arrays, order = [], []
            for offset in range(group):
                seen = [target ^ offset for target in targets]
                source = row_halves.index(
                    next(half for half in row_halves if set(half) == set(seen))
                )
                order.append(tuple(row_halves[source].index(block) for block in seen))
                array = ready[source]
                if offset:
                    array = swap(array, group, offset, count)
                arrays.append(array)
            gathered.append(arrays)
            orders.append(tuple(order))
        for number, targets in enumerate(row_halves):
            send, keep = project(gathered[number], weights, planes, orders[number])
            other = lax.ppermute(send, "head", [(0, 1), (1, 0)])
            for offset, part in zip(targets, sum_parts(keep, other, len(targets))):
                parts[offset] = swap(part, group, offset, count) if offset else part
        return lay_out(parts, out_weight.shape[1])

    (mixed_heads,) = join(states, local, lifted, (tuple(range(group)),))
    if group > 1:
        position_rows = []
        for offset in range(group):
            part = lax.dynamic_slice_in_dim(mixed_heads, offset * tokens, tokens, 0)
            position_rows.append(swap(part, group, offset, count) if offset else part)
        stacked = jnp.stack(position_rows)
        order = jnp.bitwise_xor(position, jnp.arange(group))
        stacked = jnp.take(stacked, order, axis=0)
        mixed_heads = jnp.swapaxes(stacked, 0, 1).reshape(tokens, heads * width)
    partial_sums = jnp.dot(
        mixed_heads,
        lax.all_gather(out_weight, "seq", axis=1, tiled=True),
        preferred_element_type=F32,
    )
    return lax.psum_scatter(
        partial_sums.astype(BF16), "head", scatter_dimension=1, tiled=True
    )


def solution(mesh):
    return jax.shard_map(
        per_device,
        mesh=mesh,
        in_specs=(
            P("seq", "head"),
            P(None, "seq", "head"),
            P(None, "seq", "head"),
            P(None, "head", "seq"),
            P("head", "seq"),
        ),
        out_specs=P("seq", "head"),
        check_vma=False,
    )
```

```python
import functools

import jax
import jax.numpy as jnp
from jax import lax
from jax.experimental import pallas as pl
from jax.experimental.pallas import tpu as pltpu
from jax.sharding import PartitionSpec as P


CHUNK = 128
EPS = 1e-06
F32 = jnp.float32
BF16 = jnp.bfloat16


def dot(a, b):
    return jnp.dot(a, b, preferred_element_type=F32)


def dot_t(a, b):
    return lax.dot_general(a, b, (((1,), (1,)), ((), ())), preferred_element_type=F32)


def split(x):
    high = x.astype(BF16)
    return high, (x - high.astype(F32)).astype(BF16)


def product3(left, right):
    left_high, left_low = split(left)
    right_high, right_low = split(right)
    lhs = jnp.concatenate([left_high, left_low], axis=1)
    rhs = jnp.concatenate(
        [
            jnp.concatenate([right_high, right_low], axis=1),
            jnp.concatenate([right_high, jnp.zeros_like(right_low)], axis=1),
        ],
        axis=0,
    )
    wide = dot(lhs, rhs)
    width = right.shape[1]
    return wide[:, :width] + wide[:, width:]


def iota(shape, axis):
    return lax.broadcasted_iota(jnp.int32, shape, axis)


def weave(first, second):
    half = first.shape[0] // 2
    return jnp.concatenate([first[:half], second[:half], first[half:], second[half:]], axis=0)


def weave_lanes(first, second):
    half = first.shape[1] // 2
    return jnp.concatenate(
        [first[:, :half], second[:, :half], first[:, half:], second[:, half:]], axis=1
    )


def place(position, offset):
    return jnp.bitwise_xor(position, offset)


VMEM = pl.BlockSpec(memory_space=pltpu.VMEM)
PARAMS = pltpu.CompilerParams(vmem_limit_bytes=12 * 2**20)


def held(*arrays):
    return [pltpu.with_memory_space_constraint(array, pltpu.VMEM) for array in arrays]


def times(chunk):
    half = chunk // 2
    row, col = iota((chunk, chunk), 0), iota((chunk, chunk), 1)
    return 2 * lax.rem(row, half) + row // half, 2 * lax.rem(col, half) + col // half


def beta_rows(tokens, width):
    return -(-4 * max(tokens // width, 1) // 16) * 16


def pack_kernel(group, key_ref, value_ref, query_ref, strength_ref, *refs):
    key_outs, rest_outs, (beta_ref, sems) = refs[:group], refs[group : 2 * group], refs[-2:]
    _, heads, tokens = beta_ref.shape
    mine = heads // group
    wide = key_outs[0].shape[1]
    width = wide // mine
    pieces = max(tokens // width, 1)
    inside = tokens // pieces
    position, _ = where_am_i(group)
    first_copy = pltpu.make_async_copy(strength_ref, beta_ref, sems.at[0])
    pairs = []
    for offset in range(group):
        lanes = pl.ds(pl.multiple_of(place(position, offset) * wide, wide), wide)
        for reflection in range(2):
            rows = pl.ds(reflection * tokens, tokens)
            pairs.append((key_ref.at[reflection, :, lanes], key_outs[offset].at[rows, :]))
    for offset in range(group):
        lanes = pl.ds(pl.multiple_of(place(position, offset) * wide, wide), wide)
        for reflection in range(2):
            pairs.append(
                (value_ref.at[reflection, :, lanes], rest_outs[offset].at[reflection])
            )
        pairs.append((query_ref.at[:, lanes], rest_outs[offset].at[2]))
    copies = [
        pltpu.make_async_copy(source, target, sems.at[1 + number])
        for number, (source, target) in enumerate(pairs)
    ]
    first_copy.start()
    for copy in copies:
        copy.start()
    first_copy.wait()
    for offset, out_ref in enumerate(key_outs):
        member = place(position, offset)
        rows = []
        for reflection in range(2):
            for piece in range(pieces):
                cuts = []
                for head in range(mine):
                    cut = beta_ref[reflection, pl.ds(member * mine + head, 1), :]
                    cuts.append(cut[:, piece * inside : (piece + 1) * inside])
                    if inside < width:
                        cuts.append(jnp.zeros((1, width - inside), F32))
                rows.append(jnp.concatenate(cuts, axis=1) if len(cuts) > 1 else cuts[0])
        both = jnp.concatenate(rows, axis=0)
        high = both.astype(BF16).astype(F32)
        spare = jnp.zeros((out_ref.shape[0] - 2 * tokens - 2 * len(rows), wide), F32)
        out_ref[2 * tokens :, :] = jnp.concatenate([high, both - high, spare], axis=0).astype(BF16)
    for copy in copies:
        copy.wait()


def pack(queries, key_vectors, values, strengths, group):
    _, tokens, wide = key_vectors.shape
    width = wide // strengths.shape[1]
    shape = (2 * tokens + beta_rows(tokens, width), wide // group)
    out = pl.pallas_call(
        functools.partial(pack_kernel, group),
        out_shape=[pltpu.VMEM(shape, BF16)] * group
        + [pltpu.VMEM((3, tokens, wide // group), BF16)] * group,
        in_specs=[pl.BlockSpec(memory_space=pltpu.HBM)] * 4,
        out_specs=[VMEM] * (2 * group),
        scratch_shapes=[
            pltpu.VMEM(strengths.shape, F32),
            pltpu.SemaphoreType.DMA((1 + 5 * group,)),
        ],
        compiler_params=PARAMS,
        name="pack",
    )(
        *(
            pltpu.with_memory_space_constraint(array, pltpu.HBM)
            for array in (key_vectors, values, queries, strengths)
        )
    )
    return list(out[:group]), list(out[group:])


def invert_kernel(heads, tokens, *refs):
    key_in, (inverse_ref, table_ref, a_buf) = refs[:-3], refs[-3:]
    width = key_in[0].shape[1] // heads
    chunk = min(CHUNK, tokens)
    per_source = tokens // chunk
    chunks = len(key_in) * per_source
    pieces = max(tokens // width, 1)
    row_time, col_time = times(chunk)
    levels = chunk.bit_length() - 1

    def joins(level):
        same = (row_time >> (level + 1)) == (col_time >> (level + 1))
        return same & (((row_time >> level) & 1) == 1) & (((col_time >> level) & 1) == 0)

    def prepare(head, index):
        lanes = lanes_of(head, width)
        key_ref, first = key_in[index // per_source], (index % per_source) * chunk
        key = woven_key(key_ref, tokens, first, chunk, lanes)
        gram = dot_t(key, key)
        wide_row, wide_col = iota(gram.shape, 0), iota(gram.shape, 1)
        square = jnp.sum(jnp.where(wide_row == wide_col, gram, 0.0), axis=0, keepdims=True)
        scale_row = lax.rsqrt(square + EPS)
        halves = key_ref[2 * tokens :, lanes].astype(F32)
        piece, inside = first // width, first % width

        def strength(reflection):
            high = reflection * pieces + piece
            low = (2 + reflection) * pieces + piece
            both = halves[high : high + 1] + halves[low : low + 1]
            return both[:, inside : inside + chunk]

        beta_row = weave_lanes(strength(0), strength(1))
        both_row = beta_row * scale_row
        table = jnp.concatenate(
            [scale_row, beta_row, both_row, jnp.zeros((5, 2 * chunk), F32)], axis=0
        )
        table_ref[head, index] = table
        system = table.T[:, 2:3] * (gram * scale_row)
        for block in range(2):
            here = slice(block * chunk, (block + 1) * chunk)
            diagonal = system[here, here]
            a_buf[head, index, block] = diagonal
            inverse_ref[head, index, block] = jnp.where(
                row_time == col_time, 1.0, 0.0
            ) - jnp.where(joins(0), diagonal, 0.0)
        inverse_ref[head, index, 2] = system[chunk:, :chunk]

    def solve(units):
        for head, index in units:
            prepare(head, index)
        every = [(head, index, block) for head, index in units for block in range(2)]
        for level in range(1, levels):
            mask = joins(level)
            inner = [
                product3(jnp.where(mask, a_buf[one], 0.0), inverse_ref[one]) for one in every
            ]
            for one, value in zip(every, inner):
                known = inverse_ref[one]
                inverse_ref[one] = known - product3(known, value)
        inner = [
            product3(inverse_ref[head, index, 2], inverse_ref[head, index, 0])
            for head, index in units
        ]
        for (head, index), value in zip(units, inner):
            inverse_ref[head, index, 2] = -product3(inverse_ref[head, index, 1], value)

    every_unit(heads, chunks, solve)


def lanes_of(head, width):
    if isinstance(head, int):
        return slice(head * width, (head + 1) * width)
    return pl.ds(pl.multiple_of(head * width, width), width)


def invert(keys, heads, tokens):
    chunk = min(CHUNK, tokens)
    chunks = len(keys) * tokens // chunk
    return pl.pallas_call(
        functools.partial(invert_kernel, heads, tokens),
        out_shape=(
            pltpu.VMEM((heads, chunks, 3, chunk, chunk), F32),
            pltpu.VMEM((heads, chunks, 8, 2 * chunk), F32),
        ),
        in_specs=[VMEM] * len(keys),
        out_specs=(VMEM, VMEM),
        scratch_shapes=[pltpu.VMEM((heads, chunks, 2, chunk, chunk), F32)],
        compiler_params=PARAMS,
        name="invert",
    )(*held(*keys))


def slot_of(group, index, per_source):
    position = lax.rem(lax.axis_index("seq"), group)
    return place(position, index // per_source) * per_source + index % per_source


def every_unit(heads, chunks, body):
    if heads * chunks <= 8:
        body([(head, index) for head in range(heads) for index in range(chunks)])
    else:

        def one_head(head, carry):
            body([(head, index) for index in range(chunks)])
            return carry

        lax.fori_loop(0, heads, one_head, 0)


def woven_key(key_ref, tokens, first, chunk, lanes):
    return weave(
        key_ref[first : first + chunk, lanes],
        key_ref[tokens + first : tokens + first + chunk, lanes],
    )


def state_kernel(group, parts, *refs):
    key_in, rest_in = refs[:group], refs[group : 2 * group]
    inverse_in = refs[2 * group : 2 * group + parts]
    table_in = refs[2 * group + parts : 2 * group + 2 * parts]
    high_ref, low_ref, step_ref, state_ref, local_ref = refs[2 * group + 2 * parts :]
    heads, per_part, _, chunk, _ = inverse_in[0].shape
    chunks = parts * per_part
    tokens = rest_in[0].shape[1]
    width = rest_in[0].shape[2] // heads
    per_source = tokens // chunk

    def solve(units):
        for head, index in units:
            lanes = lanes_of(head, width)
            part, inside = index // per_part, index % per_part
            source, first = index // per_source, (index % per_source) * chunk
            key_ref, rest_ref = key_in[source], rest_in[source]
            key = woven_key(key_ref, tokens, first, chunk, lanes).astype(F32)
            rows = slice(first, first + chunk)
            value = weave(rest_ref[0, rows, lanes], rest_ref[1, rows, lanes]).astype(F32)
            table = table_in[part][head, inside].T
            inverse = jnp.concatenate(
                [
                    jnp.concatenate(
                        [inverse_in[part][head, inside, 0], jnp.zeros((chunk, chunk), F32)],
                        axis=1,
                    ),
                    jnp.concatenate(
                        [inverse_in[part][head, inside, 2], inverse_in[part][head, inside, 1]],
                        axis=1,
                    ),
                ],
                axis=0,
            )
            right = jnp.concatenate([table[:, 2:3] * key, table[:, 1:2] * value], axis=1)
            high, low = split(table[:, 0:1] * dot3(inverse, *split(right)))
            high_ref[head, index] = high
            low_ref[head, index] = low
        for head, index in units:
            source, first = index // per_source, (index % per_source) * chunk
            turned = woven_key(key_in[source], tokens, first, chunk, lanes_of(head, width)).T
            step_ref[head, slot_of(group, index, per_source)] = dot(
                jnp.concatenate([turned, turned], axis=1),
                jnp.concatenate([high_ref[head, index], low_ref[head, index]], axis=0),
            )

    every_unit(heads, chunks, solve)
    totals = [[step_ref[head, slot] for slot in range(chunks)] for head in range(heads)]
    while len(totals[0]) > 1:
        totals = [
            [after(one[i], one[i + 1]) for i in range(0, len(one) - 1, 2)]
            + one[len(one) - len(one) % 2 :]
            for one in totals
        ]
    for head, (total,) in enumerate(totals):
        state_ref[head] = total.astype(BF16)
        local_ref[head] = total[:, width:].astype(BF16)


def after(earlier, later):
    width = earlier.shape[0]
    return earlier + later - dot(later[:, :width].astype(BF16), earlier.astype(BF16))


def dot3(left, high, low):
    left_high, left_low = split(left)
    return dot(
        jnp.concatenate([left_high, left_low, left_high], axis=1),
        jnp.concatenate([high, high, low], axis=0),
    )


def carry_state(keys, rests, inverses, tables):
    group, parts = len(keys), len(inverses)
    heads, per_part, _, chunk, _ = inverses[0].shape
    chunks = parts * per_part
    width = rests[0].shape[2] // heads
    solved = pltpu.VMEM((heads, chunks, 2 * chunk, 2 * width), BF16)
    return pl.pallas_call(
        functools.partial(state_kernel, group, parts),
        out_shape=(
            solved,
            solved,
            pltpu.VMEM((heads, chunks, width, 2 * width), F32),
            pltpu.VMEM((heads, width, 2 * width), BF16),
            pltpu.VMEM((heads, width, width), BF16),
        ),
        in_specs=[VMEM] * (2 * group + 2 * parts),
        out_specs=(VMEM,) * 5,
        compiler_params=PARAMS,
        name="carry_state",
    )(*held(*keys, *rests, *inverses, *tables))


def read_kernel(group, *refs):
    key_in, rest_in = refs[:group], refs[group : 2 * group]
    high_ref, low_ref, step_ref, out_ref, lift_ref = refs[2 * group : -3]
    before_buf, local_buf, lift_buf = refs[-3:]
    heads, chunks, wide, _ = high_ref.shape
    chunk = wide // 2
    half = chunk // 2
    tokens = rest_in[0].shape[1]
    width = rest_in[0].shape[2] // heads
    per_source = tokens // chunk
    token_row = iota((chunk, 2 * chunk), 0)
    token_col = iota((chunk, 2 * chunk), 1)
    token_col = (token_col // chunk) * half + lax.rem(token_col, half)

    def answer(units):
        for head, index in units:
            lanes = lanes_of(head, width)
            source, first = index // per_source, (index % per_source) * chunk
            key = woven_key(key_in[source], tokens, first, chunk, lanes)
            query = rest_in[source][2, first : first + chunk, lanes]
            wide_query = query.astype(F32)
            scale = lax.rsqrt(jnp.sum(wide_query * wide_query, axis=1, keepdims=True) + EPS)
            scores = jnp.where(token_col <= token_row, dot_t(query, key) * scale, 0.0)
            applied = dot3(scores, high_ref[head, index], low_ref[head, index])
            local_buf[head, index] = applied[:, width:]
            lift_buf[head, index] = scale * wide_query - applied[:, :width]

    every_unit(heads, chunks, answer)
    totals = [step_ref[head, 0] for head in range(heads)]
    for head in range(heads):
        before_buf[head, 0] = jnp.zeros((width, 2 * width), BF16)
    for slot in range(1, chunks):
        for head in range(heads):
            before_buf[head, slot] = totals[head].astype(BF16)
        if slot + 1 < chunks:
            totals = [after(totals[head], step_ref[head, slot]) for head in range(heads)]

    def correct(units):
        for head, index in units:
            lanes = lanes_of(head, width)
            slot = slot_of(group, index, per_source)
            lifted = lift_buf[head, index]
            moved = dot(lifted.astype(BF16), before_buf[head, slot])
            rows = pl.ds(pl.multiple_of(slot * chunk, chunk), chunk)
            out_ref[rows, lanes] = local_buf[head, index] + moved[:, width:]
            lift_ref[rows, lanes] = (lifted - moved[:, :width]).astype(BF16)

    every_unit(heads, chunks, correct)


def read(keys, rests, high, low, steps):
    group = len(keys)
    _, tokens, wide = rests[0].shape
    chunk, width = high.shape[2] // 2, steps.shape[2]
    return pl.pallas_call(
        functools.partial(read_kernel, group),
        out_shape=(
            pltpu.VMEM((group * tokens, wide), F32),
            pltpu.VMEM((group * tokens, wide), BF16),
        ),
        in_specs=[VMEM] * (2 * group + 3),
        out_specs=(VMEM, VMEM),
        scratch_shapes=[
            pltpu.VMEM(steps.shape, BF16),
            pltpu.VMEM(steps.shape[:2] + (chunk, width), F32),
            pltpu.VMEM(steps.shape[:2] + (chunk, width), F32),
        ],
        compiler_params=PARAMS,
        name="read",
    )(*held(*keys, *rests, high, low, steps))


def join_kernel(count, splits, *refs):
    states, (local_ref, lift_ref), outs = refs[:count], refs[count : count + 2], refs[count + 2 :]
    heads, width, _ = states[0].shape
    group = sum(len(split) for split in splits)
    tokens = local_ref.shape[0] // group
    position, _ = where_am_i(group)
    for head in range(heads):
        lanes = slice(head * width, (head + 1) * width)
        total = None
        for state in reversed(states):
            if total is None:
                total = state[head].astype(F32)
            else:
                step = state[head].astype(F32)
                total = (
                    total + step[:, width:] - dot(state[head, :, :width], total.astype(BF16))
                )
        total = total.astype(BF16)
        for split_of, out_ref in zip(splits, outs):
            for number, offset in enumerate(split_of):
                rows = pl.ds(pl.multiple_of(place(position, offset) * tokens, tokens), tokens)
                out_ref[number * tokens : (number + 1) * tokens, lanes] = (
                    local_ref[rows, lanes] + dot(lift_ref[rows, lanes], total)
                ).astype(BF16)


def join(states, local, lifted, splits):
    group = sum(len(split) for split in splits)
    rows, wide = local.shape
    return pl.pallas_call(
        functools.partial(join_kernel, len(states), splits),
        out_shape=[pltpu.VMEM((rows // group * len(split), wide), BF16) for split in splits],
        in_specs=[VMEM] * (len(states) + 2),
        out_specs=[VMEM] * len(splits),
        compiler_params=PARAMS,
        name="join",
    )(*held(*states, local, lifted))


def compose(earlier, later):
    width = earlier.shape[1]
    moved = jnp.einsum("hab,hbc->hac", later[:, :, :width], earlier, preferred_element_type=F32)
    return (earlier.astype(F32) + later.astype(F32) - moved).astype(BF16)


def weight_rows(weights, offset, inner, first, count):
    rows = pl.ds(first, count)
    if offset < 2:
        return weights[offset][rows, :]
    near, far = (4, 5) if offset == 2 else (2, 3)
    return jnp.where(inner, weights[near][rows, :], weights[far][rows, :])


def where_am_i(group):
    device = lax.axis_index("seq")
    return lax.rem(device, group), device // group


def project_kernel(group, orders, offsets, *refs):
    heads_in, weight_in, (send_ref, keep_ref) = refs[:group], refs[group:-2], refs[-2:]
    core = lax.axis_index("head")
    position, plane = where_am_i(group)
    rows, wide = heads_in[0].shape
    tokens = rows // len(orders[0])
    columns = weight_in[0].shape[1]
    side = keep_ref.shape[1] // columns
    inner = (plane == 1) | (plane == 2)
    left = jnp.concatenate(
        [
            jnp.concatenate(
                [heads_in[member][at * tokens : (at + 1) * tokens, :] for at in orders[member]],
                axis=0,
            )
            for member in range(group)
        ],
        axis=1,
    )
    firsts = [
        pl.multiple_of(place(position, member) * wide, wide) for member in range(group)
    ]
    for offset in offsets:
        owner = jnp.bitwise_xor(plane, offset)
        right = jnp.concatenate(
            [weight_rows(weight_in, offset, inner, first, wide) for first in firsts], axis=0
        )
        result = dot(left, right).astype(BF16)
        lanes = pl.ds(pl.multiple_of(lax.rem(owner, side) * columns, columns), columns)

        @pl.when(owner // side == core)
        def _():
            keep_ref[:, lanes] = result

        @pl.when(owner // side != core)
        def _():
            send_ref[:, lanes] = result


def project(heads, weights, planes, orders):
    group = len(heads)
    rows = heads[0].shape[0]
    columns = weights[0].shape[1]
    offsets = (0, 1, 3, 2) if planes == 4 else (0, 1)
    shape = pltpu.VMEM((rows, columns * planes // 2), BF16)
    return pl.pallas_call(
        functools.partial(project_kernel, group, orders, offsets),
        out_shape=(shape, shape),
        in_specs=[VMEM] * (group + len(weights)),
        out_specs=(VMEM, VMEM),
        compiler_params=PARAMS,
        name="project",
    )(*held(*heads, *weights))


def sum_kernel(keep_ref, other_ref, *outs):
    tokens = outs[0].shape[0]
    for index, out_ref in enumerate(outs):
        rows = slice(index * tokens, (index + 1) * tokens)
        out_ref[...] = (keep_ref[rows, :].astype(F32) + other_ref[rows, :].astype(F32)).astype(
            BF16
        )


def sum_parts(keep, other, count):
    rows, columns = keep.shape
    return pl.pallas_call(
        sum_kernel,
        out_shape=[pltpu.VMEM((rows // count, columns), BF16)] * count,
        in_specs=[VMEM, VMEM],
        out_specs=[VMEM] * count,
        compiler_params=PARAMS,
        name="sum_parts",
    )(*held(keep, other))


def lay_kernel(group, columns, *refs):
    parts, out_ref, sems = refs[:group], refs[group], refs[group + 1]
    position = lax.rem(lax.axis_index("seq"), group)
    copies = []
    for offset in range(group):
        for index in range(parts[0].shape[1] // columns):
            first = (index * group + place(position, offset)) * columns
            copies.append(
                pltpu.make_async_copy(
                    parts[offset].at[:, index * columns : (index + 1) * columns],
                    out_ref.at[:, pl.ds(pl.multiple_of(first, columns), columns)],
                    sems.at[len(copies)],
                )
            )
    for copy in copies:
        copy.start()
    for copy in copies:
        copy.wait()


def lay_out(parts, columns):
    group = len(parts)
    rows, wide = parts[0].shape
    return pl.pallas_call(
        functools.partial(lay_kernel, group, columns),
        out_shape=jax.ShapeDtypeStruct((rows, group * wide), BF16),
        in_specs=[VMEM] * group,
        out_specs=pl.BlockSpec(memory_space=pl.ANY),
        scratch_shapes=[pltpu.SemaphoreType.DMA((group * wide // columns,))],
        compiler_params=PARAMS,
        name="lay_out",
    )(*held(*parts))


def swap(value, group, offset, count):
    pairs = [(i, (i // group) * group + ((i % group) ^ offset)) for i in range(count)]
    return lax.ppermute(value, "seq", pairs)


def per_device(queries, key_vectors, values, strengths, out_weight):
    count = lax.axis_size("seq")
    sides = lax.axis_size("head")
    heads = strengths.shape[1]
    tokens = queries.shape[0]
    width = queries.shape[1] // heads
    group = 1
    while group < 4 and heads % (2 * group) == 0 and count % (2 * group) == 0:
        group *= 2
    planes = count // group
    position = lax.axis_index("seq") % group
    mine = heads // group
    keys, rests = pack(queries, key_vectors, values, strengths, group)
    for offset in range(1, group):
        keys[offset] = swap(keys[offset], group, offset, count)
        rests[offset] = swap(rests[offset], group, offset, count)

    def between_planes(value, pairs):
        return lax.ppermute(
            value,
            "seq",
            [
                (source * group + i, target * group + i)
                for source, target in pairs
                for i in range(group)
            ],
        )

    split_out = sides == 2 and planes in (2, 4) and group > 1
    weights = [out_weight]
    if split_out:
        swapped = [(plane, plane ^ 1) for plane in range(planes)]
        weights.append(between_planes(out_weight, swapped))
    if split_out and planes == 4:
        for pairs in (((1, 2), (2, 1)), ((0, 3), (3, 0))):
            weights.append(between_planes(out_weight, pairs))

    near = max(group // 2, 1)
    solved = []
    for part in (keys[:near], keys[near:]):
        if part:
            solved.append(invert(part, mine, tokens))
    inverses, tables = zip(*solved)
    high, low, steps, state, local_state = carry_state(keys, rests, inverses, tables)
    local, lifted = read(keys, rests, high, low, steps)

    def from_earlier(value, distance):
        pairs = [(i, i + distance * group) for i in range(count - distance * group)]
        return lax.ppermute(value, "seq", pairs)

    if planes <= 4:
        states = []
        for distance in range(1, planes):
            sent = state if distance + 1 < planes else local_state
            states.append(from_earlier(sent, distance))
    else:
        total = from_earlier(state, 1)
        distance = 1
        while distance < planes - 1:
            total = compose(from_earlier(total, distance), total)
            distance *= 2
        states = [total[:, :, width:]]
    if split_out and planes == 4:
        weights += [
            between_planes(weights[1], ((1, 2), (2, 1))),
            between_planes(weights[2], ((1, 0), (2, 3))),
        ]

    if split_out:
        row_halves = ((3, 1), (2, 0)) if group == 4 else ((1,), (0,))
        ready = join(states, local, lifted, row_halves)
        parts = [None] * group
        gathered, orders = [], []
        for targets in row_halves:
            arrays, order = [], []
            for offset in range(group):
                seen = [target ^ offset for target in targets]
                source = row_halves.index(
                    next(half for half in row_halves if set(half) == set(seen))
                )
                order.append(tuple(row_halves[source].index(block) for block in seen))
                array = ready[source]
                if offset:
                    array = swap(array, group, offset, count)
                arrays.append(array)
            gathered.append(arrays)
            orders.append(tuple(order))
        for number, targets in enumerate(row_halves):
            send, keep = project(gathered[number], weights, planes, orders[number])
            other = lax.ppermute(send, "head", [(0, 1), (1, 0)])
            for offset, part in zip(targets, sum_parts(keep, other, len(targets))):
                parts[offset] = swap(part, group, offset, count) if offset else part
        return lay_out(parts, out_weight.shape[1])

    (mixed_heads,) = join(states, local, lifted, (tuple(range(group)),))
    if group > 1:
        position_rows = []
        for offset in range(group):
            part = lax.dynamic_slice_in_dim(mixed_heads, offset * tokens, tokens, 0)
            position_rows.append(swap(part, group, offset, count) if offset else part)
        stacked = jnp.stack(position_rows)
        order = jnp.bitwise_xor(position, jnp.arange(group))
        stacked = jnp.take(stacked, order, axis=0)
        mixed_heads = jnp.swapaxes(stacked, 0, 1).reshape(tokens, heads * width)
    partial_sums = jnp.dot(
        mixed_heads,
        lax.all_gather(out_weight, "seq", axis=1, tiled=True),
        preferred_element_type=F32,
    )
    return lax.psum_scatter(
        partial_sums.astype(BF16), "head", scatter_dimension=1, tiled=True
    )


def solution(mesh):
    return jax.shard_map(
        per_device,
        mesh=mesh,
        in_specs=(
            P("seq", "head"),
            P(None, "seq", "head"),
            P(None, "seq", "head"),
            P(None, "head", "seq"),
            P("head", "seq"),
        ),
        out_specs=P("seq", "head"),
        check_vma=False,
    )
```

```python
import functools

import jax
import jax.numpy as jnp
from jax import lax
from jax.experimental import pallas as pl
from jax.experimental.pallas import tpu as pltpu
from jax.sharding import PartitionSpec as P


CHUNK = 128
EPS = 1e-06
F32 = jnp.float32
BF16 = jnp.bfloat16


def dot(a, b):
    return jnp.dot(a, b, preferred_element_type=F32)


def dot_t(a, b):
    return lax.dot_general(a, b, (((1,), (1,)), ((), ())), preferred_element_type=F32)


def split(x):
    high = x.astype(BF16)
    return high, (x - high.astype(F32)).astype(BF16)


def product3(left, right):
    left_high, left_low = split(left)
    right_high, right_low = split(right)
    lhs = jnp.concatenate([left_high, left_low], axis=1)
    rhs = jnp.concatenate(
        [
            jnp.concatenate([right_high, right_low], axis=1),
            jnp.concatenate([right_high, jnp.zeros_like(right_low)], axis=1),
        ],
        axis=0,
    )
    wide = dot(lhs, rhs)
    width = right.shape[1]
    return wide[:, :width] + wide[:, width:]


def iota(shape, axis):
    return lax.broadcasted_iota(jnp.int32, shape, axis)


def weave(first, second):
    half = first.shape[0] // 2
    return jnp.concatenate([first[:half], second[:half], first[half:], second[half:]], axis=0)


def weave_lanes(first, second):
    half = first.shape[1] // 2
    return jnp.concatenate(
        [first[:, :half], second[:, :half], first[:, half:], second[:, half:]], axis=1
    )


def place(position, offset):
    return jnp.bitwise_xor(position, offset)


VMEM = pl.BlockSpec(memory_space=pltpu.VMEM)
PARAMS = pltpu.CompilerParams(vmem_limit_bytes=12 * 2**20)


def held(*arrays):
    return [pltpu.with_memory_space_constraint(array, pltpu.VMEM) for array in arrays]


def times(chunk):
    half = chunk // 2
    row, col = iota((chunk, chunk), 0), iota((chunk, chunk), 1)
    return 2 * lax.rem(row, half) + row // half, 2 * lax.rem(col, half) + col // half


def beta_rows(tokens, width):
    return -(-4 * max(tokens // width, 1) // 16) * 16


def pack_kernel(group, key_ref, value_ref, query_ref, strength_ref, *refs):
    key_outs, rest_outs, (beta_ref, sems) = refs[:group], refs[group : 2 * group], refs[-2:]
    _, heads, tokens = beta_ref.shape
    mine = heads // group
    wide = key_outs[0].shape[1]
    width = wide // mine
    pieces = max(tokens // width, 1)
    inside = tokens // pieces
    position, _ = where_am_i(group)
    first_copy = pltpu.make_async_copy(strength_ref, beta_ref, sems.at[0])
    pairs = []
    for offset in range(group):
        lanes = pl.ds(pl.multiple_of(place(position, offset) * wide, wide), wide)
        for reflection in range(2):
            rows = pl.ds(reflection * tokens, tokens)
            pairs.append((key_ref.at[reflection, :, lanes], key_outs[offset].at[rows, :]))
    for offset in range(group):
        lanes = pl.ds(pl.multiple_of(place(position, offset) * wide, wide), wide)
        for reflection in range(2):
            pairs.append(
                (value_ref.at[reflection, :, lanes], rest_outs[offset].at[reflection])
            )
        pairs.append((query_ref.at[:, lanes], rest_outs[offset].at[2]))
    copies = [
        pltpu.make_async_copy(source, target, sems.at[1 + number])
        for number, (source, target) in enumerate(pairs)
    ]
    first_copy.start()
    for copy in copies:
        copy.start()
    first_copy.wait()
    for offset, out_ref in enumerate(key_outs):
        member = place(position, offset)
        rows = []
        for reflection in range(2):
            for piece in range(pieces):
                cuts = []
                for head in range(mine):
                    cut = beta_ref[reflection, pl.ds(member * mine + head, 1), :]
                    cuts.append(cut[:, piece * inside : (piece + 1) * inside])
                    if inside < width:
                        cuts.append(jnp.zeros((1, width - inside), F32))
                rows.append(jnp.concatenate(cuts, axis=1) if len(cuts) > 1 else cuts[0])
        both = jnp.concatenate(rows, axis=0)
        high = both.astype(BF16).astype(F32)
        spare = jnp.zeros((out_ref.shape[0] - 2 * tokens - 2 * len(rows), wide), F32)
        out_ref[2 * tokens :, :] = jnp.concatenate([high, both - high, spare], axis=0).astype(BF16)
    for copy in copies:
        copy.wait()


def pack(queries, key_vectors, values, strengths, group):
    _, tokens, wide = key_vectors.shape
    width = wide // strengths.shape[1]
    shape = (2 * tokens + beta_rows(tokens, width), wide // group)
    out = pl.pallas_call(
        functools.partial(pack_kernel, group),
        out_shape=[pltpu.VMEM(shape, BF16)] * group
        + [pltpu.VMEM((3, tokens, wide // group), BF16)] * group,
        in_specs=[pl.BlockSpec(memory_space=pltpu.HBM)] * 4,
        out_specs=[VMEM] * (2 * group),
        scratch_shapes=[
            pltpu.VMEM(strengths.shape, F32),
            pltpu.SemaphoreType.DMA((1 + 5 * group,)),
        ],
        compiler_params=PARAMS,
        name="pack",
    )(
        *(
            pltpu.with_memory_space_constraint(array, pltpu.HBM)
            for array in (key_vectors, values, queries, strengths)
        )
    )
    return list(out[:group]), list(out[group:])


def invert_kernel(heads, tokens, *refs):
    key_in, (inverse_ref, table_ref, a_buf) = refs[:-3], refs[-3:]
    width = key_in[0].shape[1] // heads
    chunk = min(CHUNK, tokens)
    per_source = tokens // chunk
    chunks = len(key_in) * per_source
    pieces = max(tokens // width, 1)
    row_time, col_time = times(chunk)
    levels = chunk.bit_length() - 1

    def joins(level):
        same = (row_time >> (level + 1)) == (col_time >> (level + 1))
        return same & (((row_time >> level) & 1) == 1) & (((col_time >> level) & 1) == 0)

    def prepare(head, index):
        lanes = lanes_of(head, width)
        key_ref, first = key_in[index // per_source], (index % per_source) * chunk
        key = woven_key(key_ref, tokens, first, chunk, lanes)
        gram = dot_t(key, key)
        wide_row, wide_col = iota(gram.shape, 0), iota(gram.shape, 1)
        square = jnp.sum(jnp.where(wide_row == wide_col, gram, 0.0), axis=0, keepdims=True)
        scale_row = lax.rsqrt(square + EPS)
        halves = key_ref[2 * tokens :, lanes].astype(F32)
        piece, inside = first // width, first % width

        def strength(reflection):
            high = reflection * pieces + piece
            low = (2 + reflection) * pieces + piece
            both = halves[high : high + 1] + halves[low : low + 1]
            return both[:, inside : inside + chunk]

        beta_row = weave_lanes(strength(0), strength(1))
        both_row = beta_row * scale_row
        table = jnp.concatenate(
            [scale_row, beta_row, both_row, jnp.zeros((5, 2 * chunk), F32)], axis=0
        )
        table_ref[head, index] = table
        system = table.T[:, 2:3] * (gram * scale_row)
        for block in range(2):
            here = slice(block * chunk, (block + 1) * chunk)
            diagonal = system[here, here]
            a_buf[head, index, block] = diagonal
            inverse_ref[head, index, block] = jnp.where(
                row_time == col_time, 1.0, 0.0
            ) - jnp.where(joins(0), diagonal, 0.0)
        inverse_ref[head, index, 2] = system[chunk:, :chunk]

    def solve(units):
        for head, index in units:
            prepare(head, index)
        every = [(head, index, block) for head, index in units for block in range(2)]
        for level in range(1, levels):
            mask = joins(level)
            inner = [
                product3(jnp.where(mask, a_buf[one], 0.0), inverse_ref[one]) for one in every
            ]
            for one, value in zip(every, inner):
                known = inverse_ref[one]
                inverse_ref[one] = known - product3(known, value)
        inner = [
            product3(inverse_ref[head, index, 2], inverse_ref[head, index, 0])
            for head, index in units
        ]
        for (head, index), value in zip(units, inner):
            inverse_ref[head, index, 2] = -product3(inverse_ref[head, index, 1], value)

    every_unit(heads, chunks, solve)


def lanes_of(head, width):
    if isinstance(head, int):
        return slice(head * width, (head + 1) * width)
    return pl.ds(pl.multiple_of(head * width, width), width)


def invert(keys, heads, tokens):
    chunk = min(CHUNK, tokens)
    chunks = len(keys) * tokens // chunk
    return pl.pallas_call(
        functools.partial(invert_kernel, heads, tokens),
        out_shape=(
            pltpu.VMEM((heads, chunks, 3, chunk, chunk), F32),
            pltpu.VMEM((heads, chunks, 8, 2 * chunk), F32),
        ),
        in_specs=[VMEM] * len(keys),
        out_specs=(VMEM, VMEM),
        scratch_shapes=[pltpu.VMEM((heads, chunks, 2, chunk, chunk), F32)],
        compiler_params=PARAMS,
        name="invert",
    )(*held(*keys))


def slot_of(group, index, per_source):
    position = lax.rem(lax.axis_index("seq"), group)
    return place(position, index // per_source) * per_source + index % per_source


def every_unit(heads, chunks, body):
    if heads * chunks <= 8:
        body([(head, index) for head in range(heads) for index in range(chunks)])
    else:

        def one_head(head, carry):
            body([(head, index) for index in range(chunks)])
            return carry

        lax.fori_loop(0, heads, one_head, 0)


def woven_key(key_ref, tokens, first, chunk, lanes):
    return weave(
        key_ref[first : first + chunk, lanes],
        key_ref[tokens + first : tokens + first + chunk, lanes],
    )


def state_kernel(group, parts, *refs):
    key_in, rest_in = refs[:group], refs[group : 2 * group]
    inverse_in = refs[2 * group : 2 * group + parts]
    table_in = refs[2 * group + parts : 2 * group + 2 * parts]
    high_ref, low_ref, step_ref, state_ref, local_ref = refs[2 * group + 2 * parts :]
    heads, per_part, _, chunk, _ = inverse_in[0].shape
    chunks = parts * per_part
    tokens = rest_in[0].shape[1]
    width = rest_in[0].shape[2] // heads
    per_source = tokens // chunk

    def solve(units):
        for head, index in units:
            lanes = lanes_of(head, width)
            part, inside = index // per_part, index % per_part
            source, first = index // per_source, (index % per_source) * chunk
            key_ref, rest_ref = key_in[source], rest_in[source]
            key = woven_key(key_ref, tokens, first, chunk, lanes).astype(F32)
            rows = slice(first, first + chunk)
            value = weave(rest_ref[0, rows, lanes], rest_ref[1, rows, lanes]).astype(F32)
            table = table_in[part][head, inside].T
            inverse = jnp.concatenate(
                [
                    jnp.concatenate(
                        [inverse_in[part][head, inside, 0], jnp.zeros((chunk, chunk), F32)],
                        axis=1,
                    ),
                    jnp.concatenate(
                        [inverse_in[part][head, inside, 2], inverse_in[part][head, inside, 1]],
                        axis=1,
                    ),
                ],
                axis=0,
            )
            right = jnp.concatenate([table[:, 2:3] * key, table[:, 1:2] * value], axis=1)
            high, low = split(table[:, 0:1] * dot3(inverse, *split(right)))
            high_ref[head, index] = high
            low_ref[head, index] = low
        for head, index in units:
            source, first = index // per_source, (index % per_source) * chunk
            turned = woven_key(key_in[source], tokens, first, chunk, lanes_of(head, width)).T
            step_ref[head, slot_of(group, index, per_source)] = dot(
                turned, high_ref[head, index]
            ) + dot(turned, low_ref[head, index])

    every_unit(heads, chunks, solve)
    totals = [[step_ref[head, slot] for slot in range(chunks)] for head in range(heads)]
    while len(totals[0]) > 1:
        totals = [
            [after(one[i], one[i + 1]) for i in range(0, len(one) - 1, 2)]
            + one[len(one) - len(one) % 2 :]
            for one in totals
        ]
    for head, (total,) in enumerate(totals):
        state_ref[head] = total.astype(BF16)
        local_ref[head] = total[:, width:].astype(BF16)


def after(earlier, later):
    width = earlier.shape[0]
    return earlier + later - dot(later[:, :width].astype(BF16), earlier.astype(BF16))


def dot3(left, high, low):
    left_high, left_low = split(left)
    return dot(left_high, high) + dot(left_low, high) + dot(left_high, low)


def carry_state(keys, rests, inverses, tables):
    group, parts = len(keys), len(inverses)
    heads, per_part, _, chunk, _ = inverses[0].shape
    chunks = parts * per_part
    width = rests[0].shape[2] // heads
    solved = pltpu.VMEM((heads, chunks, 2 * chunk, 2 * width), BF16)
    return pl.pallas_call(
        functools.partial(state_kernel, group, parts),
        out_shape=(
            solved,
            solved,
            pltpu.VMEM((heads, chunks, width, 2 * width), F32),
            pltpu.VMEM((heads, width, 2 * width), BF16),
            pltpu.VMEM((heads, width, width), BF16),
        ),
        in_specs=[VMEM] * (2 * group + 2 * parts),
        out_specs=(VMEM,) * 5,
        compiler_params=PARAMS,
        name="carry_state",
    )(*held(*keys, *rests, *inverses, *tables))


def read_kernel(group, *refs):
    key_in, rest_in = refs[:group], refs[group : 2 * group]
    high_ref, low_ref, step_ref, out_ref, lift_ref = refs[2 * group : -3]
    before_buf, local_buf, lift_buf = refs[-3:]
    heads, chunks, wide, _ = high_ref.shape
    chunk = wide // 2
    half = chunk // 2
    tokens = rest_in[0].shape[1]
    width = rest_in[0].shape[2] // heads
    per_source = tokens // chunk
    token_row = iota((chunk, 2 * chunk), 0)
    token_col = iota((chunk, 2 * chunk), 1)
    token_col = (token_col // chunk) * half + lax.rem(token_col, half)

    def answer(units):
        for head, index in units:
            lanes = lanes_of(head, width)
            source, first = index // per_source, (index % per_source) * chunk
            key = woven_key(key_in[source], tokens, first, chunk, lanes)
            query = rest_in[source][2, first : first + chunk, lanes]
            wide_query = query.astype(F32)
            scale = lax.rsqrt(jnp.sum(wide_query * wide_query, axis=1, keepdims=True) + EPS)
            scores = jnp.where(token_col <= token_row, dot_t(query, key) * scale, 0.0)
            applied = dot3(scores, high_ref[head, index], low_ref[head, index])
            local_buf[head, index] = applied[:, width:]
            lift_buf[head, index] = scale * wide_query - applied[:, :width]

    every_unit(heads, chunks, answer)
    totals = [step_ref[head, 0] for head in range(heads)]
    for head in range(heads):
        before_buf[head, 0] = jnp.zeros((width, 2 * width), BF16)
    for slot in range(1, chunks):
        for head in range(heads):
            before_buf[head, slot] = totals[head].astype(BF16)
        if slot + 1 < chunks:
            totals = [after(totals[head], step_ref[head, slot]) for head in range(heads)]

    def correct(units):
        for head, index in units:
            lanes = lanes_of(head, width)
            slot = slot_of(group, index, per_source)
            lifted = lift_buf[head, index]
            moved = dot(lifted.astype(BF16), before_buf[head, slot])
            rows = pl.ds(pl.multiple_of(slot * chunk, chunk), chunk)
            out_ref[rows, lanes] = local_buf[head, index] + moved[:, width:]
            lift_ref[rows, lanes] = (lifted - moved[:, :width]).astype(BF16)

    every_unit(heads, chunks, correct)


def read(keys, rests, high, low, steps):
    group = len(keys)
    _, tokens, wide = rests[0].shape
    chunk, width = high.shape[2] // 2, steps.shape[2]
    return pl.pallas_call(
        functools.partial(read_kernel, group),
        out_shape=(
            pltpu.VMEM((group * tokens, wide), F32),
            pltpu.VMEM((group * tokens, wide), BF16),
        ),
        in_specs=[VMEM] * (2 * group + 3),
        out_specs=(VMEM, VMEM),
        scratch_shapes=[
            pltpu.VMEM(steps.shape, BF16),
            pltpu.VMEM(steps.shape[:2] + (chunk, width), F32),
            pltpu.VMEM(steps.shape[:2] + (chunk, width), F32),
        ],
        compiler_params=PARAMS,
        name="read",
    )(*held(*keys, *rests, high, low, steps))


def join_kernel(count, splits, *refs):
    states, (local_ref, lift_ref), outs = refs[:count], refs[count : count + 2], refs[count + 2 :]
    heads, width, _ = states[0].shape
    group = sum(len(split) for split in splits)
    tokens = local_ref.shape[0] // group
    position, _ = where_am_i(group)
    for head in range(heads):
        lanes = slice(head * width, (head + 1) * width)
        total = None
        for state in reversed(states):
            if total is None:
                total = state[head].astype(F32)
            else:
                step = state[head].astype(F32)
                total = (
                    total + step[:, width:] - dot(state[head, :, :width], total.astype(BF16))
                )
        total = total.astype(BF16)
        for split_of, out_ref in zip(splits, outs):
            for number, offset in enumerate(split_of):
                rows = pl.ds(pl.multiple_of(place(position, offset) * tokens, tokens), tokens)
                out_ref[number * tokens : (number + 1) * tokens, lanes] = (
                    local_ref[rows, lanes] + dot(lift_ref[rows, lanes], total)
                ).astype(BF16)


def join(states, local, lifted, splits):
    group = sum(len(split) for split in splits)
    rows, wide = local.shape
    return pl.pallas_call(
        functools.partial(join_kernel, len(states), splits),
        out_shape=[pltpu.VMEM((rows // group * len(split), wide), BF16) for split in splits],
        in_specs=[VMEM] * (len(states) + 2),
        out_specs=[VMEM] * len(splits),
        compiler_params=PARAMS,
        name="join",
    )(*held(*states, local, lifted))


def compose(earlier, later):
    width = earlier.shape[1]
    moved = jnp.einsum("hab,hbc->hac", later[:, :, :width], earlier, preferred_element_type=F32)
    return (earlier.astype(F32) + later.astype(F32) - moved).astype(BF16)


def where_am_i(group):
    device = lax.axis_index("seq")
    return lax.rem(device, group), device // group


def project_kernel(group, orders, *refs):
    heads_in, weight_in, (send_ref, keep_ref, left_buf) = refs[:group], refs[group:-3], refs[-3:]
    core = lax.axis_index("head")
    position, plane = where_am_i(group)
    rows, wide = heads_in[0].shape
    tokens = rows // len(orders[0])
    columns = weight_in[0].shape[1]
    side = keep_ref.shape[1] // columns
    for member in range(group):
        lanes = pl.ds(pl.multiple_of(place(position, member) * wide, wide), wide)
        for to, at in enumerate(orders[member]):
            left_buf[to * tokens : (to + 1) * tokens, lanes] = heads_in[member][
                at * tokens : (at + 1) * tokens, :
            ]
    offsets = (0, 1, 3, 2) if len(weight_in) > 2 else (0, 1)
    for number, offset in enumerate(offsets):
        if offset == 2:
            inner = (plane == 1) | (plane == 2)
            right = jnp.where(inner, weight_in[3][...], weight_in[4][...])
        else:
            right = weight_in[number][...]
        result = dot(left_buf[...], right).astype(BF16)
        owner = jnp.bitwise_xor(plane, offset)
        even = lax.rem(owner, side) == 0
        mine = owner // side == core
        for slot in range(side):
            here = (even if slot == 0 else ~even) if side == 2 else owner == owner
            lanes = slice(slot * columns, (slot + 1) * columns)

            @pl.when(mine & here)
            def _():
                keep_ref[:, lanes] = result

            @pl.when(~mine & here)
            def _():
                send_ref[:, lanes] = result


def project(heads, weights, planes, orders):
    group = len(heads)
    rows = heads[0].shape[0]
    columns = weights[0].shape[1]
    shape = pltpu.VMEM((rows, columns * planes // 2), BF16)
    return pl.pallas_call(
        functools.partial(project_kernel, group, orders),
        out_shape=(shape, shape),
        in_specs=[VMEM] * (group + len(weights)),
        out_specs=(VMEM, VMEM),
        scratch_shapes=[pltpu.VMEM((rows, weights[0].shape[0]), BF16)],
        compiler_params=PARAMS,
        name="project",
    )(*held(*heads, *weights))


def sum_kernel(keep_ref, other_ref, *outs):
    tokens = outs[0].shape[0]
    for index, out_ref in enumerate(outs):
        rows = slice(index * tokens, (index + 1) * tokens)
        out_ref[...] = (keep_ref[rows, :].astype(F32) + other_ref[rows, :].astype(F32)).astype(
            BF16
        )


def sum_parts(keep, other, count):
    rows, columns = keep.shape
    return pl.pallas_call(
        sum_kernel,
        out_shape=[pltpu.VMEM((rows // count, columns), BF16)] * count,
        in_specs=[VMEM, VMEM],
        out_specs=[VMEM] * count,
        compiler_params=PARAMS,
        name="sum_parts",
    )(*held(keep, other))


def lay_kernel(group, columns, *refs):
    parts, out_ref, sems = refs[:group], refs[group], refs[group + 1]
    position = lax.rem(lax.axis_index("seq"), group)
    copies = []
    for offset in range(group):
        for index in range(parts[0].shape[1] // columns):
            first = (index * group + place(position, offset)) * columns
            copies.append(
                pltpu.make_async_copy(
                    parts[offset].at[:, index * columns : (index + 1) * columns],
                    out_ref.at[:, pl.ds(pl.multiple_of(first, columns), columns)],
                    sems.at[len(copies)],
                )
            )
    for copy in copies:
        copy.start()
    for copy in copies:
        copy.wait()


def lay_out(parts, columns):
    group = len(parts)
    rows, wide = parts[0].shape
    return pl.pallas_call(
        functools.partial(lay_kernel, group, columns),
        out_shape=jax.ShapeDtypeStruct((rows, group * wide), BF16),
        in_specs=[VMEM] * group,
        out_specs=pl.BlockSpec(memory_space=pl.ANY),
        scratch_shapes=[pltpu.SemaphoreType.DMA((group * wide // columns,))],
        compiler_params=PARAMS,
        name="lay_out",
    )(*held(*parts))


def swap(value, group, offset, count):
    pairs = [(i, (i // group) * group + ((i % group) ^ offset)) for i in range(count)]
    return lax.ppermute(value, "seq", pairs)


def per_device(queries, key_vectors, values, strengths, out_weight):
    count = lax.axis_size("seq")
    sides = lax.axis_size("head")
    heads = strengths.shape[1]
    tokens = queries.shape[0]
    width = queries.shape[1] // heads
    group = 1
    while group < 4 and heads % (2 * group) == 0 and count % (2 * group) == 0:
        group *= 2
    planes = count // group
    position = lax.axis_index("seq") % group
    mine = heads // group
    keys, rests = pack(queries, key_vectors, values, strengths, group)
    for offset in range(1, group):
        keys[offset] = swap(keys[offset], group, offset, count)
        rests[offset] = swap(rests[offset], group, offset, count)

    def between_planes(value, pairs):
        return lax.ppermute(
            value,
            "seq",
            [
                (source * group + i, target * group + i)
                for source, target in pairs
                for i in range(group)
            ],
        )

    split_out = sides == 2 and planes in (2, 4) and group > 1
    weights = [out_weight]
    if split_out:
        for offset in range(1, planes, 2):
            swapped = [(plane, plane ^ offset) for plane in range(planes)]
            weights.append(between_planes(out_weight, swapped))

    near = max(group // 2, 1)
    solved = []
    for part in (keys[:near], keys[near:]):
        if part:
            solved.append(invert(part, mine, tokens))
    inverses, tables = zip(*solved)
    high, low, steps, state, local_state = carry_state(keys, rests, inverses, tables)
    local, lifted = read(keys, rests, high, low, steps)

    def from_earlier(value, distance):
        pairs = [(i, i + distance * group) for i in range(count - distance * group)]
        return lax.ppermute(value, "seq", pairs)

    if planes <= 4:
        states = []
        for distance in range(1, planes):
            sent = state if distance + 1 < planes else local_state
            states.append(from_earlier(sent, distance))
    else:
        total = from_earlier(state, 1)
        distance = 1
        while distance < planes - 1:
            total = compose(from_earlier(total, distance), total)
            distance *= 2
        states = [total[:, :, width:]]
    if split_out and planes == 4:
        weights += [
            between_planes(weights[1], ((1, 2), (2, 1))),
            between_planes(weights[2], ((1, 0), (2, 3))),
        ]

    if split_out:
        row_halves = ((3, 1), (2, 0)) if group == 4 else ((1,), (0,))
        ready = join(states, local, lifted, row_halves)
        parts = [None] * group
        gathered, orders = [], []
        for targets in row_halves:
            arrays, order = [], []
            for offset in range(group):
                seen = [target ^ offset for target in targets]
                source = row_halves.index(
                    next(half for half in row_halves if set(half) == set(seen))
                )
                order.append(tuple(row_halves[source].index(block) for block in seen))
                array = ready[source]
                if offset:
                    array = swap(array, group, offset, count)
                arrays.append(array)
            gathered.append(arrays)
            orders.append(tuple(order))
        for number, targets in enumerate(row_halves):
            send, keep = project(gathered[number], weights, planes, orders[number])
            other = lax.ppermute(send, "head", [(0, 1), (1, 0)])
            for offset, part in zip(targets, sum_parts(keep, other, len(targets))):
                parts[offset] = swap(part, group, offset, count) if offset else part
        return lay_out(parts, out_weight.shape[1])

    (mixed_heads,) = join(states, local, lifted, (tuple(range(group)),))
    if group > 1:
        position_rows = []
        for offset in range(group):
            part = lax.dynamic_slice_in_dim(mixed_heads, offset * tokens, tokens, 0)
            position_rows.append(swap(part, group, offset, count) if offset else part)
        stacked = jnp.stack(position_rows)
        order = jnp.bitwise_xor(position, jnp.arange(group))
        stacked = jnp.take(stacked, order, axis=0)
        mixed_heads = jnp.swapaxes(stacked, 0, 1).reshape(tokens, heads * width)
    partial_sums = jnp.dot(
        mixed_heads,
        lax.all_gather(out_weight, "seq", axis=1, tiled=True),
        preferred_element_type=F32,
    )
    return lax.psum_scatter(
        partial_sums.astype(BF16), "head", scatter_dimension=1, tiled=True
    )


def solution(mesh):
    return jax.shard_map(
        per_device,
        mesh=mesh,
        in_specs=(
            P("seq", "head"),
            P(None, "seq", "head"),
            P(None, "seq", "head"),
            P(None, "head", "seq"),
            P("head", "seq"),
        ),
        out_specs=P("seq", "head"),
        check_vma=False,
    )
```

```python
import functools

import jax
import jax.numpy as jnp
from jax import lax
from jax.experimental import pallas as pl
from jax.experimental.pallas import tpu as pltpu
from jax.sharding import PartitionSpec as P


CHUNK = 128
EPS = 1e-06
F32 = jnp.float32
BF16 = jnp.bfloat16


def dot(a, b):
    return jnp.dot(a, b, preferred_element_type=F32)


def dot_t(a, b):
    return lax.dot_general(a, b, (((1,), (1,)), ((), ())), preferred_element_type=F32)


def split(x):
    high = x.astype(BF16)
    return high, (x - high.astype(F32)).astype(BF16)


def product3(left, right):
    left_high, left_low = split(left)
    right_high, right_low = split(right)
    lhs = jnp.concatenate([left_high, left_low], axis=1)
    rhs = jnp.concatenate(
        [
            jnp.concatenate([right_high, right_low], axis=1),
            jnp.concatenate([right_high, jnp.zeros_like(right_low)], axis=1),
        ],
        axis=0,
    )
    wide = dot(lhs, rhs)
    width = right.shape[1]
    return wide[:, :width] + wide[:, width:]


def iota(shape, axis):
    return lax.broadcasted_iota(jnp.int32, shape, axis)


def weave(first, second):
    half = first.shape[0] // 2
    return jnp.concatenate([first[:half], second[:half], first[half:], second[half:]], axis=0)


def weave_lanes(first, second):
    half = first.shape[1] // 2
    return jnp.concatenate(
        [first[:, :half], second[:, :half], first[:, half:], second[:, half:]], axis=1
    )


def place(position, offset):
    return jnp.bitwise_xor(position, offset)


VMEM = pl.BlockSpec(memory_space=pltpu.VMEM)
PARAMS = pltpu.CompilerParams(vmem_limit_bytes=12 * 2**20)


def held(*arrays):
    return [pltpu.with_memory_space_constraint(array, pltpu.VMEM) for array in arrays]


def times(chunk):
    half = chunk // 2
    row, col = iota((chunk, chunk), 0), iota((chunk, chunk), 1)
    return 2 * lax.rem(row, half) + row // half, 2 * lax.rem(col, half) + col // half


def beta_rows(tokens, width):
    return -(-4 * max(tokens // width, 1) // 16) * 16


def pack_kernel(group, key_ref, value_ref, query_ref, strength_ref, *refs):
    key_outs, rest_outs, (beta_ref, sems) = refs[:group], refs[group : 2 * group], refs[-2:]
    _, heads, tokens = beta_ref.shape
    mine = heads // group
    wide = key_outs[0].shape[1]
    width = wide // mine
    pieces = max(tokens // width, 1)
    inside = tokens // pieces
    position, _ = where_am_i(group)
    first_copy = pltpu.make_async_copy(strength_ref, beta_ref, sems.at[0])
    pairs = []
    for offset in range(group):
        lanes = pl.ds(pl.multiple_of(place(position, offset) * wide, wide), wide)
        for reflection in range(2):
            rows = pl.ds(reflection * tokens, tokens)
            pairs.append((key_ref.at[reflection, :, lanes], key_outs[offset].at[rows, :]))
    for offset in range(group):
        lanes = pl.ds(pl.multiple_of(place(position, offset) * wide, wide), wide)
        for reflection in range(2):
            pairs.append(
                (value_ref.at[reflection, :, lanes], rest_outs[offset].at[reflection])
            )
        pairs.append((query_ref.at[:, lanes], rest_outs[offset].at[2]))
    copies = [
        pltpu.make_async_copy(source, target, sems.at[1 + number])
        for number, (source, target) in enumerate(pairs)
    ]
    first_copy.start()
    for copy in copies:
        copy.start()
    first_copy.wait()
    for offset, out_ref in enumerate(key_outs):
        member = place(position, offset)
        rows = []
        for reflection in range(2):
            for piece in range(pieces):
                cuts = []
                for head in range(mine):
                    cut = beta_ref[reflection, pl.ds(member * mine + head, 1), :]
                    cuts.append(cut[:, piece * inside : (piece + 1) * inside])
                    if inside < width:
                        cuts.append(jnp.zeros((1, width - inside), F32))
                rows.append(jnp.concatenate(cuts, axis=1) if len(cuts) > 1 else cuts[0])
        both = jnp.concatenate(rows, axis=0)
        high = both.astype(BF16).astype(F32)
        spare = jnp.zeros((out_ref.shape[0] - 2 * tokens - 2 * len(rows), wide), F32)
        out_ref[2 * tokens :, :] = jnp.concatenate([high, both - high, spare], axis=0).astype(BF16)
    for copy in copies:
        copy.wait()


def pack(queries, key_vectors, values, strengths, group):
    _, tokens, wide = key_vectors.shape
    width = wide // strengths.shape[1]
    shape = (2 * tokens + beta_rows(tokens, width), wide // group)
    out = pl.pallas_call(
        functools.partial(pack_kernel, group),
        out_shape=[pltpu.VMEM(shape, BF16)] * group
        + [pltpu.VMEM((3, tokens, wide // group), BF16)] * group,
        in_specs=[pl.BlockSpec(memory_space=pltpu.HBM)] * 4,
        out_specs=[VMEM] * (2 * group),
        scratch_shapes=[
            pltpu.VMEM(strengths.shape, F32),
            pltpu.SemaphoreType.DMA((1 + 5 * group,)),
        ],
        compiler_params=PARAMS,
        name="pack",
    )(
        *(
            pltpu.with_memory_space_constraint(array, pltpu.HBM)
            for array in (key_vectors, values, queries, strengths)
        )
    )
    return list(out[:group]), list(out[group:])


def invert_kernel(heads, tokens, *refs):
    key_in, (inverse_ref, table_ref, a_buf) = refs[:-3], refs[-3:]
    width = key_in[0].shape[1] // heads
    chunk = min(CHUNK, tokens)
    per_source = tokens // chunk
    chunks = len(key_in) * per_source
    pieces = max(tokens // width, 1)
    row_time, col_time = times(chunk)
    levels = chunk.bit_length() - 1

    def joins(level):
        same = (row_time >> (level + 1)) == (col_time >> (level + 1))
        return same & (((row_time >> level) & 1) == 1) & (((col_time >> level) & 1) == 0)

    def prepare(head, index):
        lanes = lanes_of(head, width)
        key_ref, first = key_in[index // per_source], (index % per_source) * chunk
        key = woven_key(key_ref, tokens, first, chunk, lanes)
        gram = dot_t(key, key)
        wide_row, wide_col = iota(gram.shape, 0), iota(gram.shape, 1)
        square = jnp.sum(jnp.where(wide_row == wide_col, gram, 0.0), axis=0, keepdims=True)
        scale_row = lax.rsqrt(square + EPS)
        halves = key_ref[2 * tokens :, lanes].astype(F32)
        piece, inside = first // width, first % width

        def strength(reflection):
            high = reflection * pieces + piece
            low = (2 + reflection) * pieces + piece
            both = halves[high : high + 1] + halves[low : low + 1]
            return both[:, inside : inside + chunk]

        beta_row = weave_lanes(strength(0), strength(1))
        both_row = beta_row * scale_row
        table = jnp.concatenate(
            [scale_row, beta_row, both_row, jnp.zeros((5, 2 * chunk), F32)], axis=0
        )
        table_ref[head, index] = table
        system = table.T[:, 2:3] * (gram * scale_row)
        for block in range(2):
            here = slice(block * chunk, (block + 1) * chunk)
            diagonal = system[here, here]
            a_buf[head, index, block] = diagonal
            inverse_ref[head, index, block] = jnp.where(
                row_time == col_time, 1.0, 0.0
            ) - jnp.where(joins(0), diagonal, 0.0)
        inverse_ref[head, index, 2] = system[chunk:, :chunk]

    def solve(units):
        for head, index in units:
            prepare(head, index)
        every = [(head, index, block) for head, index in units for block in range(2)]
        for level in range(1, levels):
            mask = joins(level)
            inner = [
                product3(jnp.where(mask, a_buf[one], 0.0), inverse_ref[one]) for one in every
            ]
            for one, value in zip(every, inner):
                known = inverse_ref[one]
                inverse_ref[one] = known - product3(known, value)
        inner = [
            product3(inverse_ref[head, index, 2], inverse_ref[head, index, 0])
            for head, index in units
        ]
        for (head, index), value in zip(units, inner):
            inverse_ref[head, index, 2] = -product3(inverse_ref[head, index, 1], value)

    every_unit(heads, chunks, solve)


def lanes_of(head, width):
    if isinstance(head, int):
        return slice(head * width, (head + 1) * width)
    return pl.ds(pl.multiple_of(head * width, width), width)


def invert(keys, heads, tokens):
    chunk = min(CHUNK, tokens)
    chunks = len(keys) * tokens // chunk
    return pl.pallas_call(
        functools.partial(invert_kernel, heads, tokens),
        out_shape=(
            pltpu.VMEM((heads, chunks, 3, chunk, chunk), F32),
            pltpu.VMEM((heads, chunks, 8, 2 * chunk), F32),
        ),
        in_specs=[VMEM] * len(keys),
        out_specs=(VMEM, VMEM),
        scratch_shapes=[pltpu.VMEM((heads, chunks, 2, chunk, chunk), F32)],
        compiler_params=PARAMS,
        name="invert",
    )(*held(*keys))


def slot_of(group, index, per_source):
    position = lax.rem(lax.axis_index("seq"), group)
    return place(position, index // per_source) * per_source + index % per_source


def every_unit(heads, chunks, body):
    if heads * chunks <= 8:
        body([(head, index) for head in range(heads) for index in range(chunks)])
    else:

        def one_head(head, carry):
            body([(head, index) for index in range(chunks)])
            return carry

        lax.fori_loop(0, heads, one_head, 0)


def woven_key(key_ref, tokens, first, chunk, lanes):
    return weave(
        key_ref[first : first + chunk, lanes],
        key_ref[tokens + first : tokens + first + chunk, lanes],
    )


def state_kernel(group, parts, *refs):
    key_in, rest_in = refs[:group], refs[group : 2 * group]
    inverse_in = refs[2 * group : 2 * group + parts]
    table_in = refs[2 * group + parts : 2 * group + 2 * parts]
    high_ref, low_ref, step_ref, state_ref, local_ref = refs[2 * group + 2 * parts :]
    heads, per_part, _, chunk, _ = inverse_in[0].shape
    chunks = parts * per_part
    tokens = rest_in[0].shape[1]
    width = rest_in[0].shape[2] // heads
    per_source = tokens // chunk

    def solve(units):
        for head, index in units:
            lanes = lanes_of(head, width)
            part, inside = index // per_part, index % per_part
            source, first = index // per_source, (index % per_source) * chunk
            key_ref, rest_ref = key_in[source], rest_in[source]
            key = woven_key(key_ref, tokens, first, chunk, lanes).astype(F32)
            rows = slice(first, first + chunk)
            value = weave(rest_ref[0, rows, lanes], rest_ref[1, rows, lanes]).astype(F32)
            table = table_in[part][head, inside].T
            inverse = jnp.concatenate(
                [
                    jnp.concatenate(
                        [inverse_in[part][head, inside, 0], jnp.zeros((chunk, chunk), F32)],
                        axis=1,
                    ),
                    jnp.concatenate(
                        [inverse_in[part][head, inside, 2], inverse_in[part][head, inside, 1]],
                        axis=1,
                    ),
                ],
                axis=0,
            )
            right = jnp.concatenate([table[:, 2:3] * key, table[:, 1:2] * value], axis=1)
            high, low = split(table[:, 0:1] * dot3(inverse, *split(right)))
            high_ref[head, index] = high
            low_ref[head, index] = low
        for head, index in units:
            source, first = index // per_source, (index % per_source) * chunk
            turned = woven_key(key_in[source], tokens, first, chunk, lanes_of(head, width)).T
            step_ref[head, slot_of(group, index, per_source)] = dot(
                turned, high_ref[head, index]
            ) + dot(turned, low_ref[head, index])

    every_unit(heads, chunks, solve)
    totals = [[step_ref[head, slot] for slot in range(chunks)] for head in range(heads)]
    while len(totals[0]) > 1:
        totals = [
            [after(one[i], one[i + 1]) for i in range(0, len(one) - 1, 2)]
            + one[len(one) - len(one) % 2 :]
            for one in totals
        ]
    for head, (total,) in enumerate(totals):
        state_ref[head] = total.astype(BF16)
        local_ref[head] = total[:, width:].astype(BF16)


def after(earlier, later):
    width = earlier.shape[0]
    return earlier + later - dot(later[:, :width].astype(BF16), earlier.astype(BF16))


def dot3(left, high, low):
    left_high, left_low = split(left)
    return dot(left_high, high) + dot(left_low, high) + dot(left_high, low)


def carry_state(keys, rests, inverses, tables):
    group, parts = len(keys), len(inverses)
    heads, per_part, _, chunk, _ = inverses[0].shape
    chunks = parts * per_part
    width = rests[0].shape[2] // heads
    solved = pltpu.VMEM((heads, chunks, 2 * chunk, 2 * width), BF16)
    return pl.pallas_call(
        functools.partial(state_kernel, group, parts),
        out_shape=(
            solved,
            solved,
            pltpu.VMEM((heads, chunks, width, 2 * width), F32),
            pltpu.VMEM((heads, width, 2 * width), BF16),
            pltpu.VMEM((heads, width, width), BF16),
        ),
        in_specs=[VMEM] * (2 * group + 2 * parts),
        out_specs=(VMEM,) * 5,
        compiler_params=PARAMS,
        name="carry_state",
    )(*held(*keys, *rests, *inverses, *tables))


def read_kernel(group, *refs):
    key_in, rest_in = refs[:group], refs[group : 2 * group]
    high_ref, low_ref, step_ref, out_ref, lift_ref = refs[2 * group : -3]
    before_buf, local_buf, lift_buf = refs[-3:]
    heads, chunks, wide, _ = high_ref.shape
    chunk = wide // 2
    half = chunk // 2
    tokens = rest_in[0].shape[1]
    width = rest_in[0].shape[2] // heads
    per_source = tokens // chunk
    token_row = iota((chunk, 2 * chunk), 0)
    token_col = iota((chunk, 2 * chunk), 1)
    token_col = (token_col // chunk) * half + lax.rem(token_col, half)

    def answer(units):
        for head, index in units:
            lanes = lanes_of(head, width)
            source, first = index // per_source, (index % per_source) * chunk
            key = woven_key(key_in[source], tokens, first, chunk, lanes)
            query = rest_in[source][2, first : first + chunk, lanes]
            wide_query = query.astype(F32)
            scale = lax.rsqrt(jnp.sum(wide_query * wide_query, axis=1, keepdims=True) + EPS)
            scores = jnp.where(token_col <= token_row, dot_t(query, key) * scale, 0.0)
            applied = dot3(scores, high_ref[head, index], low_ref[head, index])
            local_buf[head, index] = applied[:, width:]
            lift_buf[head, index] = scale * wide_query - applied[:, :width]

    every_unit(heads, chunks, answer)
    totals = [step_ref[head, 0] for head in range(heads)]
    for head in range(heads):
        before_buf[head, 0] = jnp.zeros((width, 2 * width), BF16)
    for slot in range(1, chunks):
        for head in range(heads):
            before_buf[head, slot] = totals[head].astype(BF16)
        if slot + 1 < chunks:
            totals = [after(totals[head], step_ref[head, slot]) for head in range(heads)]

    def correct(units):
        for head, index in units:
            lanes = lanes_of(head, width)
            slot = slot_of(group, index, per_source)
            lifted = lift_buf[head, index]
            moved = dot(lifted.astype(BF16), before_buf[head, slot])
            rows = pl.ds(pl.multiple_of(slot * chunk, chunk), chunk)
            out_ref[rows, lanes] = local_buf[head, index] + moved[:, width:]
            lift_ref[rows, lanes] = (lifted - moved[:, :width]).astype(BF16)

    every_unit(heads, chunks, correct)


def read(keys, rests, high, low, steps):
    group = len(keys)
    _, tokens, wide = rests[0].shape
    chunk, width = high.shape[2] // 2, steps.shape[2]
    return pl.pallas_call(
        functools.partial(read_kernel, group),
        out_shape=(
            pltpu.VMEM((group * tokens, wide), F32),
            pltpu.VMEM((group * tokens, wide), BF16),
        ),
        in_specs=[VMEM] * (2 * group + 3),
        out_specs=(VMEM, VMEM),
        scratch_shapes=[
            pltpu.VMEM(steps.shape, BF16),
            pltpu.VMEM(steps.shape[:2] + (chunk, width), F32),
            pltpu.VMEM(steps.shape[:2] + (chunk, width), F32),
        ],
        compiler_params=PARAMS,
        name="read",
    )(*held(*keys, *rests, high, low, steps))


def join_kernel(count, splits, *refs):
    states, (local_ref, lift_ref), outs = refs[:count], refs[count : count + 2], refs[count + 2 :]
    heads, width, _ = states[0].shape
    group = sum(len(split) for split in splits)
    tokens = local_ref.shape[0] // group
    position, _ = where_am_i(group)
    for head in range(heads):
        lanes = slice(head * width, (head + 1) * width)
        total = jnp.zeros((width, width), F32)
        for state in reversed(states):
            step = state[head].astype(F32)
            if step.shape[1] == width:
                total = total + step
            else:
                total = (
                    total + step[:, width:] - dot(state[head, :, :width], total.astype(BF16))
                )
        total = total.astype(BF16)
        for split_of, out_ref in zip(splits, outs):
            for number, offset in enumerate(split_of):
                rows = pl.ds(pl.multiple_of(place(position, offset) * tokens, tokens), tokens)
                out_ref[number * tokens : (number + 1) * tokens, lanes] = (
                    local_ref[rows, lanes] + dot(lift_ref[rows, lanes], total)
                ).astype(BF16)


def join(states, local, lifted, splits):
    group = sum(len(split) for split in splits)
    rows, wide = local.shape
    return pl.pallas_call(
        functools.partial(join_kernel, len(states), splits),
        out_shape=[pltpu.VMEM((rows // group * len(split), wide), BF16) for split in splits],
        in_specs=[VMEM] * (len(states) + 2),
        out_specs=[VMEM] * len(splits),
        compiler_params=PARAMS,
        name="join",
    )(*held(*states, local, lifted))


def compose(earlier, later):
    width = earlier.shape[1]
    moved = jnp.einsum("hab,hbc->hac", later[:, :, :width], earlier, preferred_element_type=F32)
    return (earlier.astype(F32) + later.astype(F32) - moved).astype(BF16)


def where_am_i(group):
    device = lax.axis_index("seq")
    return lax.rem(device, group), device // group


def project_kernel(group, orders, *refs):
    heads_in, weight_in = refs[:group], refs[group:-4]
    send_ref, keep_ref, left_buf, all_buf = refs[-4:]
    core = lax.axis_index("head")
    position, plane = where_am_i(group)
    rows, wide = heads_in[0].shape
    tokens = rows // len(orders[0])
    columns = weight_in[0].shape[1]
    side = keep_ref.shape[1] // columns
    for member in range(group):
        lanes = pl.ds(pl.multiple_of(place(position, member) * wide, wide), wide)
        for to, at in enumerate(orders[member]):
            left_buf[to * tokens : (to + 1) * tokens, lanes] = heads_in[member][
                at * tokens : (at + 1) * tokens, :
            ]
    offsets = (0, 1, 3, 2) if len(weight_in) > 2 else (0, 1)
    for number, offset in enumerate(offsets):
        if offset == 2:
            inner = (plane == 1) | (plane == 2)
            right = jnp.where(inner, weight_in[3][...], weight_in[4][...])
        else:
            right = weight_in[number][...]
        all_buf[:, number * columns : (number + 1) * columns] = dot(left_buf[...], right).astype(
            BF16
        )
    for target, owner in ((send_ref, 1 - core), (keep_ref, core)):
        for slot in range(side):
            offset = jnp.bitwise_xor(plane, owner * side + slot)
            number = jnp.bitwise_xor(offset, offset // 2)
            target[:, slot * columns : (slot + 1) * columns] = all_buf[
                :, pl.ds(pl.multiple_of(number * columns, columns), columns)
            ]


def project(heads, weights, planes, orders):
    group = len(heads)
    rows = heads[0].shape[0]
    columns = weights[0].shape[1]
    shape = pltpu.VMEM((rows, columns * planes // 2), BF16)
    return pl.pallas_call(
        functools.partial(project_kernel, group, orders),
        out_shape=(shape, shape),
        in_specs=[VMEM] * (group + len(weights)),
        out_specs=(VMEM, VMEM),
        scratch_shapes=[
            pltpu.VMEM((rows, weights[0].shape[0]), BF16),
            pltpu.VMEM((rows, columns * planes), BF16),
        ],
        compiler_params=PARAMS,
        name="project",
    )(*held(*heads, *weights))


def sum_kernel(keep_ref, other_ref, *outs):
    tokens = outs[0].shape[0]
    for index, out_ref in enumerate(outs):
        rows = slice(index * tokens, (index + 1) * tokens)
        out_ref[...] = (keep_ref[rows, :].astype(F32) + other_ref[rows, :].astype(F32)).astype(
            BF16
        )


def sum_parts(keep, other, count):
    rows, columns = keep.shape
    return pl.pallas_call(
        sum_kernel,
        out_shape=[pltpu.VMEM((rows // count, columns), BF16)] * count,
        in_specs=[VMEM, VMEM],
        out_specs=[VMEM] * count,
        compiler_params=PARAMS,
        name="sum_parts",
    )(*held(keep, other))


def lay_kernel(group, columns, *refs):
    parts, out_ref, sems = refs[:group], refs[group], refs[group + 1]
    position = lax.rem(lax.axis_index("seq"), group)
    copies = []
    for offset in range(group):
        for index in range(parts[0].shape[1] // columns):
            first = (index * group + place(position, offset)) * columns
            copies.append(
                pltpu.make_async_copy(
                    parts[offset].at[:, index * columns : (index + 1) * columns],
                    out_ref.at[:, pl.ds(pl.multiple_of(first, columns), columns)],
                    sems.at[len(copies)],
                )
            )
    for copy in copies:
        copy.start()
    for copy in copies:
        copy.wait()


def lay_out(parts, columns):
    group = len(parts)
    rows, wide = parts[0].shape
    return pl.pallas_call(
        functools.partial(lay_kernel, group, columns),
        out_shape=jax.ShapeDtypeStruct((rows, group * wide), BF16),
        in_specs=[VMEM] * group,
        out_specs=pl.BlockSpec(memory_space=pl.ANY),
        scratch_shapes=[pltpu.SemaphoreType.DMA((group * wide // columns,))],
        compiler_params=PARAMS,
        name="lay_out",
    )(*held(*parts))


def swap(value, group, offset, count):
    pairs = [(i, (i // group) * group + ((i % group) ^ offset)) for i in range(count)]
    return lax.ppermute(value, "seq", pairs)


def per_device(queries, key_vectors, values, strengths, out_weight):
    count = lax.axis_size("seq")
    sides = lax.axis_size("head")
    heads = strengths.shape[1]
    tokens = queries.shape[0]
    width = queries.shape[1] // heads
    group = 1
    while group < 4 and heads % (2 * group) == 0 and count % (2 * group) == 0:
        group *= 2
    planes = count // group
    position = lax.axis_index("seq") % group
    mine = heads // group
    keys, rests = pack(queries, key_vectors, values, strengths, group)
    for offset in range(1, group):
        keys[offset] = swap(keys[offset], group, offset, count)
        rests[offset] = swap(rests[offset], group, offset, count)

    def between_planes(value, pairs):
        return lax.ppermute(
            value,
            "seq",
            [
                (source * group + i, target * group + i)
                for source, target in pairs
                for i in range(group)
            ],
        )

    split_out = sides == 2 and planes in (2, 4) and group > 1
    weights = [out_weight]
    if split_out:
        for offset in range(1, planes, 2):
            swapped = [(plane, plane ^ offset) for plane in range(planes)]
            weights.append(between_planes(out_weight, swapped))

    near = max(group // 2, 1)
    solved = []
    for part in (keys[:near], keys[near:]):
        if part:
            solved.append(invert(part, mine, tokens))
    inverses, tables = zip(*solved)
    high, low, steps, state, local_state = carry_state(keys, rests, inverses, tables)
    local, lifted = read(keys, rests, high, low, steps)

    def from_earlier(value, distance):
        pairs = [(i, i + distance * group) for i in range(count - distance * group)]
        return lax.ppermute(value, "seq", pairs)

    if planes <= 4:
        states, firsts = [], []
        for distance in range(1, planes):
            pairs = [(plane, plane + distance) for plane in range(planes - distance)]
            if distance == 1:
                states.append(between_planes(state, pairs))
                continue
            firsts.append(between_planes(local_state, pairs[:1]))
            if pairs[1:]:
                states.append(between_planes(state, pairs[1:]))
        states += firsts
    else:
        total = from_earlier(state, 1)
        distance = 1
        while distance < planes - 1:
            total = compose(from_earlier(total, distance), total)
            distance *= 2
        states = [total[:, :, width:]]
    if split_out and planes == 4:
        weights += [
            between_planes(weights[1], ((1, 2), (2, 1))),
            between_planes(weights[2], ((1, 0), (2, 3))),
        ]

    if split_out:
        row_halves = ((3, 1), (2, 0)) if group == 4 else ((1,), (0,))
        ready = join(states, local, lifted, row_halves)
        parts = [None] * group
        gathered, orders = [], []
        for targets in row_halves:
            arrays, order = [], []
            for offset in range(group):
                seen = [target ^ offset for target in targets]
                source = row_halves.index(
                    next(half for half in row_halves if set(half) == set(seen))
                )
                order.append(tuple(row_halves[source].index(block) for block in seen))
                array = ready[source]
                if offset:
                    array = swap(array, group, offset, count)
                arrays.append(array)
            gathered.append(arrays)
            orders.append(tuple(order))
        for number, targets in enumerate(row_halves):
            send, keep = project(gathered[number], weights, planes, orders[number])
            other = lax.ppermute(send, "head", [(0, 1), (1, 0)])
            for offset, part in zip(targets, sum_parts(keep, other, len(targets))):
                parts[offset] = swap(part, group, offset, count) if offset else part
        return lay_out(parts, out_weight.shape[1])

    (mixed_heads,) = join(states, local, lifted, (tuple(range(group)),))
    if group > 1:
        position_rows = []
        for offset in range(group):
            part = lax.dynamic_slice_in_dim(mixed_heads, offset * tokens, tokens, 0)
            position_rows.append(swap(part, group, offset, count) if offset else part)
        stacked = jnp.stack(position_rows)
        order = jnp.bitwise_xor(position, jnp.arange(group))
        stacked = jnp.take(stacked, order, axis=0)
        mixed_heads = jnp.swapaxes(stacked, 0, 1).reshape(tokens, heads * width)
    partial_sums = jnp.dot(
        mixed_heads,
        lax.all_gather(out_weight, "seq", axis=1, tiled=True),
        preferred_element_type=F32,
    )
    return lax.psum_scatter(
        partial_sums.astype(BF16), "head", scatter_dimension=1, tiled=True
    )


def solution(mesh):
    return jax.shard_map(
        per_device,
        mesh=mesh,
        in_specs=(
            P("seq", "head"),
            P(None, "seq", "head"),
            P(None, "seq", "head"),
            P(None, "head", "seq"),
            P("head", "seq"),
        ),
        out_specs=P("seq", "head"),
        check_vma=False,
    )
```

```python
import functools

import jax
import jax.numpy as jnp
from jax import lax
from jax.experimental import pallas as pl
from jax.experimental.pallas import tpu as pltpu
from jax.sharding import PartitionSpec as P


CHUNK = 128
EPS = 1e-06
F32 = jnp.float32
BF16 = jnp.bfloat16


def dot(a, b):
    return jnp.dot(a, b, preferred_element_type=F32)


def dot_t(a, b):
    return lax.dot_general(a, b, (((1,), (1,)), ((), ())), preferred_element_type=F32)


def split(x):
    high = x.astype(BF16)
    return high, (x - high.astype(F32)).astype(BF16)


def product3(left, right):
    left_high, left_low = split(left)
    right_high, right_low = split(right)
    lhs = jnp.concatenate([left_high, left_low], axis=1)
    rhs = jnp.concatenate(
        [
            jnp.concatenate([right_high, right_low], axis=1),
            jnp.concatenate([right_high, jnp.zeros_like(right_low)], axis=1),
        ],
        axis=0,
    )
    wide = dot(lhs, rhs)
    width = right.shape[1]
    return wide[:, :width] + wide[:, width:]


def iota(shape, axis):
    return lax.broadcasted_iota(jnp.int32, shape, axis)


def weave(first, second):
    half = first.shape[0] // 2
    return jnp.concatenate([first[:half], second[:half], first[half:], second[half:]], axis=0)


def weave_lanes(first, second):
    half = first.shape[1] // 2
    return jnp.concatenate(
        [first[:, :half], second[:, :half], first[:, half:], second[:, half:]], axis=1
    )


def place(position, offset):
    return jnp.bitwise_xor(position, offset)


VMEM = pl.BlockSpec(memory_space=pltpu.VMEM)
PARAMS = pltpu.CompilerParams(vmem_limit_bytes=12 * 2**20)


def held(*arrays):
    return [pltpu.with_memory_space_constraint(array, pltpu.VMEM) for array in arrays]


def times(chunk):
    half = chunk // 2
    row, col = iota((chunk, chunk), 0), iota((chunk, chunk), 1)
    return 2 * lax.rem(row, half) + row // half, 2 * lax.rem(col, half) + col // half


def beta_rows(tokens, width):
    return -(-4 * max(tokens // width, 1) // 16) * 16


def pack_kernel(group, key_ref, value_ref, query_ref, strength_ref, *refs):
    key_outs, rest_outs, (beta_ref, sems) = refs[:group], refs[group : 2 * group], refs[-2:]
    _, heads, tokens = beta_ref.shape
    mine = heads // group
    wide = key_outs[0].shape[1]
    width = wide // mine
    pieces = max(tokens // width, 1)
    inside = tokens // pieces
    position, _ = where_am_i(group)
    first_copy = pltpu.make_async_copy(strength_ref, beta_ref, sems.at[0])
    pairs = []
    for offset in range(group):
        lanes = pl.ds(pl.multiple_of(place(position, offset) * wide, wide), wide)
        for reflection in range(2):
            rows = pl.ds(reflection * tokens, tokens)
            pairs.append((key_ref.at[reflection, :, lanes], key_outs[offset].at[rows, :]))
    for offset in range(group):
        lanes = pl.ds(pl.multiple_of(place(position, offset) * wide, wide), wide)
        for reflection in range(2):
            pairs.append(
                (value_ref.at[reflection, :, lanes], rest_outs[offset].at[reflection])
            )
        pairs.append((query_ref.at[:, lanes], rest_outs[offset].at[2]))
    copies = [
        pltpu.make_async_copy(source, target, sems.at[1 + number])
        for number, (source, target) in enumerate(pairs)
    ]
    first_copy.start()
    for copy in copies:
        copy.start()
    first_copy.wait()
    for offset, out_ref in enumerate(key_outs):
        member = place(position, offset)
        rows = []
        for reflection in range(2):
            for piece in range(pieces):
                cuts = []
                for head in range(mine):
                    cut = beta_ref[reflection, pl.ds(member * mine + head, 1), :]
                    cuts.append(cut[:, piece * inside : (piece + 1) * inside])
                    if inside < width:
                        cuts.append(jnp.zeros((1, width - inside), F32))
                rows.append(jnp.concatenate(cuts, axis=1) if len(cuts) > 1 else cuts[0])
        both = jnp.concatenate(rows, axis=0)
        high = both.astype(BF16).astype(F32)
        spare = jnp.zeros((out_ref.shape[0] - 2 * tokens - 2 * len(rows), wide), F32)
        out_ref[2 * tokens :, :] = jnp.concatenate([high, both - high, spare], axis=0).astype(BF16)
    for copy in copies:
        copy.wait()


def pack(queries, key_vectors, values, strengths, group):
    _, tokens, wide = key_vectors.shape
    width = wide // strengths.shape[1]
    shape = (2 * tokens + beta_rows(tokens, width), wide // group)
    out = pl.pallas_call(
        functools.partial(pack_kernel, group),
        out_shape=[pltpu.VMEM(shape, BF16)] * group
        + [pltpu.VMEM((3, tokens, wide // group), BF16)] * group,
        in_specs=[pl.BlockSpec(memory_space=pltpu.HBM)] * 4,
        out_specs=[VMEM] * (2 * group),
        scratch_shapes=[
            pltpu.VMEM(strengths.shape, F32),
            pltpu.SemaphoreType.DMA((1 + 5 * group,)),
        ],
        compiler_params=PARAMS,
        name="pack",
    )(
        *(
            pltpu.with_memory_space_constraint(array, pltpu.HBM)
            for array in (key_vectors, values, queries, strengths)
        )
    )
    return list(out[:group]), list(out[group:])


def invert_kernel(heads, tokens, *refs):
    key_in, (inverse_ref, table_ref, a_buf) = refs[:-3], refs[-3:]
    width = key_in[0].shape[1] // heads
    chunk = min(CHUNK, tokens)
    per_source = tokens // chunk
    chunks = len(key_in) * per_source
    pieces = max(tokens // width, 1)
    row_time, col_time = times(chunk)
    levels = chunk.bit_length() - 1

    def joins(level):
        same = (row_time >> (level + 1)) == (col_time >> (level + 1))
        return same & (((row_time >> level) & 1) == 1) & (((col_time >> level) & 1) == 0)

    def prepare(head, index):
        lanes = lanes_of(head, width)
        key_ref, first = key_in[index // per_source], (index % per_source) * chunk
        key = woven_key(key_ref, tokens, first, chunk, lanes)
        gram = dot_t(key, key)
        wide_row, wide_col = iota(gram.shape, 0), iota(gram.shape, 1)
        square = jnp.sum(jnp.where(wide_row == wide_col, gram, 0.0), axis=0, keepdims=True)
        scale_row = lax.rsqrt(square + EPS)
        halves = key_ref[2 * tokens :, lanes].astype(F32)
        piece, inside = first // width, first % width

        def strength(reflection):
            high = reflection * pieces + piece
            low = (2 + reflection) * pieces + piece
            both = halves[high : high + 1] + halves[low : low + 1]
            return both[:, inside : inside + chunk]

        beta_row = weave_lanes(strength(0), strength(1))
        both_row = beta_row * scale_row
        table = jnp.concatenate(
            [scale_row, beta_row, both_row, jnp.zeros((5, 2 * chunk), F32)], axis=0
        )
        table_ref[head, index] = table
        system = table.T[:, 2:3] * (gram * scale_row)
        for block in range(2):
            here = slice(block * chunk, (block + 1) * chunk)
            diagonal = system[here, here]
            a_buf[head, index, block] = diagonal
            inverse_ref[head, index, block] = jnp.where(
                row_time == col_time, 1.0, 0.0
            ) - jnp.where(joins(0), diagonal, 0.0)
        inverse_ref[head, index, 2] = system[chunk:, :chunk]

    def solve(units):
        for head, index in units:
            prepare(head, index)
        every = [(head, index, block) for head, index in units for block in range(2)]
        for level in range(1, levels):
            mask = joins(level)
            inner = [
                product3(jnp.where(mask, a_buf[one], 0.0), inverse_ref[one]) for one in every
            ]
            for one, value in zip(every, inner):
                known = inverse_ref[one]
                inverse_ref[one] = known - product3(known, value)
        inner = [
            product3(inverse_ref[head, index, 2], inverse_ref[head, index, 0])
            for head, index in units
        ]
        for (head, index), value in zip(units, inner):
            inverse_ref[head, index, 2] = -product3(inverse_ref[head, index, 1], value)

    every_unit(heads, chunks, solve)


def lanes_of(head, width):
    if isinstance(head, int):
        return slice(head * width, (head + 1) * width)
    return pl.ds(pl.multiple_of(head * width, width), width)


def invert(keys, heads, tokens):
    chunk = min(CHUNK, tokens)
    chunks = len(keys) * tokens // chunk
    return pl.pallas_call(
        functools.partial(invert_kernel, heads, tokens),
        out_shape=(
            pltpu.VMEM((heads, chunks, 3, chunk, chunk), F32),
            pltpu.VMEM((heads, chunks, 8, 2 * chunk), F32),
        ),
        in_specs=[VMEM] * len(keys),
        out_specs=(VMEM, VMEM),
        scratch_shapes=[pltpu.VMEM((heads, chunks, 2, chunk, chunk), F32)],
        compiler_params=PARAMS,
        name="invert",
    )(*held(*keys))


def slot_of(group, index, per_source):
    position = lax.rem(lax.axis_index("seq"), group)
    return place(position, index // per_source) * per_source + index % per_source


def every_unit(heads, chunks, body):
    if heads * chunks <= 8:
        body([(head, index) for head in range(heads) for index in range(chunks)])
    else:

        def one_head(head, carry):
            body([(head, index) for index in range(chunks)])
            return carry

        lax.fori_loop(0, heads, one_head, 0)


def woven_key(key_ref, tokens, first, chunk, lanes):
    return weave(
        key_ref[first : first + chunk, lanes],
        key_ref[tokens + first : tokens + first + chunk, lanes],
    )


def state_kernel(group, parts, *refs):
    key_in, rest_in = refs[:group], refs[group : 2 * group]
    inverse_in = refs[2 * group : 2 * group + parts]
    table_in = refs[2 * group + parts : 2 * group + 2 * parts]
    high_ref, low_ref, step_ref, state_ref, local_ref = refs[2 * group + 2 * parts :]
    heads, per_part, _, chunk, _ = inverse_in[0].shape
    chunks = parts * per_part
    tokens = rest_in[0].shape[1]
    width = rest_in[0].shape[2] // heads
    per_source = tokens // chunk

    def solve(units):
        for head, index in units:
            lanes = lanes_of(head, width)
            part, inside = index // per_part, index % per_part
            source, first = index // per_source, (index % per_source) * chunk
            key_ref, rest_ref = key_in[source], rest_in[source]
            key = woven_key(key_ref, tokens, first, chunk, lanes).astype(F32)
            rows = slice(first, first + chunk)
            value = weave(rest_ref[0, rows, lanes], rest_ref[1, rows, lanes]).astype(F32)
            table = table_in[part][head, inside].T
            inverse = jnp.concatenate(
                [
                    jnp.concatenate(
                        [inverse_in[part][head, inside, 0], jnp.zeros((chunk, chunk), F32)],
                        axis=1,
                    ),
                    jnp.concatenate(
                        [inverse_in[part][head, inside, 2], inverse_in[part][head, inside, 1]],
                        axis=1,
                    ),
                ],
                axis=0,
            )
            right = jnp.concatenate([table[:, 2:3] * key, table[:, 1:2] * value], axis=1)
            high, low = split(table[:, 0:1] * dot3(inverse, *split(right)))
            high_ref[head, index] = high
            low_ref[head, index] = low
        for head, index in units:
            source, first = index // per_source, (index % per_source) * chunk
            turned = woven_key(key_in[source], tokens, first, chunk, lanes_of(head, width)).T
            step_ref[head, slot_of(group, index, per_source)] = dot(
                turned, high_ref[head, index]
            ) + dot(turned, low_ref[head, index])

    every_unit(heads, chunks, solve)
    totals = [[step_ref[head, slot] for slot in range(chunks)] for head in range(heads)]
    while len(totals[0]) > 1:
        totals = [
            [after(one[i], one[i + 1]) for i in range(0, len(one) - 1, 2)]
            + one[len(one) - len(one) % 2 :]
            for one in totals
        ]
    for head, (total,) in enumerate(totals):
        state_ref[head] = total.astype(BF16)
        local_ref[head] = total[:, width:].astype(BF16)


def after(earlier, later):
    width = earlier.shape[0]
    return earlier + later - dot(later[:, :width].astype(BF16), earlier.astype(BF16))


def dot3(left, high, low):
    left_high, left_low = split(left)
    return dot(left_high, high) + dot(left_low, high) + dot(left_high, low)


def carry_state(keys, rests, inverses, tables):
    group, parts = len(keys), len(inverses)
    heads, per_part, _, chunk, _ = inverses[0].shape
    chunks = parts * per_part
    width = rests[0].shape[2] // heads
    solved = pltpu.VMEM((heads, chunks, 2 * chunk, 2 * width), BF16)
    return pl.pallas_call(
        functools.partial(state_kernel, group, parts),
        out_shape=(
            solved,
            solved,
            pltpu.VMEM((heads, chunks, width, 2 * width), F32),
            pltpu.VMEM((heads, width, 2 * width), BF16),
            pltpu.VMEM((heads, width, width), BF16),
        ),
        in_specs=[VMEM] * (2 * group + 2 * parts),
        out_specs=(VMEM,) * 5,
        compiler_params=PARAMS,
        name="carry_state",
    )(*held(*keys, *rests, *inverses, *tables))


def read_kernel(group, *refs):
    key_in, rest_in = refs[:group], refs[group : 2 * group]
    high_ref, low_ref, step_ref, out_ref, lift_ref = refs[2 * group : -3]
    before_buf, local_buf, lift_buf = refs[-3:]
    heads, chunks, wide, _ = high_ref.shape
    chunk = wide // 2
    half = chunk // 2
    tokens = rest_in[0].shape[1]
    width = rest_in[0].shape[2] // heads
    per_source = tokens // chunk
    token_row = iota((chunk, 2 * chunk), 0)
    token_col = iota((chunk, 2 * chunk), 1)
    token_col = (token_col // chunk) * half + lax.rem(token_col, half)

    def answer(units):
        for head, index in units:
            lanes = lanes_of(head, width)
            source, first = index // per_source, (index % per_source) * chunk
            key = woven_key(key_in[source], tokens, first, chunk, lanes)
            query = rest_in[source][2, first : first + chunk, lanes]
            wide_query = query.astype(F32)
            scale = lax.rsqrt(jnp.sum(wide_query * wide_query, axis=1, keepdims=True) + EPS)
            scores = jnp.where(token_col <= token_row, dot_t(query, key) * scale, 0.0)
            applied = dot3(scores, high_ref[head, index], low_ref[head, index])
            local_buf[head, index] = applied[:, width:]
            lift_buf[head, index] = scale * wide_query - applied[:, :width]

    every_unit(heads, chunks, answer)
    totals = [step_ref[head, 0] for head in range(heads)]
    for head in range(heads):
        before_buf[head, 0] = jnp.zeros((width, 2 * width), BF16)
    for slot in range(1, chunks):
        for head in range(heads):
            before_buf[head, slot] = totals[head].astype(BF16)
        if slot + 1 < chunks:
            totals = [after(totals[head], step_ref[head, slot]) for head in range(heads)]

    def correct(units):
        for head, index in units:
            lanes = lanes_of(head, width)
            slot = slot_of(group, index, per_source)
            lifted = lift_buf[head, index]
            moved = dot(lifted.astype(BF16), before_buf[head, slot])
            rows = pl.ds(pl.multiple_of(slot * chunk, chunk), chunk)
            out_ref[rows, lanes] = local_buf[head, index] + moved[:, width:]
            lift_ref[rows, lanes] = (lifted - moved[:, :width]).astype(BF16)

    every_unit(heads, chunks, correct)


def read(keys, rests, high, low, steps):
    group = len(keys)
    _, tokens, wide = rests[0].shape
    chunk, width = high.shape[2] // 2, steps.shape[2]
    return pl.pallas_call(
        functools.partial(read_kernel, group),
        out_shape=(
            pltpu.VMEM((group * tokens, wide), F32),
            pltpu.VMEM((group * tokens, wide), BF16),
        ),
        in_specs=[VMEM] * (2 * group + 3),
        out_specs=(VMEM, VMEM),
        scratch_shapes=[
            pltpu.VMEM(steps.shape, BF16),
            pltpu.VMEM(steps.shape[:2] + (chunk, width), F32),
            pltpu.VMEM(steps.shape[:2] + (chunk, width), F32),
        ],
        compiler_params=PARAMS,
        name="read",
    )(*held(*keys, *rests, high, low, steps))


def join_kernel(count, splits, *refs):
    states, (local_ref, lift_ref), outs = refs[:count], refs[count : count + 2], refs[count + 2 :]
    heads, width, _ = states[0].shape
    group = sum(len(split) for split in splits)
    tokens = local_ref.shape[0] // group
    position, _ = where_am_i(group)
    for head in range(heads):
        lanes = slice(head * width, (head + 1) * width)
        total = None
        for state in reversed(states):
            if total is None:
                total = state[head].astype(F32)
            else:
                step = state[head].astype(F32)
                total = (
                    total + step[:, width:] - dot(state[head, :, :width], total.astype(BF16))
                )
        total = total.astype(BF16)
        for split_of, out_ref in zip(splits, outs):
            for number, offset in enumerate(split_of):
                rows = pl.ds(pl.multiple_of(place(position, offset) * tokens, tokens), tokens)
                out_ref[number * tokens : (number + 1) * tokens, lanes] = (
                    local_ref[rows, lanes] + dot(lift_ref[rows, lanes], total)
                ).astype(BF16)


def join(states, local, lifted, splits):
    group = sum(len(split) for split in splits)
    rows, wide = local.shape
    return pl.pallas_call(
        functools.partial(join_kernel, len(states), splits),
        out_shape=[pltpu.VMEM((rows // group * len(split), wide), BF16) for split in splits],
        in_specs=[VMEM] * (len(states) + 2),
        out_specs=[VMEM] * len(splits),
        compiler_params=PARAMS,
        name="join",
    )(*held(*states, local, lifted))


def compose(earlier, later):
    width = earlier.shape[1]
    moved = jnp.einsum("hab,hbc->hac", later[:, :, :width], earlier, preferred_element_type=F32)
    return (earlier.astype(F32) + later.astype(F32) - moved).astype(BF16)


def where_am_i(group):
    device = lax.axis_index("seq")
    return lax.rem(device, group), device // group


def project_kernel(group, orders, *refs):
    heads_in, weight_in = refs[:group], refs[group:-4]
    send_ref, keep_ref, left_buf, all_buf = refs[-4:]
    core = lax.axis_index("head")
    position, plane = where_am_i(group)
    rows, wide = heads_in[0].shape
    tokens = rows // len(orders[0])
    columns = weight_in[0].shape[1]
    side = keep_ref.shape[1] // columns
    for member in range(group):
        lanes = pl.ds(pl.multiple_of(place(position, member) * wide, wide), wide)
        for to, at in enumerate(orders[member]):
            left_buf[to * tokens : (to + 1) * tokens, lanes] = heads_in[member][
                at * tokens : (at + 1) * tokens, :
            ]
    offsets = (0, 1, 3, 2) if len(weight_in) > 2 else (0, 1)
    for number, offset in enumerate(offsets):
        if offset == 2:
            inner = (plane == 1) | (plane == 2)
            right = jnp.where(inner, weight_in[3][...], weight_in[4][...])
        else:
            right = weight_in[number][...]
        all_buf[:, number * columns : (number + 1) * columns] = dot(left_buf[...], right).astype(
            BF16
        )
    for target, owner in ((send_ref, 1 - core), (keep_ref, core)):
        for slot in range(side):
            offset = jnp.bitwise_xor(plane, owner * side + slot)
            number = jnp.bitwise_xor(offset, offset // 2)
            target[:, slot * columns : (slot + 1) * columns] = all_buf[
                :, pl.ds(pl.multiple_of(number * columns, columns), columns)
            ]


def project(heads, weights, planes, orders):
    group = len(heads)
    rows = heads[0].shape[0]
    columns = weights[0].shape[1]
    shape = pltpu.VMEM((rows, columns * planes // 2), BF16)
    return pl.pallas_call(
        functools.partial(project_kernel, group, orders),
        out_shape=(shape, shape),
        in_specs=[VMEM] * (group + len(weights)),
        out_specs=(VMEM, VMEM),
        scratch_shapes=[
            pltpu.VMEM((rows, weights[0].shape[0]), BF16),
            pltpu.VMEM((rows, columns * planes), BF16),
        ],
        compiler_params=PARAMS,
        name="project",
    )(*held(*heads, *weights))


def sum_kernel(keep_ref, other_ref, *outs):
    tokens = outs[0].shape[0]
    for index, out_ref in enumerate(outs):
        rows = slice(index * tokens, (index + 1) * tokens)
        out_ref[...] = (keep_ref[rows, :].astype(F32) + other_ref[rows, :].astype(F32)).astype(
            BF16
        )


def sum_parts(keep, other, count):
    rows, columns = keep.shape
    return pl.pallas_call(
        sum_kernel,
        out_shape=[pltpu.VMEM((rows // count, columns), BF16)] * count,
        in_specs=[VMEM, VMEM],
        out_specs=[VMEM] * count,
        compiler_params=PARAMS,
        name="sum_parts",
    )(*held(keep, other))


def lay_kernel(group, columns, *refs):
    parts, out_ref, sems = refs[:group], refs[group], refs[group + 1]
    position = lax.rem(lax.axis_index("seq"), group)
    copies = []
    for offset in range(group):
        for index in range(parts[0].shape[1] // columns):
            first = (index * group + place(position, offset)) * columns
            copies.append(
                pltpu.make_async_copy(
                    parts[offset].at[:, index * columns : (index + 1) * columns],
                    out_ref.at[:, pl.ds(pl.multiple_of(first, columns), columns)],
                    sems.at[len(copies)],
                )
            )
    for copy in copies:
        copy.start()
    for copy in copies:
        copy.wait()


def lay_out(parts, columns):
    group = len(parts)
    rows, wide = parts[0].shape
    return pl.pallas_call(
        functools.partial(lay_kernel, group, columns),
        out_shape=jax.ShapeDtypeStruct((rows, group * wide), BF16),
        in_specs=[VMEM] * group,
        out_specs=pl.BlockSpec(memory_space=pl.ANY),
        scratch_shapes=[pltpu.SemaphoreType.DMA((group * wide // columns,))],
        compiler_params=PARAMS,
        name="lay_out",
    )(*held(*parts))


def swap(value, group, offset, count):
    pairs = [(i, (i // group) * group + ((i % group) ^ offset)) for i in range(count)]
    return lax.ppermute(value, "seq", pairs)


def per_device(queries, key_vectors, values, strengths, out_weight):
    count = lax.axis_size("seq")
    sides = lax.axis_size("head")
    heads = strengths.shape[1]
    tokens = queries.shape[0]
    width = queries.shape[1] // heads
    group = 1
    while group < 4 and heads % (2 * group) == 0 and count % (2 * group) == 0:
        group *= 2
    planes = count // group
    position = lax.axis_index("seq") % group
    mine = heads // group
    keys, rests = pack(queries, key_vectors, values, strengths, group)
    for offset in range(1, group):
        keys[offset] = swap(keys[offset], group, offset, count)
        rests[offset] = swap(rests[offset], group, offset, count)

    def between_planes(value, pairs):
        return lax.ppermute(
            value,
            "seq",
            [
                (source * group + i, target * group + i)
                for source, target in pairs
                for i in range(group)
            ],
        )

    split_out = sides == 2 and planes in (2, 4) and group > 1
    weights = [out_weight]
    if split_out:
        for offset in range(1, planes, 2):
            swapped = [(plane, plane ^ offset) for plane in range(planes)]
            weights.append(between_planes(out_weight, swapped))

    near = max(group // 2, 1)
    solved = []
    for part in (keys[:near], keys[near:]):
        if part:
            solved.append(invert(part, mine, tokens))
    inverses, tables = zip(*solved)
    high, low, steps, state, local_state = carry_state(keys, rests, inverses, tables)
    local, lifted = read(keys, rests, high, low, steps)

    def from_earlier(value, distance):
        pairs = [(i, i + distance * group) for i in range(count - distance * group)]
        return lax.ppermute(value, "seq", pairs)

    if planes <= 4:
        states = []
        for distance in range(1, planes):
            sent = state if distance + 1 < planes else local_state
            states.append(from_earlier(sent, distance))
    else:
        total = from_earlier(state, 1)
        distance = 1
        while distance < planes - 1:
            total = compose(from_earlier(total, distance), total)
            distance *= 2
        states = [total[:, :, width:]]
    if split_out and planes == 4:
        weights += [
            between_planes(weights[1], ((1, 2), (2, 1))),
            between_planes(weights[2], ((1, 0), (2, 3))),
        ]

    if split_out:
        row_halves = ((3, 1), (2, 0)) if group == 4 else ((1,), (0,))
        ready = join(states, local, lifted, row_halves)
        parts = [None] * group
        gathered, orders = [], []
        for targets in row_halves:
            arrays, order = [], []
            for offset in range(group):
                seen = [target ^ offset for target in targets]
                source = row_halves.index(
                    next(half for half in row_halves if set(half) == set(seen))
                )
                order.append(tuple(row_halves[source].index(block) for block in seen))
                array = ready[source]
                if offset:
                    array = swap(array, group, offset, count)
                arrays.append(array)
            gathered.append(arrays)
            orders.append(tuple(order))
        for number, targets in enumerate(row_halves):
            send, keep = project(gathered[number], weights, planes, orders[number])
            other = lax.ppermute(send, "head", [(0, 1), (1, 0)])
            for offset, part in zip(targets, sum_parts(keep, other, len(targets))):
                parts[offset] = swap(part, group, offset, count) if offset else part
        return lay_out(parts, out_weight.shape[1])

    (mixed_heads,) = join(states, local, lifted, (tuple(range(group)),))
    if group > 1:
        position_rows = []
        for offset in range(group):
            part = lax.dynamic_slice_in_dim(mixed_heads, offset * tokens, tokens, 0)
            position_rows.append(swap(part, group, offset, count) if offset else part)
        stacked = jnp.stack(position_rows)
        order = jnp.bitwise_xor(position, jnp.arange(group))
        stacked = jnp.take(stacked, order, axis=0)
        mixed_heads = jnp.swapaxes(stacked, 0, 1).reshape(tokens, heads * width)
    partial_sums = jnp.dot(
        mixed_heads,
        lax.all_gather(out_weight, "seq", axis=1, tiled=True),
        preferred_element_type=F32,
    )
    return lax.psum_scatter(
        partial_sums.astype(BF16), "head", scatter_dimension=1, tiled=True
    )


def solution(mesh):
    return jax.shard_map(
        per_device,
        mesh=mesh,
        in_specs=(
            P("seq", "head"),
            P(None, "seq", "head"),
            P(None, "seq", "head"),
            P(None, "head", "seq"),
            P("head", "seq"),
        ),
        out_specs=P("seq", "head"),
        check_vma=False,
    )
```
